32 devices in a mesh: gx: 4 (over x, core), gy: 4 (over z), gz: 2 (over y).
Axes of the slice: x: 2, y: 2, z: 4, core: 2. Of those that a mesh axis runs over, the one named last changes fastest.
Arguments:
- grad_bucket: bfloat16 [32, 1, 3584, 1024], P(('gx', 'gy', 'gz')), may hold values from -72000 to 72000
- parameters: bfloat16 [1, 3584, 1024], P(None, ('gx', 'gy', 'gz')), may hold values from -4 to 4
- row_state: float32 [1, 3584], P(None, ('gx', 'gy', 'gz')), may hold values from 0.01 to 10
- column_state: float32 [1, 1024], replicated, may hold values from 0.01 to 10
Outputs:
- new_parameters: bfloat16 [1, 3584, 1024], P(None, ('gx', 'gy', 'gz'))
- row_next: float32 [1, 3584], P(None, ('gx', 'gy', 'gz'))
- column_next: float32 [1, 1024], replicated
- first_layer: bfloat16 [3584, 1024], replicated
The draws below stay inside these ranges and needn't reach their ends.
All inputs are finite; a program needn't handle non-finite values.
Results may differ from the reference program's by a relative error of at most 0.011.
Values may be sent and summed in bfloat16 or wider, within the bound.
A program may use at most 128 MiB of HBM per device.

```python
import math
import jax
import jax.numpy as jnp
from jax import lax

D = 3584
LAYERS = 1
KW = 1024
DEVICES = 32


def draw_grad_bucket(key, part):
    row_key = jax.random.fold_in(key, 11)
    column_key = jax.random.fold_in(key, 12)
    owner_key = jax.random.fold_in(key, 13)
    row_index = jnp.arange(D, dtype=jnp.int32)
    rising = jnp.exp(math.log(3.0) * row_index.astype(jnp.float32) / (D - 1))
    row_scale = rising[None, :] * jnp.exp(math.log(10.0) * jax.random.uniform(row_key, (LAYERS, D)))
    column_scale = jnp.exp(math.log(10.0) * jax.random.uniform(column_key, (LAYERS, KW)))
    owners = jax.random.permutation(owner_key, DEVICES).astype(jnp.int32)
    row_owner = row_index // (D // DEVICES)

    def one_device(device):
        device_key = jax.random.fold_in(key, 1000 + device)
        noise_part = jnp.clip(jax.random.normal(device_key, (LAYERS, D, KW)), -6.0, 6.0)
        spiked = jnp.where(row_owner == owners[device], 24.0, 1.0)
        values = noise_part * row_scale[:, :, None] * column_scale[:, None, :] * spiked[None, :, None]
        return values.astype(jnp.bfloat16)
    return lax.map(one_device, jnp.arange(DEVICES, dtype=jnp.int32))


def steps_of(rng, dims, pieces, low, high):
    loudness, own = 1.0, jax.random.fold_in(rng, 6)
    for axis_at, shards_of in pieces:
        steps = jnp.exp(jax.random.uniform(jax.random.fold_in(own, axis_at), (shards_of,), jnp.float32, low / len(pieces), high / len(pieces)))
        loudness = loudness * jnp.repeat(steps, dims[axis_at] // shards_of).reshape([-1 if axis == axis_at else 1 for axis in range(len(dims))])
    return loudness


def normal_values(stream_key, extent, scale, most, shards=(), kind=jnp.bfloat16):
    array = scale * jax.random.normal(stream_key, extent, jnp.float32)
    if shards:
        array = array * steps_of(stream_key, extent, shards, -0.22, 0.18)
    return jnp.clip(array, -most, most).astype(kind)


def setup_inputs(seed: int = 0) -> dict:
    key_of = jax.random.split(jax.random.key(seed), 5)
    grad_bucket = draw_grad_bucket(jax.random.fold_in(key_of[4], 71), 0)
    parameters = normal_values(key_of[1], (LAYERS, D, KW), 1.0, 4.0, ((1, 32),))
    row_state = jnp.clip(jnp.exp(math.log(10.0) - 6.9077553 * jax.random.uniform(key_of[2], (LAYERS, D), jnp.float32) ** steps_of(key_of[2], (LAYERS, D), ((1, 32),), -0.2, 0.2)), 0.01, 10.0)
    column_state = jnp.clip(jnp.exp(jax.random.uniform(key_of[3], (LAYERS, KW), jnp.float32, math.log(0.01), math.log(10.0))), 0.01, 10.0)
    return dict(grad_bucket=grad_bucket, parameters=parameters, row_state=row_state, column_state=column_state)


beta_two = 0.8
step_size = 0.5

def reference(grad_bucket, parameters, row_state, column_state):

    def accumulate(running, device_grad):
        return (running + device_grad.astype(jnp.float32), None)
    summed, unused = lax.scan(accumulate, jnp.zeros((LAYERS, D, KW), jnp.float32), grad_bucket)
    norm_square = jnp.sum(summed * summed)
    clip_level = 0.5 * math.sqrt(LAYERS * D * KW)
    factor = jnp.minimum(jnp.float32(1.0), clip_level / jnp.sqrt(norm_square + 1e-06))
    clipped = factor * summed
    squares = clipped * clipped
    row_next = beta_two * row_state + (1.0 - beta_two) * lax.optimization_barrier(jnp.mean(squares, axis=2))
    column_next = beta_two * column_state + (1.0 - beta_two) * lax.optimization_barrier(jnp.mean(squares, axis=1))
    row_average = lax.optimization_barrier(jnp.mean(row_next, axis=1))
    second = row_next[:, :, None] * column_next[:, None, :] / row_average[:, None, None]
    update = clipped / jnp.sqrt(second)
    new_parameters = (parameters.astype(jnp.float32) - step_size * update).astype(jnp.bfloat16)
    return (new_parameters, row_next, column_next, new_parameters[0])
```

```python
import functools
import math

import jax
import jax.numpy as jnp
from jax import lax
from jax.experimental import pallas as pl
from jax.experimental.pallas import tpu as pltpu
from jax.sharding import PartitionSpec as P

beta_two = 0.8
step_size = 0.5
AXES = ("gx", "gy", "gz")
TILE = 16
VMEM_BYTES = 67043328 - 131072


def shards(grad_bucket, parameters, row_state, column_state):
    local_grad = grad_bucket[0].astype(jnp.float32)
    layer_count, full_width, columns = local_grad.shape
    summed = lax.psum_scatter(local_grad, AXES, scatter_dimension=1, tiled=True)
    clip_level = 0.5 * math.sqrt(layer_count * full_width * columns)
    squares = summed * summed
    norm_square = lax.psum(jnp.sum(squares), AXES)
    factor = jnp.minimum(jnp.float32(1.0), clip_level / jnp.sqrt(norm_square + 1e-06))
    clipped = factor * summed
    clipped_square = clipped * clipped
    row_next = beta_two * row_state + (1.0 - beta_two) * jnp.mean(clipped_square, axis=2)
    column_part, row_total = lax.psum((jnp.sum(clipped_square, axis=1), jnp.sum(row_next, axis=1)), AXES)
    column_next = beta_two * column_state + (1.0 - beta_two) * column_part / full_width
    row_average = row_total / full_width
    second = row_next[:, :, None] * column_next[:, None, :] / row_average[:, None, None]
    update = clipped / jnp.sqrt(second)
    new_parameters = (parameters.astype(jnp.float32) - step_size * update).astype(jnp.bfloat16)
    first_layer = lax.all_gather(new_parameters[0], AXES, axis=0, tiled=True)
    return (new_parameters, row_next, column_next, first_layer)


def flip(index, mask, size):
    out, bit = 0, 1
    while bit < size:
        out = out + bit * (((index // bit) % 2 + (mask // bit) % 2) % 2)
        bit *= 2
    return out


def kernel(nx, nz, grad, params_in, row_in, col_in, new_ref, row_ref, col_ref, full,
           lg, cr, rx, rz, rc, summed, own, st, st1, tot, st2, params, row_state, col_state,
           lsem, isem, cs, cfr, cvr, fs, fr, hr, zs, zr, ks, kr, s1s, s1r, s2s, s2r,
           gzs, gzr, qs, q1r, q2r, q3r, gks, gkr, gcs, gcr):
    gx, z, y = lax.axis_index("gx"), lax.axis_index("gy"), lax.axis_index("gz")
    x, c = gx // 2, gx % 2
    rows, columns = params.shape
    lane = columns // 8
    stat_width = st.shape[1]
    full_width = rows * 4 * nz * 2
    core_peer = (x * 2 + 1 - c, z, y)
    x_peer = ((1 - x) * 2 + c, z, y)
    y_peer = (gx, z, 1 - y)
    tiles = rows // TILE
    f32, bf16 = jnp.float32, jnp.bfloat16
    scope = jax.named_scope
    blocks = [(1 - x, 1 - y), (1 - x, y), (x, 1 - y), (x, y)]
    every, flat, line_cols = pl.ds(0, columns), pl.ds(0, 7 * lane), pl.ds(7 * lane, lane)

    def zof(t):
        return flip(z, t, nz)

    def spans(t):
        low = pl.ds(0, 4 * lane)
        high = pl.ds(4 * lane, 3 * lane if t else 4 * lane)
        return (high, low) if t % 2 else (low, high)

    def width(t):
        return flat if t else every

    at_end = (z == 0) | (z == nz - 1)
    near, middle = (gx, zof(1), y), (gx, zof(3), y)

    def rdma(src, dst, ssem, rsem, peer):
        return pltpu.make_async_remote_copy(
            src_ref=src, dst_ref=dst, send_sem=ssem, recv_sem=rsem,
            device_id=peer, device_id_type=pl.DeviceIdType.MESH)

    def take_recv(view, sem):
        rdma(view, view, sem, sem, core_peer).wait_recv()

    def take_send(view, sem):
        rdma(view, view, sem, sem, core_peer).wait_send()

    rs_order = [3, 2, 1, 0]
    first = rs_order[0]
    loads = {t: pltpu.make_async_copy(grad.at[:, c, zof(t)], lg.at[t], lsem.at[t]) for t in rs_order}
    for t in rs_order:
        loads[t].start()
    small = [pltpu.make_async_copy(src, dst, isem.at[k]) for k, (src, dst) in enumerate(
        [(params_in, params), (row_in, row_state), (col_in, col_state)])]
    for copy in small:
        copy.start()

    barrier = pltpu.get_barrier_semaphore()
    plane = [((gx + a) % nx, z, (y + b) % 2) for a in range(nx) for b in range(2) if (a, b) != (0, 0)]
    line = [(gx, zof(t), y) for t in range(1, nz)]
    for peer in line + plane:
        pl.semaphore_signal(barrier, inc=1, device_id=peer, device_id_type=pl.DeviceIdType.MESH)
    with scope("barrier"):
        pl.semaphore_wait(barrier, len(plane) + len(line))

    for k, (bx, by) in enumerate(blocks):
        rdma(grad.at[bx, 1 - c, zof(first), by], cr.at[first, bx, by], cs, cfr.at[k], core_peer).start()
    for t in rs_order[1:]:
        rdma(grad.at[:, 1 - c, zof(t)], cr.at[t], cs, cvr.at[t], core_peer).start()

    def add(*terms):
        total = terms[0].astype(f32)
        for term in terms[1:]:
            total = total + term.astype(f32)
        return total

    def over_rows(step):
        @pl.loop(0, tiles, unroll=True)
        def _(i):
            step(pl.ds(pl.multiple_of(i * TILE, TILE), TILE))

    def pair_sum(t, bx, by):
        def step(r):
            lg[t, bx, by, r, :] = add(lg[t, bx, by, r, :], cr[t, bx, by, r, :]).astype(bf16)
        over_rows(step)

    def cross(t):
        return fs.at[1 if t else 0]

    def send_f(t):
        a, b = spans(t)
        rdma(lg.at[t, 1 - x, 1 - y, :, a], rx.at[t, 0, :, a], cross(t), fr.at[t], x_peer).start()
        rdma(lg.at[t, 1 - x, 1 - y, :, b], rx.at[t, 0, :, b], cross(t), fr.at[t], y_peer).start()

    def send_ga(t):
        a, b = spans(t)
        rdma(lg.at[t, 1 - x, y, :, a], rx.at[t, 1, :, a], cross(t), hr.at[t], x_peer).start()

    def send_gb(t):
        a, b = spans(t)
        rdma(lg.at[t, x, 1 - y, :, b], rx.at[t, 1, :, b], cross(t), hr.at[t], y_peer).start()

    def send_h(t):
        a, b = spans(t)
        rdma(lg.at[t, x, 1 - y, :, a], rx.at[t, 2, :, a], cross(t), hr.at[t], y_peer).start()
        rdma(lg.at[t, 1 - x, y, :, b], rx.at[t, 2, :, b], cross(t), hr.at[t], x_peer).start()

    def send_all(t):
        send_f(t)
        send_ga(t)
        send_gb(t)

    def send_line(t, slot, peer):
        rdma(lg.at[t, :, :, :, line_cols], rc.at[slot], ks, kr.at[slot], peer).start()

    def line_add(t, *slots):
        for bx in range(2):
            for by in range(2):
                def step(r):
                    lg[t, bx, by, r, line_cols] = add(
                        lg[t, bx, by, r, line_cols], *[rc[slot, bx, by, r, :] for slot in slots]).astype(bf16)
                over_rows(step)

    def stage_pair(t):
        with scope(f"pair{t}"):
            take_recv(cr.at[t], cvr.at[t])
            loads[t].wait()
            for bx, by in blocks:
                pair_sum(t, bx, by)

    def stage_first(t):
        a, b = spans(t)
        with scope(f"f{t}"):
            take_recv(rx.at[t, 0, :, width(t)], fr.at[t])

        def step(r):
            lg[t, x, 1 - y, r, a] = add(lg[t, x, 1 - y, r, a], rx[t, 0, r, a]).astype(bf16)
            lg[t, 1 - x, y, r, b] = add(lg[t, 1 - x, y, r, b], rx[t, 0, r, b]).astype(bf16)
        over_rows(step)
        send_h(t)

    def stage_second(t):
        with scope(f"h{t}"):
            take_recv(rx.at[t, 1:3, :, width(t)], hr.at[t])
        if t == 0:
            return

        def step(r):
            lg[t, x, y, r, flat] = add(lg[t, x, y, r, flat], rx[t, 1, r, flat], rx[t, 2, r, flat]).astype(bf16)
        over_rows(step)
        rdma(lg.at[t, x, y, :, flat], rz.at[t, :, flat], zs, zr.at[t], (gx, zof(t), y)).start()

    loads[first].wait()
    for k, (bx, by) in enumerate(blocks):
        with scope(f"core{k}"):
            take_recv(cr.at[first, bx, by], cfr.at[k])
        pair_sum(first, bx, by)
        if k == 0:
            send_f(first)
        elif k == 1:
            send_ga(first)
        elif k == 2:
            send_gb(first)
    for t in (3, 2, 1, 0):
        if t != first:
            stage_pair(t)
        if t:
            @pl.when(at_end)
            def _():
                send_line(t, t, near)
    stage_first(3)
    send_all(2)

    @pl.when(jnp.logical_not(at_end))
    def _():
        with scope("line3"):
            take_recv(rc.at[3], kr.at[3])
        line_add(2, 3)
        send_line(2, 4, middle)
        with scope("line2"):
            take_recv(rc.at[2], kr.at[2])
        line_add(3, 2)
        send_line(3, 5, middle)

    stage_second(3)

    @pl.when(jnp.logical_not(at_end))
    def _():
        with scope("line4"):
            take_recv(rc.at[4], kr.at[4])
        line_add(1, 4)
        send_line(1, 0, near)

    stage_first(2)
    send_all(1)
    stage_second(2)

    @pl.when(at_end)
    def _():
        with scope("line0"):
            take_recv(rc.at[0], kr.at[0])
        line_add(0, 0)

    @pl.when(jnp.logical_not(at_end))
    def _():
        with scope("line15"):
            take_recv(rc.at[1], kr.at[1])
            take_recv(rc.at[5], kr.at[5])
        line_add(0, 1, 5)

    stage_first(1)
    send_all(0)
    stage_second(1)
    stage_first(0)
    for copy in small:
        copy.wait()
    st[:, columns:] = jnp.broadcast_to(jnp.sum(row_state[...], axis=1, keepdims=True), (1, stat_width - columns))
    with scope("zearly"):
        for t in (3, 2):
            take_recv(rz.at[t, :, flat], zr.at[t])

    def gathered(r):
        summed[r, flat] = add(lg[0, x, y, r, flat], rz[3, r, flat], rz[2, r, flat])
        summed[r, line_cols] = lg[0, x, y, r, line_cols].astype(f32)
    over_rows(gathered)
    stage_second(0)
    with scope("zlate"):
        take_recv(rz.at[1, :, flat], zr.at[1])

    def final(i, carry):
        r = pl.ds(pl.multiple_of(i * TILE, TILE), TILE)
        left = add(summed[r, flat], rx[0, 1, r, flat], rx[0, 2, r, flat], rz[1, r, flat])
        right = add(summed[r, line_cols], rx[0, 1, r, line_cols], rx[0, 2, r, line_cols])
        summed[r, flat] = left
        summed[r, line_cols] = right
        left, right = left * left, right * right
        own[r, :] = jnp.sum(left, axis=1, keepdims=True) + jnp.sum(right, axis=1, keepdims=True)
        return (carry[0] + left, carry[1] + right)

    with scope("final"):
        left, right = lax.fori_loop(
            0, tiles, final, (jnp.zeros((TILE, 7 * lane), f32), jnp.zeros((TILE, lane), f32)), unroll=True)
        st[:, flat] = jnp.sum(left, axis=0, keepdims=True)
        st[:, line_cols] = jnp.sum(right, axis=0, keepdims=True)

    me = gx * 2 + y
    for peer in plane:
        rdma(st, st1.at[me], s1s, s1r, peer).start()
    st1[me] = st[...]
    take_send(cr, cs)
    take_send(rx.at[0], fs.at[0])
    take_send(rx.at[1:nz, :, :, flat], fs.at[1])
    take_send(rz.at[1:nz, :, flat], zs)
    take_send(rc.at[0:3], ks)
    diagonal = lax.broadcasted_iota(jnp.int32, (rows, rows), 0) == lax.broadcasted_iota(jnp.int32, (rows, rows), 1)
    state_down = jnp.sum(jnp.where(diagonal, jnp.broadcast_to(row_state[...], (rows, rows)), 0.0), axis=1, keepdims=True)
    with scope("stat1"):
        take_recv(st1.at[0:nx * 2 - 1], s1r)
    total = st1[0]
    for k in range(1, nx * 2):
        total = total + st1[k]
    tot[...] = total
    for t in range(1, nz):
        rdma(tot, st2.at[z], s2s, s2r, (gx, zof(t), y)).start()
    st2[z] = total
    with scope("stat2"):
        take_recv(st2.at[0:nz - 1], s2r)
    total = st2[0]
    for k in range(1, nz):
        total = total + st2[k]
    column_sum = total[:, 0:columns]
    norm_square = jnp.sum(column_sum, axis=1, keepdims=True)
    state_sum = total[:, columns:columns + 1]
    clip_level = 0.5 * math.sqrt(full_width * columns)
    factor = jnp.minimum(jnp.float32(1.0), clip_level / jnp.sqrt(norm_square + 1e-06))
    square_factor = factor * factor
    column_next = beta_two * col_state[...] + (1.0 - beta_two) * (square_factor * column_sum / full_width)
    row_average = (beta_two * state_sum + (1.0 - beta_two) * (square_factor * norm_square / columns)) / full_width
    row_next = beta_two * state_down + (1.0 - beta_two) * (square_factor * own[...] / columns)
    own[...] = (step_size * factor) / jnp.sqrt(row_next / row_average)
    col_scale = 1.0 / jnp.sqrt(column_next)

    def update(r):
        new = params[r, :].astype(f32) - (summed[r, :] * own[r, :]) * col_scale
        full[x, c, z, y, r, :] = new.astype(bf16)
    with scope("update"):
        over_rows(update)

    def same(view, ssem, rsem, peer):
        rdma(view, view, ssem, rsem, peer).start()

    def moves(t):
        return qs.at[1 if t else 0]

    def pass_core(view):
        same(view, gcs, gcr, core_peer)

    def send_q1(t):
        u, (a, b) = zof(t), spans(t)
        same(full.at[x, c, u, y, :, a], moves(t), q1r.at[t], y_peer)
        same(full.at[x, c, u, y, :, b], moves(t), q1r.at[t], x_peer)

    def send_q2(t):
        u, (a, b) = zof(t), spans(t)
        same(full.at[x, c, u, y, :, a], moves(t), q2r.at[t], x_peer)
        same(full.at[x, c, u, y, :, b], moves(t), q2r.at[t], y_peer)
        pass_core(full.at[x, c, u, y, :, width(t)])

    def gather_own(t):
        with scope(f"gz{t}"):
            take_recv(full.at[x, c, zof(t), y, :, flat], gzr.at[t])
        send_q1(t)
        send_q2(t)

    def gather_cross(t):
        u, (a, b) = zof(t), spans(t)
        with scope(f"q1_{t}"):
            take_recv(full.at[x, c, u, y, :, width(t)], q1r.at[t])
        same(full.at[x, c, u, 1 - y, :, a], moves(t), q3r.at[t], x_peer)
        same(full.at[1 - x, c, u, y, :, b], moves(t), q3r.at[t], y_peer)

    def gather_side(t):
        u = zof(t)
        with scope(f"q2_{t}"):
            take_recv(full.at[x, c, u, y, :, width(t)], q2r.at[t])
        pass_core(full.at[1 - x, c, u, y, :, width(t)])
        pass_core(full.at[x, c, u, 1 - y, :, width(t)])

    def gather_far(t):
        u = zof(t)
        with scope(f"q3_{t}"):
            take_recv(full.at[x, c, u, y, :, width(t)], q3r.at[t])
        pass_core(full.at[1 - x, c, u, 1 - y, :, width(t)])

    def strip(t):
        return full.at[:, c, zof(t), :, :, line_cols]

    def pass_strip(t, slot, peer):
        same(strip(t), gks, gkr.at[slot], peer)

    def take_strip(t):
        with scope(f"strip{t}"):
            take_recv(strip(t), gkr.at[t])
        pass_core(strip(t))

    inner = jnp.logical_not(at_end)
    send_q1(0)
    for t in range(1, nz):
        same(full.at[x, c, z, y, :, flat], gzs, gzr.at[t], (gx, zof(t), y))
    send_q2(0)
    new_ref[...] = full[x, c, z, y]
    col_ref[...] = column_next
    row_ref[...] = jnp.sum(jnp.where(diagonal, jnp.broadcast_to(row_next, (rows, rows)), 0.0), axis=0, keepdims=True)
    gather_cross(0)
    gather_own(1)
    gather_side(0)
    gather_far(0)
    pass_strip(0, 1, near)

    @pl.when(inner)
    def _():
        pass_strip(0, 3, middle)

    gather_cross(1)
    gather_own(2)
    gather_side(1)
    gather_far(1)
    gather_cross(2)
    gather_own(3)
    take_strip(1)

    @pl.when(inner)
    def _():
        pass_strip(1, 2, middle)

    gather_side(2)
    gather_far(2)

    @pl.when(inner)
    def _():
        take_strip(3)
        pass_strip(3, 2, near)

    gather_cross(3)

    @pl.when(inner)
    def _():
        take_strip(2)
        pass_strip(2, 3, near)

    gather_side(3)

    @pl.when(at_end)
    def _():
        take_strip(2)

    gather_far(3)

    @pl.when(at_end)
    def _():
        take_strip(3)

    with scope("finish"):
        take_send(st1.at[0:nx * 2 - 1], s1s)
        take_send(st2.at[0:nz - 1], s2s)
        take_send(rz.at[1:nz, :, flat], gzs)
        take_send(rx.at[0], qs.at[0])
        take_send(rx.at[1:nz, :, :, flat], qs.at[1])

        @pl.when(at_end)
        def _():
            take_send(rc.at[0], gks)

        @pl.when(inner)
        def _():
            take_send(rc.at[0:5], gks)

        take_send(full.at[:, c], gcs)
        take_recv(full.at[:, c], gcr)


def write_out(nz, new, row, col, full, new_out, row_out, col_out, full_out, sem):
    pieces = [(full.at[a, b, u], full_out.at[a, b, u]) for a in range(2) for b in range(2) for u in range(nz)]
    copies = [pltpu.make_async_copy(src, dst, sem.at[0]) for src, dst in pieces]
    small = [pltpu.make_async_copy(src, dst, sem.at[k + 1])
             for k, (src, dst) in enumerate([(new, new_out), (row, row_out), (col, col_out)])]
    for copy in copies + small:
        copy.start()
    for copy in small:
        copy.wait()
    pltpu.make_async_copy(full, full_out, sem.at[0]).wait()


def fused(nx, nz, grad_bucket, parameters, row_state, column_state):
    _, _, full_width, columns = grad_bucket.shape
    rows = parameters.shape[1]
    lane = columns // 8
    bf16, f32 = jnp.bfloat16, jnp.float32
    vmem = pl.BlockSpec(memory_space=pltpu.VMEM)
    hbm = pl.BlockSpec(memory_space=pltpu.HBM)
    dma = pltpu.SemaphoreType.DMA
    one = dma(())
    shapes = [((rows, columns), bf16), ((1, rows), f32), ((1, columns), f32), ((2, 2, nz, 2, rows, columns), bf16)]
    held = 2 * columns * (rows + full_width) + 4 * (columns + -(-rows // 128) * 128)
    stat = columns + 128
    results = pl.pallas_call(
        functools.partial(kernel, nx, nz),
        out_shape=tuple(pltpu.VMEM(*shape) for shape in shapes),
        in_specs=[hbm] * 4,
        out_specs=(vmem,) * 4,
        scratch_shapes=[
            pltpu.VMEM((nz, 2, 2, rows, columns), bf16),
            pltpu.VMEM((nz, 2, 2, rows, columns), bf16),
            pltpu.VMEM((nz, 3, rows, columns), bf16),
            pltpu.VMEM((nz, rows, columns), bf16),
            pltpu.VMEM((6, 2, 2, rows, lane), bf16),
            pltpu.VMEM((rows, columns), f32),
            pltpu.VMEM((rows, 1), f32),
            pltpu.VMEM((1, stat), f32),
            pltpu.VMEM((nx * 2, 1, stat), f32),
            pltpu.VMEM((1, stat), f32),
            pltpu.VMEM((nz, 1, stat), f32),
            pltpu.VMEM((rows, columns), bf16),
            pltpu.VMEM((1, rows), f32),
            pltpu.VMEM((1, columns), f32),
            dma((nz,)), dma((3,)), one, dma((4,)), dma((nz,)), dma((2,)), dma((nz,)), dma((nz,)),
            one, dma((nz,)), one, dma((6,)), one, one, one, one,
            one, dma((nz,)), dma((2,)), dma((nz,)), dma((nz,)), dma((nz,)), one, dma((nz,)), one, one,
        ],
        compiler_params=pltpu.CompilerParams(
            collective_id=0, has_side_effects=True, vmem_limit_bytes=VMEM_BYTES - held),
    )(grad_bucket.reshape(2, 2, nz, 2, rows, columns), parameters[0], row_state, column_state)
    new, row, col, full = pl.pallas_call(
        functools.partial(write_out, nz),
        out_shape=tuple(jax.ShapeDtypeStruct(*shape) for shape in shapes),
        in_specs=[vmem] * 4,
        out_specs=(hbm,) * 4,
        scratch_shapes=[dma((4,))],
        compiler_params=pltpu.CompilerParams(vmem_limit_bytes=4 * 1024 * 1024),
    )(*[pltpu.with_memory_space_constraint(result, pltpu.VMEM) for result in results])
    return (new[None], row, col, full.reshape(full_width, columns))


def solution(mesh):
    nx, nz, ny = (mesh.shape[a] for a in AXES)
    in_specs = (
        P(AXES, None, None, None),
        P(None, AXES, None),
        P(None, AXES),
        P(),
    )
    out_specs = (P(None, AXES, None), P(None, AXES), P(), P())
    fits = nx == 4 and ny == 2 and nz == 4

    def body(grad_bucket, parameters, row_state, column_state):
        if fits and grad_bucket.shape[1] == 1 and parameters.shape[1] % TILE == 0 and grad_bucket.shape[3] % 1024 == 0:
            return fused(nx, nz, grad_bucket, parameters, row_state, column_state)
        return shards(grad_bucket, parameters, row_state, column_state)

    return jax.shard_map(body, mesh=mesh, in_specs=in_specs, out_specs=out_specs, check_vma=False)
```

```python
import functools
import math

import jax
import jax.numpy as jnp
from jax import lax
from jax.experimental import pallas as pl
from jax.experimental.pallas import tpu as pltpu
from jax.sharding import PartitionSpec as P

beta_two = 0.8
step_size = 0.5
AXES = ("gx", "gy", "gz")
TILE = 16
VMEM_BYTES = 67043328 - 131072


def shards(grad_bucket, parameters, row_state, column_state):
    local_grad = grad_bucket[0].astype(jnp.float32)
    layer_count, full_width, columns = local_grad.shape
    summed = lax.psum_scatter(local_grad, AXES, scatter_dimension=1, tiled=True)
    clip_level = 0.5 * math.sqrt(layer_count * full_width * columns)
    squares = summed * summed
    norm_square = lax.psum(jnp.sum(squares), AXES)
    factor = jnp.minimum(jnp.float32(1.0), clip_level / jnp.sqrt(norm_square + 1e-06))
    clipped = factor * summed
    clipped_square = clipped * clipped
    row_next = beta_two * row_state + (1.0 - beta_two) * jnp.mean(clipped_square, axis=2)
    column_part, row_total = lax.psum((jnp.sum(clipped_square, axis=1), jnp.sum(row_next, axis=1)), AXES)
    column_next = beta_two * column_state + (1.0 - beta_two) * column_part / full_width
    row_average = row_total / full_width
    second = row_next[:, :, None] * column_next[:, None, :] / row_average[:, None, None]
    update = clipped / jnp.sqrt(second)
    new_parameters = (parameters.astype(jnp.float32) - step_size * update).astype(jnp.bfloat16)
    first_layer = lax.all_gather(new_parameters[0], AXES, axis=0, tiled=True)
    return (new_parameters, row_next, column_next, first_layer)


def flip(index, mask, size):
    out, bit = 0, 1
    while bit < size:
        out = out + bit * (((index // bit) % 2 + (mask // bit) % 2) % 2)
        bit *= 2
    return out


def kernel(nx, nz, grad, params_in, row_in, col_in, new_ref, row_ref, col_ref, full,
           lg, cr, rx, rz, rc, summed, own, st, st1, tot, st2, params, row_state, col_state,
           lsem, isem, cs, cfr, cvr, fs, fr, hr, zs, zr, ks, kr, s1s, s1r, s2s, s2r,
           gzs, gzr, qs, q1r, q2r, q3r, gks, gkr, gcs, gcr):
    gx, z, y = lax.axis_index("gx"), lax.axis_index("gy"), lax.axis_index("gz")
    x, c = gx // 2, gx % 2
    rows, columns = params.shape
    lane = columns // 8
    stat_width = st.shape[1]
    full_width = rows * 4 * nz * 2
    core_peer = (x * 2 + 1 - c, z, y)
    x_peer = ((1 - x) * 2 + c, z, y)
    y_peer = (gx, z, 1 - y)
    tiles = rows // TILE
    f32, bf16 = jnp.float32, jnp.bfloat16
    scope = jax.named_scope
    blocks = [(1 - x, 1 - y), (1 - x, y), (x, 1 - y), (x, y)]
    every, flat, line_cols = pl.ds(0, columns), pl.ds(0, 7 * lane), pl.ds(7 * lane, lane)

    def zof(t):
        return flip(z, t, nz)

    def spans(t):
        low = pl.ds(0, 4 * lane)
        high = pl.ds(4 * lane, 3 * lane if t else 4 * lane)
        return (high, low) if t % 2 else (low, high)

    def width(t):
        return flat if t else every

    inside = (z + z // 2) % 2
    near, middle = (gx, zof(1), y), (gx, zof(3), y)
    origin = [z, zof(1), flip(z, 2 + inside, nz), flip(z, 3 - inside, nz)]

    def on_end(step):
        pl.when(inside == 0)(step)

    def on_inner(step):
        pl.when(inside == 1)(step)

    def rdma(src, dst, ssem, rsem, peer):
        return pltpu.make_async_remote_copy(
            src_ref=src, dst_ref=dst, send_sem=ssem, recv_sem=rsem,
            device_id=peer, device_id_type=pl.DeviceIdType.MESH)

    def take_recv(view, sem):
        rdma(view, view, sem, sem, core_peer).wait_recv()

    def take_send(view, sem):
        rdma(view, view, sem, sem, core_peer).wait_send()

    rs_order = [3, 2, 1, 0]
    first = rs_order[0]
    loads = {t: pltpu.make_async_copy(grad.at[:, c, zof(t)], lg.at[t], lsem.at[t]) for t in rs_order}
    for t in rs_order:
        loads[t].start()
    small = [pltpu.make_async_copy(src, dst, isem.at[k]) for k, (src, dst) in enumerate(
        [(params_in, params), (row_in, row_state), (col_in, col_state)])]
    for copy in small:
        copy.start()

    barrier = pltpu.get_barrier_semaphore()
    plane = [((gx + a) % nx, z, (y + b) % 2) for a in range(nx) for b in range(2) if (a, b) != (0, 0)]
    line = [(gx, zof(t), y) for t in range(1, nz)]
    for peer in line + plane:
        pl.semaphore_signal(barrier, inc=1, device_id=peer, device_id_type=pl.DeviceIdType.MESH)
    with scope("barrier"):
        pl.semaphore_wait(barrier, len(plane) + len(line))

    for k, (bx, by) in enumerate(blocks):
        rdma(grad.at[bx, 1 - c, zof(first), by], cr.at[first, bx, by], cs, cfr.at[k], core_peer).start()
    for t in rs_order[1:]:
        rdma(grad.at[:, 1 - c, zof(t)], cr.at[t], cs, cvr.at[t], core_peer).start()

    def add(*terms):
        total = terms[0].astype(f32)
        for term in terms[1:]:
            total = total + term.astype(f32)
        return total

    def over_rows(step):
        @pl.loop(0, tiles, unroll=True)
        def _(i):
            step(pl.ds(pl.multiple_of(i * TILE, TILE), TILE))

    def pair_sum(t, bx, by):
        def step(r):
            lg[t, bx, by, r, :] = add(lg[t, bx, by, r, :], cr[t, bx, by, r, :]).astype(bf16)
        over_rows(step)

    def cross(t):
        return fs.at[1 if t else 0]

    def send_f(t):
        a, b = spans(t)
        rdma(lg.at[t, 1 - x, 1 - y, :, a], rx.at[t, 0, :, a], cross(t), fr.at[t], x_peer).start()
        rdma(lg.at[t, 1 - x, 1 - y, :, b], rx.at[t, 0, :, b], cross(t), fr.at[t], y_peer).start()

    def send_ga(t):
        a, b = spans(t)
        rdma(lg.at[t, 1 - x, y, :, a], rx.at[t, 1, :, a], cross(t), hr.at[t], x_peer).start()

    def send_gb(t):
        a, b = spans(t)
        rdma(lg.at[t, x, 1 - y, :, b], rx.at[t, 1, :, b], cross(t), hr.at[t], y_peer).start()

    def send_h(t):
        a, b = spans(t)
        rdma(lg.at[t, x, 1 - y, :, a], rx.at[t, 2, :, a], cross(t), hr.at[t], y_peer).start()
        rdma(lg.at[t, 1 - x, y, :, b], rx.at[t, 2, :, b], cross(t), hr.at[t], x_peer).start()

    def send_all(t):
        send_f(t)
        send_ga(t)
        send_gb(t)

    def send_line(t, slot, peer):
        rdma(lg.at[t, :, :, :, line_cols], rc.at[slot], ks, kr.at[slot], peer).start()

    def line_add(t, *slots):
        for bx in range(2):
            for by in range(2):
                def step(r):
                    lg[t, bx, by, r, line_cols] = add(
                        lg[t, bx, by, r, line_cols], *[rc[slot, bx, by, r, :] for slot in slots]).astype(bf16)
                over_rows(step)

    def stage_pair(t):
        with scope(f"pair{t}"):
            take_recv(cr.at[t], cvr.at[t])
            loads[t].wait()
            for bx, by in blocks:
                pair_sum(t, bx, by)

    def stage_first(t):
        a, b = spans(t)
        with scope(f"f{t}"):
            take_recv(rx.at[t, 0, :, width(t)], fr.at[t])

        def step(r):
            lg[t, x, 1 - y, r, a] = add(lg[t, x, 1 - y, r, a], rx[t, 0, r, a]).astype(bf16)
            lg[t, 1 - x, y, r, b] = add(lg[t, 1 - x, y, r, b], rx[t, 0, r, b]).astype(bf16)
        over_rows(step)
        send_h(t)

    def send_far(t, slot, peer):
        rdma(lg.at[t, x, y, :, flat], rz.at[slot, :, flat], zs, zr.at[slot], peer).start()

    def take_far(slot):
        with scope(f"far{slot}"):
            take_recv(rz.at[slot, :, flat], zr.at[slot])

    def second_add(t, *slots):
        def step(r):
            lg[t, x, y, r, flat] = add(lg[t, x, y, r, flat], rx[t, 1, r, flat], rx[t, 2, r, flat],
                                       *[rz[slot, r, flat] for slot in slots]).astype(bf16)
        over_rows(step)

    def stage_second(t):
        with scope(f"h{t}"):
            take_recv(rx.at[t, 1:3, :, width(t)], hr.at[t])

    loads[first].wait()
    for k, (bx, by) in enumerate(blocks):
        with scope(f"core{k}"):
            take_recv(cr.at[first, bx, by], cfr.at[k])
        pair_sum(first, bx, by)
        if k == 0:
            send_f(first)
        elif k == 1:
            send_ga(first)
        elif k == 2:
            send_gb(first)
    on_end(lambda: send_line(3, 3, near))
    stage_pair(2)
    on_end(lambda: send_line(2, 2, near))
    stage_first(3)
    send_all(2)
    stage_pair(1)
    on_end(lambda: send_line(1, 1, near))
    stage_pair(0)

    @on_end
    def _():
        rz[5] = jnp.zeros((rows, columns), bf16)

    @on_inner
    def _():
        with scope("line3"):
            take_recv(rc.at[3], kr.at[3])
        line_add(2, 3)
        send_line(2, 4, middle)
        with scope("line2"):
            take_recv(rc.at[2], kr.at[2])
        line_add(3, 2)
        send_line(3, 5, middle)

    stage_second(3)
    second_add(3)
    on_end(lambda: send_far(3, 3, near))

    @on_inner
    def _():
        with scope("line4"):
            take_recv(rc.at[4], kr.at[4])
        line_add(1, 4)
        send_line(1, 0, near)

    stage_first(2)
    send_all(1)
    stage_second(2)

    @on_end
    def _():
        second_add(2)
        send_far(2, 2, near)
        with scope("line0"):
            take_recv(rc.at[0], kr.at[0])
        line_add(0, 0)

    @on_inner
    def _():
        take_far(3)
        second_add(2, 3)
        send_far(2, 4, middle)
        with scope("line15"):
            take_recv(rc.at[1], kr.at[1])
            take_recv(rc.at[5], kr.at[5])
        line_add(0, 1, 5)

    stage_first(1)
    send_all(0)

    @on_inner
    def _():
        take_far(2)

        def step(r):
            lg[3, x, y, r, flat] = add(lg[3, x, y, r, flat], rz[2, r, flat]).astype(bf16)
        over_rows(step)
        send_far(3, 5, middle)

    stage_second(1)

    @on_end
    def _():
        second_add(1)
        send_far(1, 1, near)

    @on_inner
    def _():
        take_far(4)
        second_add(1, 4)
        send_far(1, 1, near)

    stage_first(0)
    for copy in small:
        copy.wait()
    st[:, columns:] = jnp.broadcast_to(jnp.sum(row_state[...], axis=1, keepdims=True), (1, stat_width - columns))
    stage_second(0)
    take_far(1)
    on_inner(lambda: take_far(5))

    def final(i, carry):
        r = pl.ds(pl.multiple_of(i * TILE, TILE), TILE)
        left = add(lg[0, x, y, r, flat], rx[0, 1, r, flat], rx[0, 2, r, flat], rz[1, r, flat], rz[5, r, flat])
        right = add(lg[0, x, y, r, line_cols], rx[0, 1, r, line_cols], rx[0, 2, r, line_cols])
        summed[r, flat] = left
        summed[r, line_cols] = right
        left, right = left * left, right * right
        own[r, :] = jnp.sum(left, axis=1, keepdims=True) + jnp.sum(right, axis=1, keepdims=True)
        return (carry[0] + left, carry[1] + right)

    with scope("final"):
        left, right = lax.fori_loop(
            0, tiles, final, (jnp.zeros((TILE, 7 * lane), f32), jnp.zeros((TILE, lane), f32)), unroll=True)
        st[:, flat] = jnp.sum(left, axis=0, keepdims=True)
        st[:, line_cols] = jnp.sum(right, axis=0, keepdims=True)

    me = gx * 2 + y
    for peer in plane:
        rdma(st, st1.at[me], s1s, s1r, peer).start()
    st1[me] = st[...]
    take_send(cr, cs)
    take_send(rx.at[0], fs.at[0])
    take_send(rx.at[1:nz, :, :, flat], fs.at[1])
    take_send(rz.at[1:4, :, flat], zs)
    take_send(rc.at[0:3], ks)
    diagonal = lax.broadcasted_iota(jnp.int32, (rows, rows), 0) == lax.broadcasted_iota(jnp.int32, (rows, rows), 1)
    state_down = jnp.sum(jnp.where(diagonal, jnp.broadcast_to(row_state[...], (rows, rows)), 0.0), axis=1, keepdims=True)
    with scope("stat1"):
        take_recv(st1.at[0:nx * 2 - 1], s1r)
    total = st1[0]
    for k in range(1, nx * 2):
        total = total + st1[k]
    tot[...] = total
    for t in range(1, nz):
        rdma(tot, st2.at[z], s2s, s2r, (gx, zof(t), y)).start()
    st2[z] = total
    with scope("stat2"):
        take_recv(st2.at[0:nz - 1], s2r)
    total = st2[0]
    for k in range(1, nz):
        total = total + st2[k]
    column_sum = total[:, 0:columns]
    norm_square = jnp.sum(column_sum, axis=1, keepdims=True)
    state_sum = total[:, columns:columns + 1]
    clip_level = 0.5 * math.sqrt(full_width * columns)
    factor = jnp.minimum(jnp.float32(1.0), clip_level / jnp.sqrt(norm_square + 1e-06))
    square_factor = factor * factor
    column_next = beta_two * col_state[...] + (1.0 - beta_two) * (square_factor * column_sum / full_width)
    row_average = (beta_two * state_sum + (1.0 - beta_two) * (square_factor * norm_square / columns)) / full_width
    row_next = beta_two * state_down + (1.0 - beta_two) * (square_factor * own[...] / columns)
    own[...] = (step_size * factor) / jnp.sqrt(row_next / row_average)
    col_scale = 1.0 / jnp.sqrt(column_next)

    def update(r):
        new = params[r, :].astype(f32) - (summed[r, :] * own[r, :]) * col_scale
        full[x, c, z, y, r, :] = new.astype(bf16)
    with scope("update"):
        over_rows(update)

    def same(view, ssem, rsem, peer):
        rdma(view, view, ssem, rsem, peer).start()

    def moves(t):
        return qs.at[1 if t else 0]

    def pass_core(view):
        same(view, gcs, gcr, core_peer)

    def send_q1(t):
        u, (a, b) = origin[t], spans(t)
        same(full.at[x, c, u, y, :, a], moves(t), q1r.at[t], y_peer)
        same(full.at[x, c, u, y, :, b], moves(t), q1r.at[t], x_peer)

    def send_q2(t):
        u, (a, b) = origin[t], spans(t)
        same(full.at[x, c, u, y, :, a], moves(t), q2r.at[t], x_peer)
        same(full.at[x, c, u, y, :, b], moves(t), q2r.at[t], y_peer)
        pass_core(full.at[x, c, u, y, :, width(t)])

    def send_own(t):
        send_q1(t)
        send_q2(t)

    def pass_far(t, slot, peer):
        same(full.at[x, c, origin[t], y, :, flat], gzs, gzr.at[slot], peer)

    def take_z(t):
        with scope(f"gz{t}"):
            take_recv(full.at[x, c, origin[t], y, :, flat], gzr.at[t])

    def gather_cross(t):
        u, (a, b) = origin[t], spans(t)
        with scope(f"q1_{t}"):
            take_recv(full.at[x, c, u, y, :, width(t)], q1r.at[t])
        same(full.at[x, c, u, 1 - y, :, a], moves(t), q3r.at[t], x_peer)
        same(full.at[1 - x, c, u, y, :, b], moves(t), q3r.at[t], y_peer)

    def gather_side(t):
        u = origin[t]
        with scope(f"q2_{t}"):
            take_recv(full.at[x, c, u, y, :, width(t)], q2r.at[t])
        pass_core(full.at[1 - x, c, u, y, :, width(t)])
        pass_core(full.at[x, c, u, 1 - y, :, width(t)])

    def gather_far(t):
        u = origin[t]
        with scope(f"q3_{t}"):
            take_recv(full.at[x, c, u, y, :, width(t)], q3r.at[t])
        pass_core(full.at[1 - x, c, u, 1 - y, :, width(t)])

    def strip(t):
        return full.at[:, c, origin[t], :, :, line_cols]

    def pass_strip(t, slot, peer):
        same(strip(t), gks, gkr.at[slot], peer)

    def take_strip(t):
        with scope(f"strip{t}"):
            take_recv(strip(t), gkr.at[t])
        pass_core(strip(t))

    pass_far(0, 1, near)
    send_q1(0)
    on_inner(lambda: pass_far(0, 2, middle))
    send_q2(0)
    new_ref[...] = full[x, c, z, y]
    col_ref[...] = column_next
    row_ref[...] = jnp.sum(jnp.where(diagonal, jnp.broadcast_to(row_next, (rows, rows)), 0.0), axis=0, keepdims=True)
    gather_cross(0)
    take_z(1)
    on_inner(lambda: pass_far(1, 3, middle))
    send_own(1)

    @on_inner
    def _():
        take_z(2)
        pass_far(2, 2, near)

    gather_side(0)
    gather_far(0)
    pass_strip(0, 1, near)
    on_inner(lambda: pass_strip(0, 2, middle))
    gather_cross(1)
    on_end(lambda: take_z(2))
    send_own(2)

    @on_inner
    def _():
        take_z(3)
        pass_far(3, 3, near)

    gather_side(1)
    gather_far(1)
    take_strip(1)
    on_inner(lambda: pass_strip(1, 3, middle))
    gather_cross(2)
    on_end(lambda: take_z(3))
    send_own(3)

    @on_inner
    def _():
        take_strip(2)
        pass_strip(2, 2, near)

    gather_side(2)
    gather_far(2)

    @on_inner
    def _():
        take_strip(3)
        pass_strip(3, 3, near)

    on_end(lambda: take_strip(2))
    gather_cross(3)
    gather_side(3)
    on_end(lambda: take_strip(3))
    gather_far(3)

    with scope("finish"):
        take_send(st1.at[0:nx * 2 - 1], s1s)
        take_send(st2.at[0:nz - 1], s2s)
        take_send(rx.at[0], qs.at[0])
        take_send(rx.at[1:nz, :, :, flat], qs.at[1])

        @on_end
        def _():
            take_send(rz.at[1, :, flat], gzs)
            take_send(rc.at[0], gks)

        @on_inner
        def _():
            take_send(rz.at[1:6, :, flat], gzs)
            take_send(rc.at[0:5], gks)

        take_send(full.at[:, c], gcs)
        take_recv(full.at[:, c], gcr)


def write_out(nz, new, row, col, full, new_out, row_out, col_out, full_out, sem):
    pieces = [(full.at[a, b, u], full_out.at[a, b, u]) for a in range(2) for b in range(2) for u in range(nz)]
    copies = [pltpu.make_async_copy(src, dst, sem.at[0]) for src, dst in pieces]
    small = [pltpu.make_async_copy(src, dst, sem.at[k + 1])
             for k, (src, dst) in enumerate([(new, new_out), (row, row_out), (col, col_out)])]
    for copy in copies + small:
        copy.start()
    for copy in small:
        copy.wait()
    pltpu.make_async_copy(full, full_out, sem.at[0]).wait()


def fused(nx, nz, grad_bucket, parameters, row_state, column_state):
    _, _, full_width, columns = grad_bucket.shape
    rows = parameters.shape[1]
    lane = columns // 8
    bf16, f32 = jnp.bfloat16, jnp.float32
    vmem = pl.BlockSpec(memory_space=pltpu.VMEM)
    hbm = pl.BlockSpec(memory_space=pltpu.HBM)
    dma = pltpu.SemaphoreType.DMA
    one = dma(())
    shapes = [((rows, columns), bf16), ((1, rows), f32), ((1, columns), f32), ((2, 2, nz, 2, rows, columns), bf16)]
    held = 2 * columns * (rows + full_width) + 4 * (columns + -(-rows // 128) * 128)
    stat = columns + 128
    results = pl.pallas_call(
        functools.partial(kernel, nx, nz),
        out_shape=tuple(pltpu.VMEM(*shape) for shape in shapes),
        in_specs=[hbm] * 4,
        out_specs=(vmem,) * 4,
        scratch_shapes=[
            pltpu.VMEM((nz, 2, 2, rows, columns), bf16),
            pltpu.VMEM((nz, 2, 2, rows, columns), bf16),
            pltpu.VMEM((nz, 3, rows, columns), bf16),
            pltpu.VMEM((6, rows, columns), bf16),
            pltpu.VMEM((6, 2, 2, rows, lane), bf16),
            pltpu.VMEM((rows, columns), f32),
            pltpu.VMEM((rows, 1), f32),
            pltpu.VMEM((1, stat), f32),
            pltpu.VMEM((nx * 2, 1, stat), f32),
            pltpu.VMEM((1, stat), f32),
            pltpu.VMEM((nz, 1, stat), f32),
            pltpu.VMEM((rows, columns), bf16),
            pltpu.VMEM((1, rows), f32),
            pltpu.VMEM((1, columns), f32),
            dma((nz,)), dma((3,)), one, dma((4,)), dma((nz,)), dma((2,)), dma((nz,)), dma((nz,)),
            one, dma((6,)), one, dma((6,)), one, one, one, one,
            one, dma((nz,)), dma((2,)), dma((nz,)), dma((nz,)), dma((nz,)), one, dma((nz,)), one, one,
        ],
        compiler_params=pltpu.CompilerParams(
            collective_id=0, has_side_effects=True, vmem_limit_bytes=VMEM_BYTES - held),
    )(grad_bucket.reshape(2, 2, nz, 2, rows, columns), parameters[0], row_state, column_state)
    new, row, col, full = pl.pallas_call(
        functools.partial(write_out, nz),
        out_shape=tuple(jax.ShapeDtypeStruct(*shape) for shape in shapes),
        in_specs=[vmem] * 4,
        out_specs=(hbm,) * 4,
        scratch_shapes=[dma((4,))],
        compiler_params=pltpu.CompilerParams(vmem_limit_bytes=4 * 1024 * 1024),
    )(*[pltpu.with_memory_space_constraint(result, pltpu.VMEM) for result in results])
    return (new[None], row, col, full.reshape(full_width, columns))


def solution(mesh):
    nx, nz, ny = (mesh.shape[a] for a in AXES)
    in_specs = (
        P(AXES, None, None, None),
        P(None, AXES, None),
        P(None, AXES),
        P(),
    )
    out_specs = (P(None, AXES, None), P(None, AXES), P(), P())
    fits = nx == 4 and ny == 2 and nz == 4

    def body(grad_bucket, parameters, row_state, column_state):
        if fits and grad_bucket.shape[1] == 1 and parameters.shape[1] % TILE == 0 and grad_bucket.shape[3] % 1024 == 0:
            return fused(nx, nz, grad_bucket, parameters, row_state, column_state)
        return shards(grad_bucket, parameters, row_state, column_state)

    return jax.shard_map(body, mesh=mesh, in_specs=in_specs, out_specs=out_specs, check_vma=False)
```

```python
import functools
import math

import jax
import jax.numpy as jnp
from jax import lax
from jax.experimental import pallas as pl
from jax.experimental.pallas import tpu as pltpu
from jax.sharding import PartitionSpec as P

beta_two = 0.8
step_size = 0.5
AXES = ("gx", "gy", "gz")
TILE = 16
VMEM_BYTES = 67043328 - 131072


def shards(grad_bucket, parameters, row_state, column_state):
    local_grad = grad_bucket[0].astype(jnp.float32)
    layer_count, full_width, columns = local_grad.shape
    summed = lax.psum_scatter(local_grad, AXES, scatter_dimension=1, tiled=True)
    clip_level = 0.5 * math.sqrt(layer_count * full_width * columns)
    squares = summed * summed
    norm_square = lax.psum(jnp.sum(squares), AXES)
    factor = jnp.minimum(jnp.float32(1.0), clip_level / jnp.sqrt(norm_square + 1e-06))
    clipped = factor * summed
    clipped_square = clipped * clipped
    row_next = beta_two * row_state + (1.0 - beta_two) * jnp.mean(clipped_square, axis=2)
    column_part, row_total = lax.psum((jnp.sum(clipped_square, axis=1), jnp.sum(row_next, axis=1)), AXES)
    column_next = beta_two * column_state + (1.0 - beta_two) * column_part / full_width
    row_average = row_total / full_width
    second = row_next[:, :, None] * column_next[:, None, :] / row_average[:, None, None]
    update = clipped / jnp.sqrt(second)
    new_parameters = (parameters.astype(jnp.float32) - step_size * update).astype(jnp.bfloat16)
    first_layer = lax.all_gather(new_parameters[0], AXES, axis=0, tiled=True)
    return (new_parameters, row_next, column_next, first_layer)


def flip(index, mask, size):
    out, bit = 0, 1
    while bit < size:
        out = out + bit * (((index // bit) % 2 + (mask // bit) % 2) % 2)
        bit *= 2
    return out


def kernel(nx, nz, grad, params_in, row_in, col_in, new_ref, row_ref, col_ref, full,
           lg, cr, rx, rz, rc, unit, summed, own, st, st1, tot, st2, params, row_state, col_state,
           lsem, isem, cs, cfr, cvr, fs, fr, hr, zs, zr, ks, kr, s1s, s1r, s2s, s2r,
           gzs, gzr, qs, q1r, q2r, q3r, gks, gkr, gcs, gcr):
    gx, z, y = lax.axis_index("gx"), lax.axis_index("gy"), lax.axis_index("gz")
    x, c = gx // 2, gx % 2
    rows, columns = params.shape
    lane = columns // 8
    stat_width = st.shape[1]
    full_width = rows * 4 * nz * 2
    core_peer = (x * 2 + 1 - c, z, y)
    x_peer = ((1 - x) * 2 + c, z, y)
    y_peer = (gx, z, 1 - y)
    tiles = rows // TILE
    f32, bf16 = jnp.float32, jnp.bfloat16
    scope = jax.named_scope
    blocks = [(1 - x, 1 - y), (1 - x, y), (x, 1 - y), (x, y)]

    cut_row = (tiles * 4 + 3) // 7
    parts = [(0, cut_row, 0, 6), (cut_row, tiles, 0, 7)]
    strips = [(0, cut_row, 6, 8), (cut_row, tiles, 7, 8)]
    halves = [(0, tiles, 0, 4), (0, tiles, 4, 8)]

    def area(regions):
        return sum((b - a) * (e - d) for a, b, d, e in regions)

    def at(region, shift=0):
        a, b, d, e = region
        return pl.ds(a * TILE, (b - a) * TILE), pl.ds((d - shift) * lane, (e - d) * lane)

    def spans(t):
        return halves if t == 0 else parts[::-1] if t % 2 else parts

    def zof(t):
        return flip(z, t, nz)

    inside = (z + z // 2) % 2
    near, middle = (gx, zof(1), y), (gx, zof(3), y)
    origin = [z, zof(1), flip(z, 2 + inside, nz), flip(z, 3 - inside, nz)]

    def on_end(step):
        pl.when(inside == 0)(step)

    def on_inner(step):
        pl.when(inside == 1)(step)

    def rdma(src, dst, ssem, rsem, peer):
        return pltpu.make_async_remote_copy(
            src_ref=src, dst_ref=dst, send_sem=ssem, recv_sem=rsem,
            device_id=peer, device_id_type=pl.DeviceIdType.MESH)

    def take_recv(view, sem):
        rdma(view, view, sem, sem, core_peer).wait_recv()

    def take_send(view, sem):
        rdma(view, view, sem, sem, core_peer).wait_send()

    def some(count):
        return unit.at[pl.ds(0, count)]

    first = 3
    loads = {t: pltpu.make_async_copy(grad.at[:, c, zof(t)], lg.at[t], lsem.at[t]) for t in (3, 2, 1, 0)}
    for t in loads:
        loads[t].start()
    small = [pltpu.make_async_copy(src, dst, isem.at[k]) for k, (src, dst) in enumerate(
        [(params_in, params), (row_in, row_state), (col_in, col_state)])]
    for copy in small:
        copy.start()

    barrier = pltpu.get_barrier_semaphore()
    plane = [((gx + a) % nx, z, (y + b) % 2) for a in range(nx) for b in range(2) if (a, b) != (0, 0)]
    line = [(gx, zof(t), y) for t in range(1, nz)]
    for peer in line + plane:
        pl.semaphore_signal(barrier, inc=1, device_id=peer, device_id_type=pl.DeviceIdType.MESH)
    with scope("barrier"):
        pl.semaphore_wait(barrier, len(plane) + len(line))

    for k, (bx, by) in enumerate(blocks):
        rdma(grad.at[bx, 1 - c, zof(first), by], cr.at[first, bx, by], cs, cfr.at[k], core_peer).start()
    for t in (2, 1, 0):
        rdma(grad.at[:, 1 - c, zof(t)], cr.at[t], cs, cvr.at[t], core_peer).start()

    def add(*terms):
        total = terms[0].astype(f32)
        for term in terms[1:]:
            total = total + term.astype(f32)
        return total

    def over(region, step, shift=0):
        a, b, d, e = region

        @pl.loop(a, b, unroll=True)
        def _(i):
            step(pl.ds(pl.multiple_of(i * TILE, TILE), TILE), pl.ds(d * lane, (e - d) * lane),
                 pl.ds((d - shift) * lane, (e - d) * lane))

    whole = (0, tiles, 0, 8)

    def pair_sum(t, bx, by):
        def step(r, l, _):
            lg[t, bx, by, r, l] = add(lg[t, bx, by, r, l], cr[t, bx, by, r, l]).astype(bf16)
        over(whole, step)

    def cross(t):
        return fs.at[1 if t else 0]

    def send(t, bx, by, slot, region, sem, peer):
        r, l = at(region)
        rdma(lg.at[t, bx, by, r, l], rx.at[t, slot, r, l], cross(t), sem.at[t], peer).start()

    def send_f(t):
        a, b = spans(t)
        send(t, 1 - x, 1 - y, 0, a, fr, x_peer)
        send(t, 1 - x, 1 - y, 0, b, fr, y_peer)

    def send_ga(t):
        send(t, 1 - x, y, 1, spans(t)[0], hr, x_peer)

    def send_gb(t):
        send(t, x, 1 - y, 1, spans(t)[1], hr, y_peer)

    def send_g(t):
        send_ga(t)
        send_gb(t)

    def send_strip(t, slot, peer):
        for region in strips:
            r, l = at(region)
            _, m = at(region, 6)
            rdma(lg.at[t, :, :, r, l], rc.at[slot, :, :, r, m], ks, kr.at[slot], peer).start()

    def take_strips(*slots):
        for slot in slots:
            with scope(f"line{slot}"):
                take_recv(some(4 * area(strips)), kr.at[slot])

    def strip_add(t, *slots):
        for bx in range(2):
            for by in range(2):
                def step(r, l, m):
                    lg[t, bx, by, r, l] = add(
                        lg[t, bx, by, r, l], *[rc[slot, bx, by, r, m] for slot in slots]).astype(bf16)
                for region in strips:
                    over(region, step, 6)

    def stage_pair(t):
        with scope(f"pair{t}"):
            take_recv(cr.at[t], cvr.at[t])
            loads[t].wait()
            for bx, by in blocks:
                pair_sum(t, bx, by)

    def stage_first(t):
        a, b = spans(t)
        with scope(f"f{t}"):
            take_recv(some(area(spans(t))), fr.at[t])

        def step_a(r, l, _):
            lg[t, x, 1 - y, r, l] = add(lg[t, x, 1 - y, r, l], rx[t, 0, r, l]).astype(bf16)

        def step_b(r, l, _):
            lg[t, 1 - x, y, r, l] = add(lg[t, 1 - x, y, r, l], rx[t, 0, r, l]).astype(bf16)
        over(a, step_a)
        send(t, x, 1 - y, 2, a, hr, y_peer)
        over(b, step_b)
        send(t, 1 - x, y, 2, b, hr, x_peer)

    def stage_second(t):
        with scope(f"h{t}"):
            take_recv(some(2 * area(spans(t))), hr.at[t])

    def send_far(t, slot, peer, p):
        r, l = at(parts[p])
        rdma(lg.at[t, x, y, r, l], rz.at[slot, r, l], zs, zr.at[slot, p], peer).start()

    def take_far(slot, p):
        with scope(f"far{slot}_{p}"):
            take_recv(some(area(parts[p:p + 1])), zr.at[slot, p])

    def second_add(t, p, *slots):
        def step(r, l, _):
            lg[t, x, y, r, l] = add(lg[t, x, y, r, l], rx[t, 1, r, l], rx[t, 2, r, l],
                                    *[rz[slot, r, l] for slot in slots]).astype(bf16)
        over(parts[p], step)

    loads[first].wait()
    for k, (bx, by) in enumerate(blocks):
        with scope(f"core{k}"):
            take_recv(cr.at[first, bx, by], cfr.at[k])
        pair_sum(first, bx, by)
        if k == 0:
            send_f(first)
        elif k == 1:
            send_ga(first)
        elif k == 2:
            send_gb(first)
    on_end(lambda: send_strip(3, 3, near))
    stage_pair(2)
    on_end(lambda: send_strip(2, 2, near))
    send_f(2)
    stage_first(3)
    send_g(2)
    stage_pair(1)
    on_end(lambda: send_strip(1, 1, near))
    send_f(1)
    stage_pair(0)

    @on_end
    def _():
        rz[5] = jnp.zeros((rows, columns), bf16)

    @on_inner
    def _():
        take_strips(3)
        strip_add(2, 3)
        send_strip(2, 4, middle)

    stage_first(2)
    send_g(1)

    @on_inner
    def _():
        take_strips(2)
        strip_add(3, 2)
        send_strip(3, 5, middle)

    stage_second(3)
    for p in range(2):
        second_add(3, p)
        on_end(lambda: send_far(3, 3, near, p))

    @on_inner
    def _():
        take_strips(4)
        strip_add(1, 4)
        send_strip(1, 0, near)

    stage_first(1)

    @on_end
    def _():
        take_strips(0)
        strip_add(0, 0)

    @on_inner
    def _():
        take_strips(1, 5)
        strip_add(0, 1, 5)

    send_f(0)
    send_g(0)
    stage_second(2)

    @on_end
    def _():
        for p in range(2):
            second_add(2, p)
            send_far(2, 2, near, p)

    @on_inner
    def _():
        for p in range(2):
            take_far(3, p)
            second_add(2, p, 3)
            send_far(2, 4, middle, p)

    def pass_far_sum(p):
        take_far(2, p)

        def step(r, l, _):
            lg[3, x, y, r, l] = add(lg[3, x, y, r, l], rz[2, r, l]).astype(bf16)
        over(parts[p], step)
        send_far(3, 5, middle, p)

    on_inner(lambda: pass_far_sum(0))
    stage_second(1)

    @on_end
    def _():
        for p in range(2):
            second_add(1, p)
            send_far(1, 1, near, p)

    @on_inner
    def _():
        pass_far_sum(1)
        for p in range(2):
            take_far(4, p)
            second_add(1, p, 4)
            send_far(1, 1, near, p)

    stage_first(0)
    for copy in small:
        copy.wait()
    st[:, columns:] = jnp.broadcast_to(jnp.sum(row_state[...], axis=1, keepdims=True), (1, stat_width - columns))
    stage_second(0)
    for p in range(2):
        take_far(1, p)

    @on_inner
    def _():
        for p in range(2):
            take_far(5, p)

    with scope("final"):
        cuts = [(0, 6), (6, 7), (7, 8)]
        sums = [None] * len(cuts)
        for i in range(tiles):
            r = pl.ds(i * TILE, TILE)
            row_sum = 0.0
            for k, (d, e) in enumerate(cuts):
                l = pl.ds(d * lane, (e - d) * lane)
                terms = [lg[0, x, y, r, l], rx[0, 1, r, l], rx[0, 2, r, l]]
                if e <= parts[0 if i < cut_row else 1][3]:
                    terms += [rz[1, r, l], rz[5, r, l]]
                value = add(*terms)
                summed[r, l] = value
                value = value * value
                row_sum = row_sum + jnp.sum(value, axis=1, keepdims=True)
                sums[k] = value if sums[k] is None else sums[k] + value
            own[r, :] = row_sum
        for (d, e), value in zip(cuts, sums):
            st[:, pl.ds(d * lane, (e - d) * lane)] = jnp.sum(value, axis=0, keepdims=True)

    me = gx * 2 + y
    for peer in plane:
        rdma(st, st1.at[me], s1s, s1r, peer).start()
    st1[me] = st[...]
    take_send(cr, cs)
    take_send(some(3 * area(halves)), fs.at[0])
    take_send(some(9 * area(parts)), fs.at[1])
    take_send(some(3 * area(parts)), zs)
    take_send(some(12 * area(strips)), ks)
    diagonal = lax.broadcasted_iota(jnp.int32, (rows, rows), 0) == lax.broadcasted_iota(jnp.int32, (rows, rows), 1)
    state_down = jnp.sum(jnp.where(diagonal, jnp.broadcast_to(row_state[...], (rows, rows)), 0.0), axis=1, keepdims=True)
    with scope("stat1"):
        take_recv(st1.at[0:nx * 2 - 1], s1r)
    total = st1[0]
    for k in range(1, nx * 2):
        total = total + st1[k]
    tot[...] = total
    for t in range(1, nz):
        rdma(tot, st2.at[z], s2s, s2r, (gx, zof(t), y)).start()
    st2[z] = total
    with scope("stat2"):
        take_recv(st2.at[0:nz - 1], s2r)
    total = st2[0]
    for k in range(1, nz):
        total = total + st2[k]
    column_sum = total[:, 0:columns]
    norm_square = jnp.sum(column_sum, axis=1, keepdims=True)
    state_sum = total[:, columns:columns + 1]
    clip_level = 0.5 * math.sqrt(full_width * columns)
    factor = jnp.minimum(jnp.float32(1.0), clip_level / jnp.sqrt(norm_square + 1e-06))
    square_factor = factor * factor
    column_next = beta_two * col_state[...] + (1.0 - beta_two) * (square_factor * column_sum / full_width)
    row_average = (beta_two * state_sum + (1.0 - beta_two) * (square_factor * norm_square / columns)) / full_width
    row_next = beta_two * state_down + (1.0 - beta_two) * (square_factor * own[...] / columns)
    own[...] = (step_size * factor) / jnp.sqrt(row_next / row_average)
    col_scale = 1.0 / jnp.sqrt(column_next)

    def update(r, l, _):
        new = params[r, l].astype(f32) - (summed[r, l] * own[r, :]) * col_scale
        full[x, c, z, y, r, l] = new.astype(bf16)
    with scope("update"):
        over(whole, update)

    def same(view, ssem, rsem, peer):
        rdma(view, view, ssem, rsem, peer).start()

    def moves(t):
        return qs.at[1 if t else 0]

    def piece(bx, u, by, region):
        r, l = at(region)
        return full.at[bx, c, u, by, r, l]

    def pass_core(t, bx, by):
        for region in parts if t else [whole]:
            same(piece(bx, origin[t], by, region), gcs, gcr, core_peer)

    def send_q1(t):
        u, (a, b) = origin[t], spans(t)
        same(piece(x, u, y, a), moves(t), q1r.at[t], y_peer)
        same(piece(x, u, y, b), moves(t), q1r.at[t], x_peer)

    def send_q2(t):
        u, (a, b) = origin[t], spans(t)
        same(piece(x, u, y, a), moves(t), q2r.at[t], x_peer)
        same(piece(x, u, y, b), moves(t), q2r.at[t], y_peer)
        pass_core(t, x, y)

    def send_own(t):
        send_q1(t)
        send_q2(t)

    def pass_far(t, slot, peer):
        for region in parts:
            same(piece(x, origin[t], y, region), gzs, gzr.at[slot], peer)

    def take_z(t):
        with scope(f"gz{t}"):
            take_recv(some(area(parts)), gzr.at[t])

    def gather_cross(t):
        u, (a, b) = origin[t], spans(t)
        with scope(f"q1_{t}"):
            take_recv(some(area(spans(t))), q1r.at[t])
        same(piece(x, u, 1 - y, a), moves(t), q3r.at[t], x_peer)
        same(piece(1 - x, u, y, b), moves(t), q3r.at[t], y_peer)

    def gather_side(t):
        with scope(f"q2_{t}"):
            take_recv(some(area(spans(t))), q2r.at[t])
        pass_core(t, 1 - x, y)
        pass_core(t, x, 1 - y)

    def gather_far(t):
        with scope(f"q3_{t}"):
            take_recv(some(area(spans(t))), q3r.at[t])
        pass_core(t, 1 - x, 1 - y)

    def each_strip(t, ssem, rsem, peer):
        for region in strips:
            r, l = at(region)
            same(full.at[:, c, origin[t], :, r, l], ssem, rsem, peer)

    def pass_strip(t, slot, peer):
        each_strip(t, gks, gkr.at[slot], peer)

    def take_strip(t):
        with scope(f"strip{t}"):
            take_recv(some(4 * area(strips)), gkr.at[t])
        each_strip(t, gcs, gcr, core_peer)

    pass_far(0, 1, near)
    send_q1(0)
    on_inner(lambda: pass_far(0, 2, middle))
    send_q2(0)
    new_ref[...] = full[x, c, z, y]
    col_ref[...] = column_next
    row_ref[...] = jnp.sum(jnp.where(diagonal, jnp.broadcast_to(row_next, (rows, rows)), 0.0), axis=0, keepdims=True)
    gather_cross(0)
    take_z(1)
    on_inner(lambda: pass_far(1, 3, middle))
    send_own(1)

    @on_inner
    def _():
        take_z(2)
        pass_far(2, 2, near)

    gather_side(0)
    gather_far(0)
    pass_strip(0, 1, near)
    on_inner(lambda: pass_strip(0, 2, middle))
    gather_cross(1)
    on_end(lambda: take_z(2))
    send_own(2)

    @on_inner
    def _():
        take_z(3)
        pass_far(3, 3, near)

    gather_side(1)
    gather_far(1)
    take_strip(1)
    on_inner(lambda: pass_strip(1, 3, middle))
    gather_cross(2)
    on_end(lambda: take_z(3))
    send_own(3)

    @on_inner
    def _():
        take_strip(2)
        pass_strip(2, 2, near)

    gather_side(2)
    gather_far(2)

    @on_inner
    def _():
        take_strip(3)
        pass_strip(3, 3, near)

    on_end(lambda: take_strip(2))
    gather_cross(3)
    gather_side(3)
    gather_far(3)
    on_end(lambda: take_strip(3))

    with scope("finish"):
        take_send(st1.at[0:nx * 2 - 1], s1s)
        take_send(st2.at[0:nz - 1], s2s)
        take_send(some(3 * area(halves)), qs.at[0])
        take_send(some(9 * area(parts)), qs.at[1])

        @on_end
        def _():
            take_send(some(area(parts)), gzs)
            take_send(some(4 * area(strips)), gks)

        @on_inner
        def _():
            take_send(some(5 * area(parts)), gzs)
            take_send(some(20 * area(strips)), gks)

        take_send(full.at[:, c], gcs)
        take_recv(full.at[:, c], gcr)


def write_out(nz, new, row, col, full, new_out, row_out, col_out, full_out, sem):
    pieces = [(full.at[a, b, u], full_out.at[a, b, u]) for a in range(2) for b in range(2) for u in range(nz)]
    copies = [pltpu.make_async_copy(src, dst, sem.at[0]) for src, dst in pieces]
    small = [pltpu.make_async_copy(src, dst, sem.at[k + 1])
             for k, (src, dst) in enumerate([(new, new_out), (row, row_out), (col, col_out)])]
    for copy in copies + small:
        copy.start()
    for copy in small:
        copy.wait()
    pltpu.make_async_copy(full, full_out, sem.at[0]).wait()


def fused(nx, nz, grad_bucket, parameters, row_state, column_state):
    _, _, full_width, columns = grad_bucket.shape
    rows = parameters.shape[1]
    lane = columns // 8
    bf16, f32 = jnp.bfloat16, jnp.float32
    vmem = pl.BlockSpec(memory_space=pltpu.VMEM)
    hbm = pl.BlockSpec(memory_space=pltpu.HBM)
    dma = pltpu.SemaphoreType.DMA
    one = dma(())
    shapes = [((rows, columns), bf16), ((1, rows), f32), ((1, columns), f32), ((2, 2, nz, 2, rows, columns), bf16)]
    held = 2 * columns * (rows + full_width) + 4 * (columns + -(-rows // 128) * 128)
    stat = columns + 128
    results = pl.pallas_call(
        functools.partial(kernel, nx, nz),
        out_shape=tuple(pltpu.VMEM(*shape) for shape in shapes),
        in_specs=[hbm] * 4,
        out_specs=(vmem,) * 4,
        scratch_shapes=[
            pltpu.VMEM((nz, 2, 2, rows, columns), bf16),
            pltpu.VMEM((nz, 2, 2, rows, columns), bf16),
            pltpu.VMEM((nz, 3, rows, columns), bf16),
            pltpu.VMEM((6, rows, columns), bf16),
            pltpu.VMEM((6, 2, 2, rows, 2 * lane), bf16),
            pltpu.VMEM((9 * 8 * (rows // TILE), TILE, lane), bf16),
            pltpu.VMEM((rows, columns), f32),
            pltpu.VMEM((rows, 1), f32),
            pltpu.VMEM((1, stat), f32),
            pltpu.VMEM((nx * 2, 1, stat), f32),
            pltpu.VMEM((1, stat), f32),
            pltpu.VMEM((nz, 1, stat), f32),
            pltpu.VMEM((rows, columns), bf16),
            pltpu.VMEM((1, rows), f32),
            pltpu.VMEM((1, columns), f32),
            dma((nz,)), dma((3,)), one, dma((4,)), dma((nz,)), dma((2,)), dma((nz,)), dma((nz,)),
            one, dma((6, 2)), one, dma((6,)), one, one, one, one,
            one, dma((nz,)), dma((2,)), dma((nz,)), dma((nz,)), dma((nz,)), one, dma((nz,)), one, one,
        ],
        compiler_params=pltpu.CompilerParams(
            collective_id=0, has_side_effects=True, vmem_limit_bytes=VMEM_BYTES - held),
    )(grad_bucket.reshape(2, 2, nz, 2, rows, columns), parameters[0], row_state, column_state)
    new, row, col, full = pl.pallas_call(
        functools.partial(write_out, nz),
        out_shape=tuple(jax.ShapeDtypeStruct(*shape) for shape in shapes),
        in_specs=[vmem] * 4,
        out_specs=(hbm,) * 4,
        scratch_shapes=[dma((4,))],
        compiler_params=pltpu.CompilerParams(vmem_limit_bytes=4 * 1024 * 1024),
    )(*[pltpu.with_memory_space_constraint(result, pltpu.VMEM) for result in results])
    return (new[None], row, col, full.reshape(full_width, columns))


def solution(mesh):
    nx, nz, ny = (mesh.shape[a] for a in AXES)
    in_specs = (
        P(AXES, None, None, None),
        P(None, AXES, None),
        P(None, AXES),
        P(),
    )
    out_specs = (P(None, AXES, None), P(None, AXES), P(), P())
    fits = nx == 4 and ny == 2 and nz == 4

    def body(grad_bucket, parameters, row_state, column_state):
        if fits and grad_bucket.shape[1] == 1 and parameters.shape[1] % TILE == 0 and parameters.shape[1] >= 2 * TILE and grad_bucket.shape[3] % 1024 == 0:
            return fused(nx, nz, grad_bucket, parameters, row_state, column_state)
        return shards(grad_bucket, parameters, row_state, column_state)

    return jax.shard_map(body, mesh=mesh, in_specs=in_specs, out_specs=out_specs, check_vma=False)
```

```python
import functools
import math

import jax
import jax.numpy as jnp
from jax import lax
from jax.experimental import pallas as pl
from jax.experimental.pallas import tpu as pltpu
from jax.sharding import PartitionSpec as P

beta_two = 0.8
step_size = 0.5
AXES = ("gx", "gy", "gz")
TILE = 16
VMEM_BYTES = 67043328 - 131072


def shards(grad_bucket, parameters, row_state, column_state):
    local_grad = grad_bucket[0].astype(jnp.float32)
    layer_count, full_width, columns = local_grad.shape
    summed = lax.psum_scatter(local_grad, AXES, scatter_dimension=1, tiled=True)
    clip_level = 0.5 * math.sqrt(layer_count * full_width * columns)
    squares = summed * summed
    norm_square = lax.psum(jnp.sum(squares), AXES)
    factor = jnp.minimum(jnp.float32(1.0), clip_level / jnp.sqrt(norm_square + 1e-06))
    clipped = factor * summed
    clipped_square = clipped * clipped
    row_next = beta_two * row_state + (1.0 - beta_two) * jnp.mean(clipped_square, axis=2)
    column_part, row_total = lax.psum((jnp.sum(clipped_square, axis=1), jnp.sum(row_next, axis=1)), AXES)
    column_next = beta_two * column_state + (1.0 - beta_two) * column_part / full_width
    row_average = row_total / full_width
    second = row_next[:, :, None] * column_next[:, None, :] / row_average[:, None, None]
    update = clipped / jnp.sqrt(second)
    new_parameters = (parameters.astype(jnp.float32) - step_size * update).astype(jnp.bfloat16)
    first_layer = lax.all_gather(new_parameters[0], AXES, axis=0, tiled=True)
    return (new_parameters, row_next, column_next, first_layer)


def flip(index, mask, size):
    out, bit = 0, 1
    while bit < size:
        out = out + bit * (((index // bit) % 2 + (mask // bit) % 2) % 2)
        bit *= 2
    return out


def kernel(nx, nz, grad, params_in, row_in, col_in, new_ref, row_ref, col_ref, full,
           lg, cr, rx, rz, rc, unit, summed, own, st, st1, tot, st2, params, row_state, col_state,
           lsem, isem, cs, cfr, cvr, fs, fr, hr, zs, zr, ks, kr, s1s, s1r, s2s, s2r,
           gzs, gzr, qs, q1r, q2r, q3r, gks, gkr, gcs, gcr):
    gx, z, y = lax.axis_index("gx"), lax.axis_index("gy"), lax.axis_index("gz")
    x, c = gx // 2, gx % 2
    rows, columns = params.shape
    lane = columns // 8
    stat_width = st.shape[1]
    full_width = rows * 4 * nz * 2
    core_peer = (x * 2 + 1 - c, z, y)
    x_peer = ((1 - x) * 2 + c, z, y)
    y_peer = (gx, z, 1 - y)
    tiles = rows // TILE
    f32, bf16 = jnp.float32, jnp.bfloat16
    scope = jax.named_scope
    blocks = [(1 - x, 1 - y), (1 - x, y), (x, 1 - y), (x, y)]

    cut_row = (tiles * 4 + 3) // 7
    parts = [(0, cut_row, 0, 6), (cut_row, tiles, 0, 7)]
    strips = [(0, cut_row, 6, 8), (cut_row, tiles, 7, 8)]
    halves = [(0, tiles, 0, 4), (0, tiles, 4, 8)]

    def area(regions):
        return sum((b - a) * (e - d) for a, b, d, e in regions)

    def at(region, shift=0):
        a, b, d, e = region
        return pl.ds(a * TILE, (b - a) * TILE), pl.ds((d - shift) * lane, (e - d) * lane)

    def spans(t):
        return halves if t == 0 else parts[::-1] if t % 2 else parts

    def zof(t):
        return flip(z, t, nz)

    inside = (z + z // 2) % 2
    near, middle = (gx, zof(1), y), (gx, zof(3), y)
    origin = [z, zof(1), flip(z, 2 + inside, nz), flip(z, 3 - inside, nz)]

    def on_end(step):
        pl.when(inside == 0)(step)

    def on_inner(step):
        pl.when(inside == 1)(step)

    def rdma(src, dst, ssem, rsem, peer):
        return pltpu.make_async_remote_copy(
            src_ref=src, dst_ref=dst, send_sem=ssem, recv_sem=rsem,
            device_id=peer, device_id_type=pl.DeviceIdType.MESH)

    def take_recv(view, sem):
        rdma(view, view, sem, sem, core_peer).wait_recv()

    def take_send(view, sem):
        rdma(view, view, sem, sem, core_peer).wait_send()

    def some(count):
        return unit.at[pl.ds(0, count)]

    first = 3
    loads = {t: pltpu.make_async_copy(grad.at[:, c, zof(t)], lg.at[t], lsem.at[t]) for t in (3, 2, 1, 0)}
    for t in loads:
        loads[t].start()
    small = [pltpu.make_async_copy(src, dst, isem.at[k]) for k, (src, dst) in enumerate(
        [(params_in, params), (row_in, row_state), (col_in, col_state)])]
    for copy in small:
        copy.start()

    barrier = pltpu.get_barrier_semaphore()
    plane = [((gx + a) % nx, z, (y + b) % 2) for a in range(nx) for b in range(2) if (a, b) != (0, 0)]
    line = [(gx, zof(t), y) for t in range(1, nz)]
    for peer in line + plane:
        pl.semaphore_signal(barrier, inc=1, device_id=peer, device_id_type=pl.DeviceIdType.MESH)
    with scope("barrier"):
        pl.semaphore_wait(barrier, len(plane) + len(line))

    for k, (bx, by) in enumerate(blocks):
        rdma(grad.at[bx, 1 - c, zof(first), by], cr.at[first, bx, by], cs, cfr.at[k], core_peer).start()
    for t in (2, 1, 0):
        rdma(grad.at[:, 1 - c, zof(t)], cr.at[t], cs, cvr.at[t], core_peer).start()

    def add(*terms):
        total = terms[0].astype(f32)
        for term in terms[1:]:
            total = total + term.astype(f32)
        return total

    def over(region, step, shift=0):
        a, b, d, e = region

        @pl.loop(a, b, unroll=True)
        def _(i):
            step(pl.ds(pl.multiple_of(i * TILE, TILE), TILE), pl.ds(d * lane, (e - d) * lane),
                 pl.ds((d - shift) * lane, (e - d) * lane))

    whole = (0, tiles, 0, 8)

    def pair_sum(t, bx, by):
        def step(r, l, _):
            lg[t, bx, by, r, l] = add(lg[t, bx, by, r, l], cr[t, bx, by, r, l]).astype(bf16)
        over(whole, step)

    def cross(t):
        return fs.at[1 if t else 0]

    def send(t, bx, by, slot, region, sem, peer):
        r, l = at(region)
        rdma(lg.at[t, bx, by, r, l], rx.at[t, slot, r, l], cross(t), sem.at[t], peer).start()

    def send_f(t):
        a, b = spans(t)
        send(t, 1 - x, 1 - y, 0, a, fr, x_peer)
        send(t, 1 - x, 1 - y, 0, b, fr, y_peer)

    def send_ga(t):
        send(t, 1 - x, y, 1, spans(t)[0], hr, x_peer)

    def send_gb(t):
        send(t, x, 1 - y, 1, spans(t)[1], hr, y_peer)

    def send_g(t):
        send_ga(t)
        send_gb(t)

    side = [1 - x, x]

    def send_strip(t, slot, peer, h):
        for region in strips:
            r, l = at(region)
            _, m = at(region, 6)
            rdma(lg.at[t, side[h], :, r, l], rc.at[slot, h, :, r, m], ks, kr.at[slot, h], peer).start()

    def send_strips(t, slot, peer):
        for h in range(2):
            send_strip(t, slot, peer, h)

    def take_strips(h, *slots):
        for slot in slots:
            with scope(f"line{slot}_{h}"):
                take_recv(some(2 * area(strips)), kr.at[slot, h])

    def strip_add(t, h, *slots):
        for by in range(2):
            def step(r, l, m):
                lg[t, side[h], by, r, l] = add(
                    lg[t, side[h], by, r, l], *[rc[slot, h, by, r, m] for slot in slots]).astype(bf16)
            for region in strips:
                over(region, step, 6)

    def relay(came, t, slot, peer):
        for h in range(2):
            take_strips(h, came)
            strip_add(t, h, came)
            send_strip(t, slot, peer, h)

    def stage_pair(t):
        with scope(f"pair{t}"):
            take_recv(cr.at[t], cvr.at[t])
            loads[t].wait()
            for bx, by in blocks:
                pair_sum(t, bx, by)

    def stage_first(t):
        a, b = spans(t)
        with scope(f"f{t}"):
            take_recv(some(area(spans(t))), fr.at[t])

        def step_a(r, l, _):
            lg[t, x, 1 - y, r, l] = add(lg[t, x, 1 - y, r, l], rx[t, 0, r, l]).astype(bf16)

        def step_b(r, l, _):
            lg[t, 1 - x, y, r, l] = add(lg[t, 1 - x, y, r, l], rx[t, 0, r, l]).astype(bf16)
        over(a, step_a)
        send(t, x, 1 - y, 2, a, hr, y_peer)
        over(b, step_b)
        send(t, 1 - x, y, 2, b, hr, x_peer)

    def stage_second(t):
        with scope(f"h{t}"):
            take_recv(some(2 * area(spans(t))), hr.at[t])

    def send_far(t, slot, peer, p):
        r, l = at(parts[p])
        rdma(lg.at[t, x, y, r, l], rz.at[slot, r, l], zs, zr.at[slot, p], peer).start()

    def take_far(slot, p):
        with scope(f"far{slot}_{p}"):
            take_recv(some(area(parts[p:p + 1])), zr.at[slot, p])

    def second_add(t, p, *slots):
        def step(r, l, _):
            lg[t, x, y, r, l] = add(lg[t, x, y, r, l], rx[t, 1, r, l], rx[t, 2, r, l],
                                    *[rz[slot, r, l] for slot in slots]).astype(bf16)
        over(parts[p], step)

    loads[first].wait()
    for k, (bx, by) in enumerate(blocks):
        with scope(f"core{k}"):
            take_recv(cr.at[first, bx, by], cfr.at[k])
        pair_sum(first, bx, by)
        if k == 0:
            send_f(first)
        elif k == 1:
            send_ga(first)
            on_end(lambda: send_strip(3, 3, near, 0))
        elif k == 2:
            send_gb(first)
        else:
            on_end(lambda: send_strip(3, 3, near, 1))
    stage_pair(2)
    on_end(lambda: send_strips(2, 2, near))
    send_f(2)
    stage_first(3)
    send_g(2)
    stage_pair(1)
    on_end(lambda: send_strips(1, 1, near))
    send_f(1)
    on_inner(lambda: relay(3, 2, 4, middle))
    stage_pair(0)

    @on_end
    def _():
        rz[5] = jnp.zeros((rows, columns), bf16)

    stage_first(2)
    send_g(1)
    on_inner(lambda: relay(2, 3, 5, middle))
    stage_second(3)
    for p in range(2):
        second_add(3, p)
        on_end(lambda: send_far(3, 3, near, p))
    on_inner(lambda: relay(4, 1, 0, near))
    stage_first(1)

    @on_end
    def _():
        stage_second(2)
        for p in range(2):
            second_add(2, p)
            send_far(2, 2, near, p)
        for h in range(2):
            take_strips(h, 0)
            strip_add(0, h, 0)

    @on_inner
    def _():
        for h in range(2):
            take_strips(h, 1, 5)
            strip_add(0, h, 1, 5)

    send_f(0)
    send_g(0)

    @on_inner
    def _():
        stage_second(2)
        for p in range(2):
            take_far(3, p)
            second_add(2, p, 3)
            send_far(2, 4, middle, p)

    def pass_far_sum(p):
        take_far(2, p)

        def step(r, l, _):
            lg[3, x, y, r, l] = add(lg[3, x, y, r, l], rz[2, r, l]).astype(bf16)
        over(parts[p], step)
        send_far(3, 5, middle, p)

    stage_second(1)

    @on_end
    def _():
        for p in range(2):
            second_add(1, p)
            send_far(1, 1, near, p)

    def pass_near_sum(p):
        take_far(4, p)
        second_add(1, p, 4)
        send_far(1, 1, near, p)

    @on_inner
    def _():
        pass_far_sum(0)
        pass_near_sum(0)

    stage_first(0)

    @on_inner
    def _():
        pass_far_sum(1)
        pass_near_sum(1)

    for copy in small:
        copy.wait()
    st[:, columns:] = jnp.broadcast_to(jnp.sum(row_state[...], axis=1, keepdims=True), (1, stat_width - columns))
    stage_second(0)
    for p in range(2):
        take_far(1, p)

    @on_inner
    def _():
        for p in range(2):
            take_far(5, p)

    with scope("final"):
        cuts = [(0, 6), (6, 7), (7, 8)]
        sums = [None] * len(cuts)
        for i in range(tiles):
            r = pl.ds(i * TILE, TILE)
            row_sum = 0.0
            for k, (d, e) in enumerate(cuts):
                l = pl.ds(d * lane, (e - d) * lane)
                terms = [lg[0, x, y, r, l], rx[0, 1, r, l], rx[0, 2, r, l]]
                if e <= parts[0 if i < cut_row else 1][3]:
                    terms += [rz[1, r, l], rz[5, r, l]]
                value = add(*terms)
                summed[r, l] = value
                value = value * value
                row_sum = row_sum + jnp.sum(value, axis=1, keepdims=True)
                sums[k] = value if sums[k] is None else sums[k] + value
            own[r, :] = row_sum
        for (d, e), value in zip(cuts, sums):
            st[:, pl.ds(d * lane, (e - d) * lane)] = jnp.sum(value, axis=0, keepdims=True)

    me = gx * 2 + y
    for peer in plane:
        rdma(st, st1.at[me], s1s, s1r, peer).start()
    st1[me] = st[...]
    take_send(cr, cs)
    take_send(some(3 * area(halves)), fs.at[0])
    take_send(some(9 * area(parts)), fs.at[1])
    take_send(some(3 * area(parts)), zs)
    take_send(some(12 * area(strips)), ks)
    diagonal = lax.broadcasted_iota(jnp.int32, (rows, rows), 0) == lax.broadcasted_iota(jnp.int32, (rows, rows), 1)
    state_down = jnp.sum(jnp.where(diagonal, jnp.broadcast_to(row_state[...], (rows, rows)), 0.0), axis=1, keepdims=True)
    with scope("stat1"):
        take_recv(st1.at[0:nx * 2 - 1], s1r)
    total = st1[0]
    for k in range(1, nx * 2):
        total = total + st1[k]
    tot[...] = total
    for t in range(1, nz):
        rdma(tot, st2.at[z], s2s, s2r, (gx, zof(t), y)).start()
    st2[z] = total
    with scope("stat2"):
        take_recv(st2.at[0:nz - 1], s2r)
    total = st2[0]
    for k in range(1, nz):
        total = total + st2[k]
    column_sum = total[:, 0:columns]
    norm_square = jnp.sum(column_sum, axis=1, keepdims=True)
    state_sum = total[:, columns:columns + 1]
    clip_level = 0.5 * math.sqrt(full_width * columns)
    factor = jnp.minimum(jnp.float32(1.0), clip_level / jnp.sqrt(norm_square + 1e-06))
    square_factor = factor * factor
    column_next = beta_two * col_state[...] + (1.0 - beta_two) * (square_factor * column_sum / full_width)
    row_average = (beta_two * state_sum + (1.0 - beta_two) * (square_factor * norm_square / columns)) / full_width
    row_next = beta_two * state_down + (1.0 - beta_two) * (square_factor * own[...] / columns)
    own[...] = (step_size * factor) / jnp.sqrt(row_next / row_average)
    col_scale = 1.0 / jnp.sqrt(column_next)

    def update(r, l, _):
        new = params[r, l].astype(f32) - (summed[r, l] * own[r, :]) * col_scale
        full[x, c, z, y, r, l] = new.astype(bf16)
    with scope("update"):
        over(whole, update)

    def same(view, ssem, rsem, peer):
        rdma(view, view, ssem, rsem, peer).start()

    def moves(t):
        return qs.at[1 if t else 0]

    def piece(bx, u, by, region):
        r, l = at(region)
        return full.at[bx, c, u, by, r, l]

    def pass_core(t, bx, by):
        for region in parts if t else [whole]:
            same(piece(bx, origin[t], by, region), gcs, gcr, core_peer)

    def send_q1(t):
        u, (a, b) = origin[t], spans(t)
        same(piece(x, u, y, a), moves(t), q1r.at[t], y_peer)
        same(piece(x, u, y, b), moves(t), q1r.at[t], x_peer)

    def send_q2(t):
        u, (a, b) = origin[t], spans(t)
        same(piece(x, u, y, a), moves(t), q2r.at[t], x_peer)
        same(piece(x, u, y, b), moves(t), q2r.at[t], y_peer)
        pass_core(t, x, y)

    def send_own(t):
        send_q1(t)
        send_q2(t)

    def pass_far(t, slot, peer):
        for region in parts:
            same(piece(x, origin[t], y, region), gzs, gzr.at[slot], peer)

    def take_z(t):
        with scope(f"gz{t}"):
            take_recv(some(area(parts)), gzr.at[t])

    def gather_cross(t):
        u, (a, b) = origin[t], spans(t)
        with scope(f"q1_{t}"):
            take_recv(some(area(spans(t))), q1r.at[t])
        same(piece(x, u, 1 - y, a), moves(t), q3r.at[t], x_peer)
        same(piece(1 - x, u, y, b), moves(t), q3r.at[t], y_peer)

    def gather_side(t):
        with scope(f"q2_{t}"):
            take_recv(some(area(spans(t))), q2r.at[t])
        pass_core(t, 1 - x, y)
        pass_core(t, x, 1 - y)

    def gather_far(t):
        with scope(f"q3_{t}"):
            take_recv(some(area(spans(t))), q3r.at[t])
        pass_core(t, 1 - x, 1 - y)

    def each_strip(t, ssem, rsem, peer):
        for region in strips:
            r, l = at(region)
            same(full.at[:, c, origin[t], :, r, l], ssem, rsem, peer)

    def pass_strip(t, slot, peer):
        each_strip(t, gks, gkr.at[slot], peer)

    def take_strip(t):
        with scope(f"strip{t}"):
            take_recv(some(4 * area(strips)), gkr.at[t])
        each_strip(t, gcs, gcr, core_peer)

    pass_far(0, 1, near)
    send_q1(0)
    on_inner(lambda: pass_far(0, 2, middle))
    send_q2(0)
    new_ref[...] = full[x, c, z, y]
    col_ref[...] = column_next
    row_ref[...] = jnp.sum(jnp.where(diagonal, jnp.broadcast_to(row_next, (rows, rows)), 0.0), axis=0, keepdims=True)
    gather_cross(0)
    take_z(1)
    on_inner(lambda: pass_far(1, 3, middle))
    send_own(1)

    @on_inner
    def _():
        take_z(2)
        pass_far(2, 2, near)

    gather_side(0)
    gather_far(0)
    pass_strip(0, 1, near)
    on_inner(lambda: pass_strip(0, 2, middle))
    gather_cross(1)
    on_end(lambda: take_z(2))
    send_own(2)

    @on_inner
    def _():
        take_z(3)
        pass_far(3, 3, near)

    gather_side(1)
    gather_far(1)
    take_strip(1)
    on_inner(lambda: pass_strip(1, 3, middle))
    gather_cross(2)
    on_end(lambda: take_z(3))
    send_own(3)

    @on_inner
    def _():
        take_strip(2)
        pass_strip(2, 2, near)

    gather_side(2)
    gather_far(2)

    @on_inner
    def _():
        take_strip(3)
        pass_strip(3, 3, near)

    on_end(lambda: take_strip(2))
    gather_cross(3)
    gather_side(3)
    gather_far(3)
    on_end(lambda: take_strip(3))

    with scope("finish"):
        take_send(st1.at[0:nx * 2 - 1], s1s)
        take_send(st2.at[0:nz - 1], s2s)
        take_send(some(3 * area(halves)), qs.at[0])
        take_send(some(9 * area(parts)), qs.at[1])

        @on_end
        def _():
            take_send(some(area(parts)), gzs)
            take_send(some(4 * area(strips)), gks)

        @on_inner
        def _():
            take_send(some(5 * area(parts)), gzs)
            take_send(some(20 * area(strips)), gks)

        take_send(full.at[:, c], gcs)
        take_recv(full.at[:, c], gcr)


def write_out(nz, new, row, col, full, new_out, row_out, col_out, full_out, sem):
    pieces = [(full.at[a, b, u], full_out.at[a, b, u]) for a in range(2) for b in range(2) for u in range(nz)]
    copies = [pltpu.make_async_copy(src, dst, sem.at[0]) for src, dst in pieces]
    small = [pltpu.make_async_copy(src, dst, sem.at[k + 1])
             for k, (src, dst) in enumerate([(new, new_out), (row, row_out), (col, col_out)])]
    for copy in copies + small:
        copy.start()
    for copy in small:
        copy.wait()
    pltpu.make_async_copy(full, full_out, sem.at[0]).wait()


def fused(nx, nz, grad_bucket, parameters, row_state, column_state):
    _, _, full_width, columns = grad_bucket.shape
    rows = parameters.shape[1]
    lane = columns // 8
    bf16, f32 = jnp.bfloat16, jnp.float32
    vmem = pl.BlockSpec(memory_space=pltpu.VMEM)
    hbm = pl.BlockSpec(memory_space=pltpu.HBM)
    dma = pltpu.SemaphoreType.DMA
    one = dma(())
    shapes = [((rows, columns), bf16), ((1, rows), f32), ((1, columns), f32), ((2, 2, nz, 2, rows, columns), bf16)]
    held = 2 * columns * (rows + full_width) + 4 * (columns + -(-rows // 128) * 128)
    stat = columns + 128
    results = pl.pallas_call(
        functools.partial(kernel, nx, nz),
        out_shape=tuple(pltpu.VMEM(*shape) for shape in shapes),
        in_specs=[hbm] * 4,
        out_specs=(vmem,) * 4,
        scratch_shapes=[
            pltpu.VMEM((nz, 2, 2, rows, columns), bf16),
            pltpu.VMEM((nz, 2, 2, rows, columns), bf16),
            pltpu.VMEM((nz, 3, rows, columns), bf16),
            pltpu.VMEM((6, rows, columns), bf16),
            pltpu.VMEM((6, 2, 2, rows, 2 * lane), bf16),
            pltpu.VMEM((9 * 8 * (rows // TILE), TILE, lane), bf16),
            pltpu.VMEM((rows, columns), f32),
            pltpu.VMEM((rows, 1), f32),
            pltpu.VMEM((1, stat), f32),
            pltpu.VMEM((nx * 2, 1, stat), f32),
            pltpu.VMEM((1, stat), f32),
            pltpu.VMEM((nz, 1, stat), f32),
            pltpu.VMEM((rows, columns), bf16),
            pltpu.VMEM((1, rows), f32),
            pltpu.VMEM((1, columns), f32),
            dma((nz,)), dma((3,)), one, dma((4,)), dma((nz,)), dma((2,)), dma((nz,)), dma((nz,)),
            one, dma((6, 2)), one, dma((6, 2)), one, one, one, one,
            one, dma((nz,)), dma((2,)), dma((nz,)), dma((nz,)), dma((nz,)), one, dma((nz,)), one, one,
        ],
        compiler_params=pltpu.CompilerParams(
            collective_id=0, has_side_effects=True, vmem_limit_bytes=VMEM_BYTES - held),
    )(grad_bucket.reshape(2, 2, nz, 2, rows, columns), parameters[0], row_state, column_state)
    new, row, col, full = pl.pallas_call(
        functools.partial(write_out, nz),
        out_shape=tuple(jax.ShapeDtypeStruct(*shape) for shape in shapes),
        in_specs=[vmem] * 4,
        out_specs=(hbm,) * 4,
        scratch_shapes=[dma((4,))],
        compiler_params=pltpu.CompilerParams(vmem_limit_bytes=4 * 1024 * 1024),
    )(*[pltpu.with_memory_space_constraint(result, pltpu.VMEM) for result in results])
    return (new[None], row, col, full.reshape(full_width, columns))


def solution(mesh):
    nx, nz, ny = (mesh.shape[a] for a in AXES)
    in_specs = (
        P(AXES, None, None, None),
        P(None, AXES, None),
        P(None, AXES),
        P(),
    )
    out_specs = (P(None, AXES, None), P(None, AXES), P(), P())
    fits = nx == 4 and ny == 2 and nz == 4

    def body(grad_bucket, parameters, row_state, column_state):
        if fits and grad_bucket.shape[1] == 1 and parameters.shape[1] % TILE == 0 and parameters.shape[1] >= 2 * TILE and grad_bucket.shape[3] % 1024 == 0:
            return fused(nx, nz, grad_bucket, parameters, row_state, column_state)
        return shards(grad_bucket, parameters, row_state, column_state)

    return jax.shard_map(body, mesh=mesh, in_specs=in_specs, out_specs=out_specs, check_vma=False)
```

```python
import functools
import math

import jax
import jax.numpy as jnp
from jax import lax
from jax.experimental import pallas as pl
from jax.experimental.pallas import tpu as pltpu
from jax.sharding import PartitionSpec as P

beta_two = 0.8
step_size = 0.5
AXES = ("gx", "gy", "gz")
TILE = 16
VMEM_BYTES = 67043328 - 131072


def shards(grad_bucket, parameters, row_state, column_state):
    local_grad = grad_bucket[0].astype(jnp.float32)
    layer_count, full_width, columns = local_grad.shape
    summed = lax.psum_scatter(local_grad, AXES, scatter_dimension=1, tiled=True)
    clip_level = 0.5 * math.sqrt(layer_count * full_width * columns)
    squares = summed * summed
    norm_square = lax.psum(jnp.sum(squares), AXES)
    factor = jnp.minimum(jnp.float32(1.0), clip_level / jnp.sqrt(norm_square + 1e-06))
    clipped = factor * summed
    clipped_square = clipped * clipped
    row_next = beta_two * row_state + (1.0 - beta_two) * jnp.mean(clipped_square, axis=2)
    column_part, row_total = lax.psum((jnp.sum(clipped_square, axis=1), jnp.sum(row_next, axis=1)), AXES)
    column_next = beta_two * column_state + (1.0 - beta_two) * column_part / full_width
    row_average = row_total / full_width
    second = row_next[:, :, None] * column_next[:, None, :] / row_average[:, None, None]
    update = clipped / jnp.sqrt(second)
    new_parameters = (parameters.astype(jnp.float32) - step_size * update).astype(jnp.bfloat16)
    first_layer = lax.all_gather(new_parameters[0], AXES, axis=0, tiled=True)
    return (new_parameters, row_next, column_next, first_layer)


def flip(index, mask, size):
    out, bit = 0, 1
    while bit < size:
        out = out + bit * (((index // bit) % 2 + (mask // bit) % 2) % 2)
        bit *= 2
    return out


def kernel(nx, nz, grad, params_in, row_in, col_in, new_ref, row_ref, col_ref, full,
           lg, cr, rx, rz, rc, unit, sums_of, params_of, info, scale, st, st1, tot, st2, row_state, col_state,
           lsem, isem, cs, cfr, cvr, fs, fr, hr, zs, zr, ks, kr, s1s, s1r, s2s, s2r,
           gzs, gzr, qs, q1r, q2r, q3r, gks, gkr, gcs, gcr, ns, nr, nzs, nzr, ins, inr):
    gx, z, y = lax.axis_index("gx"), lax.axis_index("gy"), lax.axis_index("gz")
    x, c = gx // 2, gx % 2
    rows, columns = new_ref.shape
    params, sums = params_of.at[0], sums_of.at[0]
    lane = columns // 8
    stat_width = st.shape[1]
    full_width = rows * 4 * nz * 2
    core_peer = (x * 2 + 1 - c, z, y)
    x_peer = ((1 - x) * 2 + c, z, y)
    y_peer = (gx, z, 1 - y)
    tiles = rows // TILE
    f32, bf16 = jnp.float32, jnp.bfloat16
    scope = jax.named_scope
    blocks = [(1 - x, 1 - y), (1 - x, y), (x, 1 - y), (x, y)]

    cut_row = (tiles * 4 + 3) // 7
    parts = [(0, cut_row, 0, 6), (cut_row, tiles, 0, 7)]
    strips = [(0, cut_row, 6, 8), (cut_row, tiles, 7, 8)]
    halves = [(0, tiles, 0, 4), (0, tiles, 4, 8)]

    def area(regions):
        return sum((b - a) * (e - d) for a, b, d, e in regions)

    def at(region, shift=0):
        a, b, d, e = region
        return pl.ds(a * TILE, (b - a) * TILE), pl.ds((d - shift) * lane, (e - d) * lane)

    def spans(t):
        return halves if t == 0 else parts[::-1] if t % 2 else parts

    def zof(t):
        return flip(z, t, nz)

    inside = (z + z // 2) % 2
    near, middle = (gx, zof(1), y), (gx, zof(3), y)
    origin = [z, zof(1), flip(z, 2 + inside, nz), flip(z, 3 - inside, nz)]

    def on_end(step):
        pl.when(inside == 0)(step)

    def on_inner(step):
        pl.when(inside == 1)(step)

    def rdma(src, dst, ssem, rsem, peer):
        return pltpu.make_async_remote_copy(
            src_ref=src, dst_ref=dst, send_sem=ssem, recv_sem=rsem,
            device_id=peer, device_id_type=pl.DeviceIdType.MESH)

    def take_recv(view, sem):
        rdma(view, view, sem, sem, core_peer).wait_recv()

    def take_send(view, sem):
        rdma(view, view, sem, sem, core_peer).wait_send()

    def some(count):
        return unit.at[pl.ds(0, count)]

    first = 3
    loads = {t: pltpu.make_async_copy(grad.at[:, c, zof(t)], lg.at[t], lsem.at[t]) for t in (3, 2, 1, 0)}
    for t in loads:
        loads[t].start()
    small = [pltpu.make_async_copy(src, dst, isem.at[k]) for k, (src, dst) in enumerate(
        [(params_in, params), (row_in, row_state), (col_in, col_state)])]
    for copy in small:
        copy.start()

    barrier = pltpu.get_barrier_semaphore()
    plane = [((gx + a) % nx, z, (y + b) % 2) for a in range(nx) for b in range(2) if (a, b) != (0, 0)]
    line = [(gx, zof(t), y) for t in range(1, nz)]
    for peer in line + plane:
        pl.semaphore_signal(barrier, inc=1, device_id=peer, device_id_type=pl.DeviceIdType.MESH)
    with scope("barrier"):
        pl.semaphore_wait(barrier, len(plane) + len(line))

    for k, (bx, by) in enumerate(blocks):
        rdma(grad.at[bx, 1 - c, zof(first), by], cr.at[first, bx, by], cs, cfr.at[k], core_peer).start()
    for t in (2, 1, 0):
        rdma(grad.at[:, 1 - c, zof(t)], cr.at[t], cs, cvr.at[t], core_peer).start()

    X, Y, NEAR, MIDDLE = 1, 2, 3, 4

    def send_plane(src, dst, swap):
        for region, (slot, peer) in zip(halves, [(X, x_peer), (Y, y_peer)] if swap else [(Y, y_peer), (X, x_peer)]):
            r, l = at(region)
            rdma(src.at[r, l], dst.at[slot, r, l], ns, nr.at[1 if swap else 0], peer).start()

    def send_near(src, dst, slot, peer, regions):
        for region in regions:
            r, l = at(region)
            rdma(src.at[r, l], dst.at[slot, r, l], nzs, nzr.at[slot - NEAR], peer).start()

    @on_inner
    def _():
        send_near(params_in, params_of, NEAR, near, parts)
        send_near(params_in, params_of, MIDDLE, middle, parts)

    def add(*terms):
        total = terms[0].astype(f32)
        for term in terms[1:]:
            total = total + term.astype(f32)
        return total

    def over(region, step, shift=0):
        a, b, d, e = region

        @pl.loop(a, b, unroll=True)
        def _(i):
            step(pl.ds(pl.multiple_of(i * TILE, TILE), TILE), pl.ds(d * lane, (e - d) * lane),
                 pl.ds((d - shift) * lane, (e - d) * lane))

    whole = (0, tiles, 0, 8)

    def pair_sum(t, bx, by):
        def step(r, l, _):
            lg[t, bx, by, r, l] = add(lg[t, bx, by, r, l], cr[t, bx, by, r, l]).astype(bf16)
        over(whole, step)

    def cross(t):
        return fs.at[1 if t else 0]

    def send(t, bx, by, slot, region, sem, peer):
        r, l = at(region)
        rdma(lg.at[t, bx, by, r, l], rx.at[t, slot, r, l], cross(t), sem.at[t], peer).start()

    def send_f(t):
        a, b = spans(t)
        send(t, 1 - x, 1 - y, 0, a, fr, x_peer)
        send(t, 1 - x, 1 - y, 0, b, fr, y_peer)

    def send_ga(t):
        send(t, 1 - x, y, 1, spans(t)[0], hr, x_peer)

    def send_gb(t):
        send(t, x, 1 - y, 1, spans(t)[1], hr, y_peer)

    def send_g(t):
        send_ga(t)
        send_gb(t)

    side = [1 - x, x]

    def send_strip(t, slot, peer, h):
        for region in strips:
            r, l = at(region)
            _, m = at(region, 6)
            rdma(lg.at[t, side[h], :, r, l], rc.at[slot, h, :, r, m], ks, kr.at[slot, h], peer).start()

    def send_strips(t, slot, peer):
        for h in range(2):
            send_strip(t, slot, peer, h)

    def take_strips(h, *slots):
        for slot in slots:
            with scope(f"line{slot}_{h}"):
                take_recv(some(2 * area(strips)), kr.at[slot, h])

    def strip_add(t, h, *slots):
        for by in range(2):
            def step(r, l, m):
                lg[t, side[h], by, r, l] = add(
                    lg[t, side[h], by, r, l], *[rc[slot, h, by, r, m] for slot in slots]).astype(bf16)
            for region in strips:
                over(region, step, 6)

    def relay(came, t, slot, peer):
        for h in range(2):
            take_strips(h, came)
            strip_add(t, h, came)
            send_strip(t, slot, peer, h)

    def stage_pair(t):
        with scope(f"pair{t}"):
            take_recv(cr.at[t], cvr.at[t])
            loads[t].wait()
            for bx, by in blocks:
                pair_sum(t, bx, by)

    def stage_first(t):
        a, b = spans(t)
        with scope(f"f{t}"):
            take_recv(some(area(spans(t))), fr.at[t])

        def step_a(r, l, _):
            lg[t, x, 1 - y, r, l] = add(lg[t, x, 1 - y, r, l], rx[t, 0, r, l]).astype(bf16)

        def step_b(r, l, _):
            lg[t, 1 - x, y, r, l] = add(lg[t, 1 - x, y, r, l], rx[t, 0, r, l]).astype(bf16)
        over(a, step_a)
        send(t, x, 1 - y, 2, a, hr, y_peer)
        over(b, step_b)
        send(t, 1 - x, y, 2, b, hr, x_peer)

    def stage_second(t):
        with scope(f"h{t}"):
            take_recv(some(2 * area(spans(t))), hr.at[t])

    def send_far(t, slot, peer, p):
        r, l = at(parts[p])
        rdma(lg.at[t, x, y, r, l], rz.at[slot, r, l], zs, zr.at[slot, p], peer).start()

    def take_far(slot, p):
        with scope(f"far{slot}_{p}"):
            take_recv(some(area(parts[p:p + 1])), zr.at[slot, p])

    def second_add(t, p, *slots):
        def step(r, l, _):
            lg[t, x, y, r, l] = add(lg[t, x, y, r, l], rx[t, 1, r, l], rx[t, 2, r, l],
                                    *[rz[slot, r, l] for slot in slots]).astype(bf16)
        over(parts[p], step)

    loads[first].wait()
    for k, (bx, by) in enumerate(blocks):
        with scope(f"core{k}"):
            take_recv(cr.at[first, bx, by], cfr.at[k])
        pair_sum(first, bx, by)
        if k == 0:
            send_f(first)
        elif k == 1:
            send_ga(first)
            on_end(lambda: send_strip(3, 3, near, 0))
        elif k == 2:
            send_gb(first)
        else:
            on_end(lambda: send_strip(3, 3, near, 1))
    stage_pair(2)
    on_end(lambda: send_strips(2, 2, near))
    send_f(2)
    stage_first(3)
    send_g(2)
    stage_pair(1)
    on_end(lambda: send_strips(1, 1, near))
    send_f(1)
    on_inner(lambda: relay(3, 2, 4, middle))
    stage_pair(0)

    @on_end
    def _():
        rz[5] = jnp.zeros((rows, columns), bf16)

    stage_first(2)
    send_g(1)
    on_inner(lambda: relay(2, 3, 5, middle))
    stage_second(3)
    for p in range(2):
        second_add(3, p)
        on_end(lambda: send_far(3, 3, near, p))
    on_inner(lambda: relay(4, 1, 0, near))
    stage_first(1)

    @on_end
    def _():
        stage_second(2)
        for p in range(2):
            second_add(2, p)
            send_far(2, 2, near, p)
        for h in range(2):
            take_strips(h, 0)
            strip_add(0, h, 0)

    @on_inner
    def _():
        for h in range(2):
            take_strips(h, 1, 5)
            strip_add(0, h, 1, 5)

    send_f(0)
    send_g(0)

    @on_inner
    def _():
        stage_second(2)
        for p in range(2):
            take_far(3, p)
            second_add(2, p, 3)
            send_far(2, 4, middle, p)

    def pass_far_sum(p):
        take_far(2, p)

        def step(r, l, _):
            lg[3, x, y, r, l] = add(lg[3, x, y, r, l], rz[2, r, l]).astype(bf16)
        over(parts[p], step)
        send_far(3, 5, middle, p)

    stage_second(1)

    @on_end
    def _():
        for p in range(2):
            second_add(1, p)
            send_far(1, 1, near, p)

    def pass_near_sum(p):
        take_far(4, p)
        second_add(1, p, 4)
        send_far(1, 1, near, p)

    @on_inner
    def _():
        pass_far_sum(0)
        pass_near_sum(0)

    stage_first(0)
    for copy in small:
        copy.wait()
    send_plane(params, params_of, False)

    @on_inner
    def _():
        pass_far_sum(1)
        pass_near_sum(1)

    on_end(lambda: send_near(params, params_of, NEAR, near, parts))
    info[0, 0:1, :] = row_state[...]
    st[:, columns:] = jnp.broadcast_to(jnp.sum(row_state[...], axis=1, keepdims=True), (1, stat_width - columns))
    stage_second(0)
    for p in range(2):
        take_far(1, p)

    @on_inner
    def _():
        for p in range(2):
            take_far(5, p)

    with scope("final"):
        cuts = [(0, 6), (6, 7), (7, 8)]
        squares = [None] * len(cuts)
        row_sums = []
        for i in range(tiles):
            r = pl.ds(i * TILE, TILE)
            row_sum = 0.0
            for k, (d, e) in enumerate(cuts):
                l = pl.ds(d * lane, (e - d) * lane)
                terms = [lg[0, x, y, r, l], rx[0, 1, r, l], rx[0, 2, r, l]]
                if e <= parts[0 if i < cut_row else 1][3]:
                    terms += [rz[1, r, l], rz[5, r, l]]
                value = add(*terms)
                sums[r, l] = value.astype(bf16)
                value = value * value
                row_sum = row_sum + jnp.sum(value, axis=1, keepdims=True)
                squares[k] = value if squares[k] is None else squares[k] + value
            scale[0, r, :] = row_sum
        for (d, e), value in zip(cuts, squares):
            st[:, pl.ds(d * lane, (e - d) * lane)] = jnp.sum(value, axis=0, keepdims=True)

    me = gx * 2 + y
    for peer in plane:
        rdma(st, st1.at[me], s1s, s1r, peer).start()
    st1[me] = st[...]
    diagonal = lax.broadcasted_iota(jnp.int32, (rows, rows), 0) == lax.broadcasted_iota(jnp.int32, (rows, rows), 1)

    def turned(vector, axis):
        return jnp.sum(jnp.where(diagonal, jnp.broadcast_to(vector, (rows, rows)), 0.0), axis=axis, keepdims=True)

    info[0, 1:2, :] = turned(scale[0], 0)

    def send_info(slot, peer):
        rdma(info.at[0], info.at[slot], ins, inr.at[slot], peer).start()

    send_info(X, x_peer)
    send_info(Y, y_peer)
    send_info(NEAR, near)
    on_inner(lambda: send_info(MIDDLE, middle))
    send_plane(sums, sums_of, False)
    send_plane(params, params_of, True)
    send_plane(sums, sums_of, True)

    def send_sums(p):
        send_near(sums, sums_of, NEAR, near, parts[p:p + 1])
        on_inner(lambda: send_near(sums, sums_of, MIDDLE, middle, parts[p:p + 1]))

    send_sums(0)
    take_send(cr, cs)
    take_send(some(3 * area(halves)), fs.at[0])
    take_send(some(9 * area(parts)), fs.at[1])
    take_send(some(3 * area(parts)), zs)
    take_send(some(12 * area(strips)), ks)
    with scope("stat1"):
        take_recv(st1.at[0:nx * 2 - 1], s1r)
    total = st1[0]
    for k in range(1, nx * 2):
        total = total + st1[k]
    tot[...] = total
    for t in range(1, nz):
        rdma(tot, st2.at[z], s2s, s2r, (gx, zof(t), y)).start()
    send_sums(1)
    st2[z] = total
    with scope("stat2"):
        take_recv(st2.at[0:nz - 1], s2r)
    total = st2[0]
    for k in range(1, nz):
        total = total + st2[k]
    column_sum = total[:, 0:columns]
    norm_square = jnp.sum(column_sum, axis=1, keepdims=True)
    state_sum = total[:, columns:columns + 1]
    clip_level = 0.5 * math.sqrt(full_width * columns)
    factor = jnp.minimum(jnp.float32(1.0), clip_level / jnp.sqrt(norm_square + 1e-06))
    square_factor = factor * factor
    column_next = beta_two * col_state[...] + (1.0 - beta_two) * (square_factor * column_sum / full_width)
    row_average = (beta_two * state_sum + (1.0 - beta_two) * (square_factor * norm_square / columns)) / full_width
    col_scale = 1.0 / jnp.sqrt(column_next)

    def next_of(slot):
        return beta_two * info[slot, 0:1, :] + (1.0 - beta_two) * (square_factor * info[slot, 1:2, :] / columns)

    def rate(slot):
        if slot:
            with scope(f"info{slot}"):
                take_recv(info.at[slot], inr.at[slot])
        scale[slot] = turned((step_size * factor) / jnp.sqrt(next_of(slot) / row_average), 1)

    def update(slot, bx, u, by, regions):
        def step(r, l, _):
            new = params_of[slot, r, l].astype(f32) - (sums_of[slot, r, l].astype(f32) * scale[slot, r, :]) * col_scale_of(l)
            full[bx, c, u, by, r, l] = new.astype(bf16)
        for region in regions:
            over(region, step)

    def col_scale_of(l):
        return col_scale[:, l.start:l.start + l.size]

    def same(view, ssem, rsem, peer):
        rdma(view, view, ssem, rsem, peer).start()

    def moves(t):
        return qs.at[1 if t else 0]

    def piece(bx, u, by, region):
        r, l = at(region)
        return full.at[bx, c, u, by, r, l]

    def pass_core(t, bx, by):
        for region in parts if t else [whole]:
            same(piece(bx, origin[t], by, region), gcs, gcr, core_peer)

    def send_q1(t):
        u, (a, b) = origin[t], spans(t)
        same(piece(x, u, y, a), moves(t), q1r.at[t], y_peer)
        same(piece(x, u, y, b), moves(t), q1r.at[t], x_peer)

    def send_q2(t):
        u, (a, b) = origin[t], spans(t)
        same(piece(x, u, y, a), moves(t), q2r.at[t], x_peer)
        same(piece(x, u, y, b), moves(t), q2r.at[t], y_peer)
        pass_core(t, x, y)

    def send_own(t):
        send_q1(t)
        send_q2(t)

    def pass_far(t, slot, peer):
        for region in parts:
            same(piece(x, origin[t], y, region), gzs, gzr.at[slot], peer)

    def take_z(t):
        with scope(f"gz{t}"):
            take_recv(some(area(parts)), gzr.at[t])

    def gather_cross(t):
        u, (a, b) = origin[t], spans(t)
        with scope(f"q1_{t}"):
            take_recv(some(area(spans(t))), q1r.at[t])
        same(piece(x, u, 1 - y, a), moves(t), q3r.at[t], x_peer)
        same(piece(1 - x, u, y, b), moves(t), q3r.at[t], y_peer)

    def gather_side(t):
        with scope(f"q2_{t}"):
            take_recv(some(area(spans(t))), q2r.at[t])
        pass_core(t, 1 - x, y)
        pass_core(t, x, 1 - y)

    def gather_far(t):
        with scope(f"q3_{t}"):
            take_recv(some(area(spans(t))), q3r.at[t])
        pass_core(t, 1 - x, 1 - y)

    def each_strip(t, ssem, rsem, peer):
        for region in strips:
            r, l = at(region)
            same(full.at[:, c, origin[t], :, r, l], ssem, rsem, peer)

    def pass_strip(t, slot, peer):
        each_strip(t, gks, gkr.at[slot], peer)

    def take_strip(t):
        with scope(f"strip{t}"):
            take_recv(some(4 * area(strips)), gkr.at[t])
        each_strip(t, gcs, gcr, core_peer)

    low, high = halves
    rate(X)
    rate(Y)
    with scope("plane1"):
        take_recv(some(4 * area(halves[:1])), nr.at[0])
    update(Y, x, z, 1 - y, [low])
    update(X, 1 - x, z, y, [high])
    same(piece(x, z, 1 - y, low), moves(0), q3r.at[0], x_peer)
    same(piece(1 - x, z, y, high), moves(0), q3r.at[0], y_peer)
    rate(NEAR)
    with scope("near"):
        take_recv(some(2 * area(parts)), nzr.at[0])
    update(NEAR, x, origin[1], y, parts)
    on_inner(lambda: pass_far(1, 3, middle))
    send_own(1)

    @on_inner
    def _():
        rate(MIDDLE)
        with scope("middle"):
            take_recv(some(2 * area(parts)), nzr.at[1])
        update(MIDDLE, x, origin[2], y, parts)
        pass_far(2, 2, near)

    rate(0)
    update(0, x, z, y, [whole])
    pass_core(0, x, y)
    new_ref[...] = full[x, c, z, y]
    col_ref[...] = column_next
    row_ref[...] = next_of(0)
    with scope("plane2"):
        take_recv(some(4 * area(halves[:1])), nr.at[1])
    update(X, 1 - x, z, y, [low])
    update(Y, x, z, 1 - y, [high])
    pass_core(0, 1 - x, y)
    pass_core(0, x, 1 - y)
    gather_far(0)
    pass_strip(0, 1, near)
    on_inner(lambda: pass_strip(0, 2, middle))
    gather_cross(1)
    on_end(lambda: take_z(2))
    send_own(2)

    @on_inner
    def _():
        take_z(3)
        pass_far(3, 3, near)

    gather_side(1)
    gather_far(1)
    take_strip(1)
    on_inner(lambda: pass_strip(1, 3, middle))
    gather_cross(2)
    on_end(lambda: take_z(3))
    send_own(3)

    @on_inner
    def _():
        take_strip(2)
        pass_strip(2, 2, near)

    gather_side(2)
    gather_far(2)

    @on_inner
    def _():
        take_strip(3)
        pass_strip(3, 3, near)

    gather_cross(3)
    gather_side(3)
    on_end(lambda: take_strip(2))
    gather_far(3)
    on_end(lambda: take_strip(3))

    with scope("finish"):
        take_send(st1.at[0:nx * 2 - 1], s1s)
        take_send(st2.at[0:nz - 1], s2s)
        take_send(some(area(halves)), qs.at[0])
        take_send(some(9 * area(parts)), qs.at[1])
        take_send(some(4 * area(halves)), ns)

        @on_end
        def _():
            take_send(some(2 * area(parts)), nzs)
            take_send(info.at[0:3], ins)
            take_send(some(4 * area(strips)), gks)

        @on_inner
        def _():
            take_send(some(4 * area(parts)), nzs)
            take_send(info.at[0:4], ins)
            take_send(some(3 * area(parts)), gzs)
            take_send(some(20 * area(strips)), gks)

        take_send(full.at[:, c], gcs)
        take_recv(full.at[:, c], gcr)


def write_out(nz, new, row, col, full, new_out, row_out, col_out, full_out, sem):
    pieces = [(full.at[a, b, u], full_out.at[a, b, u]) for a in range(2) for b in range(2) for u in range(nz)]
    copies = [pltpu.make_async_copy(src, dst, sem.at[0]) for src, dst in pieces]
    small = [pltpu.make_async_copy(src, dst, sem.at[k + 1])
             for k, (src, dst) in enumerate([(new, new_out), (row, row_out), (col, col_out)])]
    for copy in copies + small:
        copy.start()
    for copy in small:
        copy.wait()
    pltpu.make_async_copy(full, full_out, sem.at[0]).wait()


def fused(nx, nz, grad_bucket, parameters, row_state, column_state):
    _, _, full_width, columns = grad_bucket.shape
    rows = parameters.shape[1]
    lane = columns // 8
    bf16, f32 = jnp.bfloat16, jnp.float32
    vmem = pl.BlockSpec(memory_space=pltpu.VMEM)
    hbm = pl.BlockSpec(memory_space=pltpu.HBM)
    dma = pltpu.SemaphoreType.DMA
    one = dma(())
    shapes = [((rows, columns), bf16), ((1, rows), f32), ((1, columns), f32), ((2, 2, nz, 2, rows, columns), bf16)]
    held = 2 * columns * (rows + full_width) + 4 * (columns + -(-rows // 128) * 128)
    stat = columns + 128
    results = pl.pallas_call(
        functools.partial(kernel, nx, nz),
        out_shape=tuple(pltpu.VMEM(*shape) for shape in shapes),
        in_specs=[hbm] * 4,
        out_specs=(vmem,) * 4,
        scratch_shapes=[
            pltpu.VMEM((nz, 2, 2, rows, columns), bf16),
            pltpu.VMEM((nz, 2, 2, rows, columns), bf16),
            pltpu.VMEM((nz, 3, rows, columns), bf16),
            pltpu.VMEM((6, rows, columns), bf16),
            pltpu.VMEM((6, 2, 2, rows, 2 * lane), bf16),
            pltpu.VMEM((9 * 8 * (rows // TILE), TILE, lane), bf16),
            pltpu.VMEM((5, rows, columns), bf16),
            pltpu.VMEM((5, rows, columns), bf16),
            pltpu.VMEM((5, 2, rows), f32),
            pltpu.VMEM((5, rows, 1), f32),
            pltpu.VMEM((1, stat), f32),
            pltpu.VMEM((nx * 2, 1, stat), f32),
            pltpu.VMEM((1, stat), f32),
            pltpu.VMEM((nz, 1, stat), f32),
            pltpu.VMEM((1, rows), f32),
            pltpu.VMEM((1, columns), f32),
            dma((nz,)), dma((3,)), one, dma((4,)), dma((nz,)), dma((2,)), dma((nz,)), dma((nz,)),
            one, dma((6, 2)), one, dma((6, 2)), one, one, one, one,
            one, dma((nz,)), dma((2,)), dma((nz,)), dma((nz,)), dma((nz,)), one, dma((nz,)), one, one,
            one, dma((2,)), one, dma((2,)), one, dma((5,)),
        ],
        compiler_params=pltpu.CompilerParams(
            collective_id=0, has_side_effects=True, vmem_limit_bytes=VMEM_BYTES - held),
    )(grad_bucket.reshape(2, 2, nz, 2, rows, columns), parameters[0], row_state, column_state)
    new, row, col, full = pl.pallas_call(
        functools.partial(write_out, nz),
        out_shape=tuple(jax.ShapeDtypeStruct(*shape) for shape in shapes),
        in_specs=[vmem] * 4,
        out_specs=(hbm,) * 4,
        scratch_shapes=[dma((4,))],
        compiler_params=pltpu.CompilerParams(vmem_limit_bytes=4 * 1024 * 1024),
    )(*[pltpu.with_memory_space_constraint(result, pltpu.VMEM) for result in results])
    return (new[None], row, col, full.reshape(full_width, columns))


def solution(mesh):
    nx, nz, ny = (mesh.shape[a] for a in AXES)
    in_specs = (
        P(AXES, None, None, None),
        P(None, AXES, None),
        P(None, AXES),
        P(),
    )
    out_specs = (P(None, AXES, None), P(None, AXES), P(), P())
    fits = nx == 4 and ny == 2 and nz == 4

    def body(grad_bucket, parameters, row_state, column_state):
        if fits and grad_bucket.shape[1] == 1 and parameters.shape[1] % TILE == 0 and parameters.shape[1] >= 2 * TILE and grad_bucket.shape[3] % 1024 == 0:
            return fused(nx, nz, grad_bucket, parameters, row_state, column_state)
        return shards(grad_bucket, parameters, row_state, column_state)

    return jax.shard_map(body, mesh=mesh, in_specs=in_specs, out_specs=out_specs, check_vma=False)
```

```python
import functools
import math

import jax
import jax.numpy as jnp
from jax import lax
from jax.experimental import pallas as pl
from jax.experimental.pallas import tpu as pltpu
from jax.sharding import PartitionSpec as P

beta_two = 0.8
step_size = 0.5
AXES = ("gx", "gy", "gz")
TILE = 16
VMEM_BYTES = 67043328 - 131072


def shards(grad_bucket, parameters, row_state, column_state):
    local_grad = grad_bucket[0].astype(jnp.float32)
    layer_count, full_width, columns = local_grad.shape
    summed = lax.psum_scatter(local_grad, AXES, scatter_dimension=1, tiled=True)
    clip_level = 0.5 * math.sqrt(layer_count * full_width * columns)
    squares = summed * summed
    norm_square = lax.psum(jnp.sum(squares), AXES)
    factor = jnp.minimum(jnp.float32(1.0), clip_level / jnp.sqrt(norm_square + 1e-06))
    clipped = factor * summed
    clipped_square = clipped * clipped
    row_next = beta_two * row_state + (1.0 - beta_two) * jnp.mean(clipped_square, axis=2)
    column_part, row_total = lax.psum((jnp.sum(clipped_square, axis=1), jnp.sum(row_next, axis=1)), AXES)
    column_next = beta_two * column_state + (1.0 - beta_two) * column_part / full_width
    row_average = row_total / full_width
    second = row_next[:, :, None] * column_next[:, None, :] / row_average[:, None, None]
    update = clipped / jnp.sqrt(second)
    new_parameters = (parameters.astype(jnp.float32) - step_size * update).astype(jnp.bfloat16)
    first_layer = lax.all_gather(new_parameters[0], AXES, axis=0, tiled=True)
    return (new_parameters, row_next, column_next, first_layer)


def flip(index, mask, size):
    out, bit = 0, 1
    while bit < size:
        out = out + bit * (((index // bit) % 2 + (mask // bit) % 2) % 2)
        bit *= 2
    return out


def kernel(nx, nz, grad, params_in, row_in, col_in, new_ref, row_ref, col_ref, full,
           lg, cr, rx, rz, rc, unit, sums_of, params_of, info, scale, state_down, sum_down, st, st1, tot, st2, row_state, col_state,
           lsem, isem, cs, cfr, cvr, fs, fr, hr, zs, zr, ks, kr, s1s, s1r, s2s, s2r,
           ns, nr, nzs, nzr, ins, inr):
    gx, z, y = lax.axis_index("gx"), lax.axis_index("gy"), lax.axis_index("gz")
    x, c = gx // 2, gx % 2
    rows, columns = new_ref.shape
    params, sums = params_of.at[0], sums_of.at[0]
    lane = columns // 8
    stat_width = st.shape[1]
    full_width = rows * 4 * nz * 2
    core_peer = (x * 2 + 1 - c, z, y)
    x_peer = ((1 - x) * 2 + c, z, y)
    y_peer = (gx, z, 1 - y)
    tiles = rows // TILE
    f32, bf16 = jnp.float32, jnp.bfloat16
    scope = jax.named_scope
    blocks = [(1 - x, 1 - y), (1 - x, y), (x, 1 - y), (x, y)]

    def regions(cut, middle_lane):
        return ([(0, cut, 0, 6), (cut, tiles, 0, 7)], [(0, cut, 6, 8), (cut, tiles, 7, 8)],
                [(0, tiles, 0, middle_lane), (0, tiles, middle_lane, 8)])

    out_row = (tiles * 4 + 3) // 7
    cut_row = (tiles * 4 + 3) // 7
    parts, strips, halves = regions(cut_row, 4)
    out_parts, out_strips, out_halves = regions(out_row, 4)

    def area(regions):
        return sum((b - a) * (e - d) for a, b, d, e in regions)

    def at(region, shift=0):
        a, b, d, e = region
        return pl.ds(a * TILE, (b - a) * TILE), pl.ds((d - shift) * lane, (e - d) * lane)

    def spans(t):
        return halves if t == 0 else parts[::-1] if t % 2 else parts

    def zof(t):
        return flip(z, t, nz)

    inside = (z + z // 2) % 2
    near, middle = (gx, zof(1), y), (gx, zof(3), y)
    origin = [z, zof(1), flip(z, 2 + inside, nz), flip(z, 3 - inside, nz)]

    def on_end(step):
        pl.when(inside == 0)(step)

    def on_inner(step):
        pl.when(inside == 1)(step)

    def rdma(src, dst, ssem, rsem, peer):
        return pltpu.make_async_remote_copy(
            src_ref=src, dst_ref=dst, send_sem=ssem, recv_sem=rsem,
            device_id=peer, device_id_type=pl.DeviceIdType.MESH)

    def take_recv(view, sem):
        rdma(view, view, sem, sem, core_peer).wait_recv()

    def take_send(view, sem):
        rdma(view, view, sem, sem, core_peer).wait_send()

    def some(count):
        return unit.at[pl.ds(0, count)]

    first = 3
    loads = {t: pltpu.make_async_copy(grad.at[:, c, zof(t)], lg.at[t], lsem.at[t]) for t in (3, 2, 1, 0)}
    for t in loads:
        loads[t].start()
    small = [pltpu.make_async_copy(src, dst, isem.at[k]) for k, (src, dst) in enumerate(
        [(params_in, params), (row_in, row_state), (col_in, col_state)])]
    for copy in small:
        copy.start()

    barrier = pltpu.get_barrier_semaphore()
    plane = [((gx + a) % nx, z, (y + b) % 2) for a in range(nx) for b in range(2) if (a, b) != (0, 0)]
    line = [(gx, zof(t), y) for t in range(1, nz)]
    for peer in line + plane:
        pl.semaphore_signal(barrier, inc=1, device_id=peer, device_id_type=pl.DeviceIdType.MESH)
    with scope("barrier"):
        pl.semaphore_wait(barrier, len(plane) + len(line))

    for k, (bx, by) in enumerate(blocks):
        rdma(grad.at[bx, 1 - c, zof(first), by], cr.at[first, bx, by], cs, cfr.at[k], core_peer).start()
    for t in (2, 1, 0):
        rdma(grad.at[:, 1 - c, zof(t)], cr.at[t], cs, cvr.at[t], core_peer).start()

    X, Y, NEAR, MIDDLE = 1, 2, 3, 4

    def send_plane(src, dst, swap, a=0, b=tiles):
        for region, (slot, peer) in zip(out_halves, [(X, x_peer), (Y, y_peer)] if swap else [(Y, y_peer), (X, x_peer)]):
            r, l = at((a, b) + region[2:])
            rdma(src.at[r, l], dst.at[slot, r, l], ns, nr.at[1 if swap else 0], peer).start()

    def send_near(src, dst, slot, peer, regions):
        for region in regions:
            r, l = at(region)
            rdma(src.at[r, l], dst.at[slot, r, l], nzs, nzr.at[slot - NEAR], peer).start()

    early = out_row
    if early:
        send_plane(params_in, params_of, True, 0, early)

    @on_inner
    def _():
        send_near(params_in, params_of, NEAR, near, out_parts)
        send_near(params_in, params_of, MIDDLE, middle, out_parts)

    on_end(lambda: send_near(params_in, params_of, NEAR, near, out_parts[1:]))

    def add(*terms):
        total = terms[0].astype(f32)
        for term in terms[1:]:
            total = total + term.astype(f32)
        return total

    def over(region, step, shift=0):
        a, b, d, e = region

        @pl.loop(a, b, unroll=True)
        def _(i):
            step(pl.ds(pl.multiple_of(i * TILE, TILE), TILE), pl.ds(d * lane, (e - d) * lane),
                 pl.ds((d - shift) * lane, (e - d) * lane))

    whole = (0, tiles, 0, 8)

    def pair_sum(t, bx, by):
        def step(r, l, _):
            lg[t, bx, by, r, l] = add(lg[t, bx, by, r, l], cr[t, bx, by, r, l]).astype(bf16)
        over(whole, step)

    def cross(t):
        return fs.at[1 if t else 0]

    def send(t, bx, by, slot, region, sem, peer):
        r, l = at(region)
        rdma(lg.at[t, bx, by, r, l], rx.at[t, slot, r, l], cross(t), sem.at[t], peer).start()

    def send_f(t):
        a, b = spans(t)
        send(t, 1 - x, 1 - y, 0, a, fr, x_peer)
        send(t, 1 - x, 1 - y, 0, b, fr, y_peer)

    def send_ga(t):
        send(t, 1 - x, y, 1, spans(t)[0], hr, x_peer)

    def send_gb(t):
        send(t, x, 1 - y, 1, spans(t)[1], hr, y_peer)

    def send_g(t):
        send_ga(t)
        send_gb(t)

    side = [1 - x, x]

    def send_strip(t, slot, peer, h):
        for region in strips:
            r, l = at(region)
            _, m = at(region, 6)
            rdma(lg.at[t, side[h], :, r, l], rc.at[slot, h, :, r, m], ks, kr.at[slot, h], peer).start()

    def send_strips(t, slot, peer):
        for h in range(2):
            send_strip(t, slot, peer, h)

    def take_strips(h, *slots):
        for slot in slots:
            with scope(f"line{slot}_{h}"):
                take_recv(some(2 * area(strips)), kr.at[slot, h])

    def strip_add(t, h, *slots):
        for by in range(2):
            def step(r, l, m):
                lg[t, side[h], by, r, l] = add(
                    lg[t, side[h], by, r, l], *[rc[slot, h, by, r, m] for slot in slots]).astype(bf16)
            for region in strips:
                over(region, step, 6)

    def relay(came, t, slot, peer):
        for h in range(2):
            take_strips(h, came)
            strip_add(t, h, came)
            send_strip(t, slot, peer, h)

    def stage_pair(t):
        with scope(f"pair{t}"):
            take_recv(cr.at[t], cvr.at[t])
            loads[t].wait()
            for bx, by in blocks:
                pair_sum(t, bx, by)

    def stage_first(t):
        a, b = spans(t)
        with scope(f"f{t}"):
            take_recv(some(area(spans(t))), fr.at[t])

        def step_a(r, l, _):
            lg[t, x, 1 - y, r, l] = add(lg[t, x, 1 - y, r, l], rx[t, 0, r, l]).astype(bf16)

        def step_b(r, l, _):
            lg[t, 1 - x, y, r, l] = add(lg[t, 1 - x, y, r, l], rx[t, 0, r, l]).astype(bf16)
        over(a, step_a)
        send(t, x, 1 - y, 2, a, hr, y_peer)
        over(b, step_b)
        send(t, 1 - x, y, 2, b, hr, x_peer)

    def stage_second(t):
        with scope(f"h{t}"):
            take_recv(some(2 * area(spans(t))), hr.at[t])

    def send_far(t, slot, peer, p):
        r, l = at(parts[p])
        rdma(lg.at[t, x, y, r, l], rz.at[slot, r, l], zs, zr.at[slot, p], peer).start()

    def take_far(slot, p):
        with scope(f"far{slot}_{p}"):
            take_recv(some(area(parts[p:p + 1])), zr.at[slot, p])

    def second_add(t, p, *slots):
        def step(r, l, _):
            lg[t, x, y, r, l] = add(lg[t, x, y, r, l], rx[t, 1, r, l], rx[t, 2, r, l],
                                    *[rz[slot, r, l] for slot in slots]).astype(bf16)
        over(parts[p], step)

    loads[first].wait()
    for k, (bx, by) in enumerate(blocks):
        with scope(f"core{k}"):
            take_recv(cr.at[first, bx, by], cfr.at[k])
        pair_sum(first, bx, by)
        if k == 0:
            send_f(first)
        elif k == 1:
            send_ga(first)
            on_end(lambda: send_strip(3, 3, near, 0))
        elif k == 2:
            send_gb(first)
        else:
            on_end(lambda: send_strip(3, 3, near, 1))
    stage_pair(2)
    on_end(lambda: send_strips(2, 2, near))
    send_f(2)
    stage_first(3)
    send_g(2)
    stage_pair(1)
    on_end(lambda: send_strips(1, 1, near))
    send_f(1)
    on_inner(lambda: relay(3, 2, 4, middle))
    stage_pair(0)

    @on_end
    def _():
        rz[5] = jnp.zeros((rows, columns), bf16)

    stage_first(2)
    send_g(1)
    on_inner(lambda: relay(2, 3, 5, middle))
    stage_second(3)
    for p in range(2):
        second_add(3, p)
        on_end(lambda: send_far(3, 3, near, p))
    on_inner(lambda: relay(4, 1, 0, near))
    stage_first(1)

    @on_end
    def _():
        stage_second(2)
        for p in range(2):
            second_add(2, p)
            send_far(2, 2, near, p)
        for h in range(2):
            take_strips(h, 0)
            strip_add(0, h, 0)

    @on_inner
    def _():
        for h in range(2):
            take_strips(h, 1, 5)
            strip_add(0, h, 1, 5)

    send_f(0)
    send_g(0)

    @on_inner
    def _():
        stage_second(2)
        for p in range(2):
            take_far(3, p)
            second_add(2, p, 3)
            send_far(2, 4, middle, p)

    def pass_far_sum(p):
        take_far(2, p)

        def step(r, l, _):
            lg[3, x, y, r, l] = add(lg[3, x, y, r, l], rz[2, r, l]).astype(bf16)
        over(parts[p], step)
        send_far(3, 5, middle, p)

    stage_second(1)

    @on_end
    def _():
        for p in range(2):
            second_add(1, p)
            send_far(1, 1, near, p)

    def pass_near_sum(p):
        take_far(4, p)
        second_add(1, p, 4)
        send_far(1, 1, near, p)

    @on_inner
    def _():
        pass_far_sum(0)
        pass_near_sum(0)

    stage_first(0)
    for copy in small:
        copy.wait()
    send_plane(params, params_of, False)

    @on_inner
    def _():
        pass_far_sum(1)
        pass_near_sum(1)

    on_end(lambda: send_near(params, params_of, NEAR, near, out_parts[:1]))
    info[0, 0:1, :] = row_state[...]
    st[:, columns:] = jnp.broadcast_to(jnp.sum(row_state[...], axis=1, keepdims=True), (1, stat_width - columns))
    stage_second(0)
    for p in range(2):
        take_far(1, p)

    @on_inner
    def _():
        for p in range(2):
            take_far(5, p)

    with scope("final"):
        cuts = [(0, 6), (6, 7), (7, 8)]
        squares = [None] * len(cuts)
        row_sums = []
        for i in range(tiles):
            r = pl.ds(i * TILE, TILE)
            row_sum = 0.0
            for k, (d, e) in enumerate(cuts):
                l = pl.ds(d * lane, (e - d) * lane)
                terms = [lg[0, x, y, r, l], rx[0, 1, r, l], rx[0, 2, r, l]]
                if e <= parts[0 if i < cut_row else 1][3]:
                    terms += [rz[1, r, l], rz[5, r, l]]
                value = add(*terms)
                sums[r, l] = value.astype(bf16)
                value = value * value
                row_sum = row_sum + jnp.sum(value, axis=1, keepdims=True)
                squares[k] = value if squares[k] is None else squares[k] + value
            sum_down[0, r, :] = row_sum
        for (d, e), value in zip(cuts, squares):
            st[:, pl.ds(d * lane, (e - d) * lane)] = jnp.sum(value, axis=0, keepdims=True)

    me = gx * 2 + y
    for peer in plane:
        rdma(st, st1.at[me], s1s, s1r, peer).start()
    st1[me] = st[...]
    diagonal = lax.broadcasted_iota(jnp.int32, (rows, rows), 0) == lax.broadcasted_iota(jnp.int32, (rows, rows), 1)

    def turned(vector, axis):
        return jnp.sum(jnp.where(diagonal, jnp.broadcast_to(vector, (rows, rows)), 0.0), axis=axis, keepdims=True)

    info[0, 1:2, :] = turned(sum_down[0], 0)

    def send_info(slot, peer):
        rdma(info.at[0], info.at[slot], ins, inr.at[slot], peer).start()

    send_info(X, x_peer)
    send_info(Y, y_peer)
    send_info(NEAR, near)
    on_inner(lambda: send_info(MIDDLE, middle))
    send_plane(sums, sums_of, False)
    if early < tiles:
        send_plane(params, params_of, True, early, tiles)
    send_plane(sums, sums_of, True)

    def send_sums(pieces):
        send_near(sums, sums_of, NEAR, near, pieces)
        on_inner(lambda: send_near(sums, sums_of, MIDDLE, middle, pieces))

    send_sums([out_parts[0]] + ([(out_row, tiles - 1, 0, 7)] if out_row < tiles - 1 else []))
    take_send(cr, cs)
    take_send(some(3 * area(halves)), fs.at[0])
    take_send(some(9 * area(parts)), fs.at[1])
    take_send(some(3 * area(parts)), zs)
    take_send(some(12 * area(strips)), ks)
    with scope("stat1"):
        take_recv(st1.at[0:nx * 2 - 1], s1r)
    total = st1[0]
    for k in range(1, nx * 2):
        total = total + st1[k]
    tot[...] = total
    for t in range(1, nz):
        rdma(tot, st2.at[z], s2s, s2r, (gx, zof(t), y)).start()
    send_sums([(tiles - 1, tiles, 0, 7)])
    st2[z] = total
    state_down[0] = turned(row_state[...], 1)

    def turn_info(slot):
        with scope(f"info{slot}"):
            take_recv(info.at[slot], inr.at[slot])
        state_down[slot] = turned(info[slot, 0:1, :], 1)
        sum_down[slot] = turned(info[slot, 1:2, :], 1)

    for slot in (X, Y, NEAR):
        turn_info(slot)
    on_inner(lambda: turn_info(MIDDLE))
    with scope("stat2"):
        take_recv(st2.at[0:nz - 1], s2r)
    total = st2[0]
    for k in range(1, nz):
        total = total + st2[k]
    column_sum = total[:, 0:columns]
    norm_square = jnp.sum(column_sum, axis=1, keepdims=True)
    state_sum = total[:, columns:columns + 1]
    clip_level = 0.5 * math.sqrt(full_width * columns)
    factor = jnp.minimum(jnp.float32(1.0), clip_level / jnp.sqrt(norm_square + 1e-06))
    square_factor = factor * factor
    column_next = beta_two * col_state[...] + (1.0 - beta_two) * (square_factor * column_sum / full_width)
    row_average = (beta_two * state_sum + (1.0 - beta_two) * (square_factor * norm_square / columns)) / full_width
    col_scale = 1.0 / jnp.sqrt(column_next)

    def next_of(state, total):
        return beta_two * state + (1.0 - beta_two) * (square_factor * total / columns)

    def rate(slot):
        scale[slot] = (step_size * factor) / jnp.sqrt(next_of(state_down[slot], sum_down[slot]) / row_average)

    def update(slot, bx, u, by, regions):
        def step(r, l, _):
            new = params_of[slot, r, l].astype(f32) - (sums_of[slot, r, l].astype(f32) * scale[slot, r, :]) * col_scale_of(l)
            full[bx, c, u, by, r, l] = new.astype(bf16)
        for region in regions:
            over(region, step)

    def col_scale_of(l):
        return col_scale[:, l.start:l.start + l.size]

    gzs, gzr, qs, q1r, q2r, q3r, gks, gcs = zs, cfr, fs, fr, hr, cvr, ks, cs
    gcr = zr.at[0, 0]
    parts, strips, halves = out_parts, out_strips, out_halves

    def same(view, ssem, rsem, peer):
        rdma(view, view, ssem, rsem, peer).start()

    def moves(t):
        return qs.at[1 if t else 0]

    def piece(bx, u, by, region):
        r, l = at(region)
        return full.at[bx, c, u, by, r, l]

    def pass_core(t, bx, by):
        for region in parts if t else [whole]:
            same(piece(bx, origin[t], by, region), gcs, gcr, core_peer)

    def send_q1(t):
        u, (a, b) = origin[t], spans(t)
        same(piece(x, u, y, a), moves(t), q1r.at[t], y_peer)
        same(piece(x, u, y, b), moves(t), q1r.at[t], x_peer)

    def send_q2(t):
        u, (a, b) = origin[t], spans(t)
        same(piece(x, u, y, a), moves(t), q2r.at[t], x_peer)
        same(piece(x, u, y, b), moves(t), q2r.at[t], y_peer)
        pass_core(t, x, y)

    def send_own(t):
        send_q1(t)
        send_q2(t)

    def pass_far(t, slot, peer):
        for region in parts:
            same(piece(x, origin[t], y, region), gzs, gzr.at[slot], peer)

    def take_z(t):
        with scope(f"gz{t}"):
            take_recv(some(area(parts)), gzr.at[t])

    def gather_cross(t):
        u, (a, b) = origin[t], spans(t)
        with scope(f"q1_{t}"):
            take_recv(some(area(spans(t))), q1r.at[t])
        same(piece(x, u, 1 - y, a), moves(t), q3r.at[t], x_peer)
        same(piece(1 - x, u, y, b), moves(t), q3r.at[t], y_peer)

    def gather_side(t):
        with scope(f"q2_{t}"):
            take_recv(some(area(spans(t))), q2r.at[t])
        pass_core(t, 1 - x, y)
        pass_core(t, x, 1 - y)

    def gather_far(t):
        with scope(f"q3_{t}"):
            take_recv(some(area(spans(t))), q3r.at[t])
        pass_core(t, 1 - x, 1 - y)

    def each_strip(t, ssem, rsem, peer):
        for region in strips:
            r, l = at(region)
            same(full.at[:, c, origin[t], :, r, l], ssem, rsem, peer)

    def pass_strip(t, slot, peer):
        each_strip(t, gks, kr.at[slot, 0], peer)

    def take_strip(t):
        with scope(f"strip{t}"):
            take_recv(some(4 * area(strips)), kr.at[t, 0])
        each_strip(t, gcs, gcr, core_peer)

    low, high = halves
    rate(X)
    rate(Y)
    with scope("plane1"):
        take_recv(some(4 * area(halves[:1])), nr.at[0])
    update(Y, x, z, 1 - y, [low])
    update(X, 1 - x, z, y, [high])
    same(piece(x, z, 1 - y, low), moves(0), q3r.at[0], x_peer)
    same(piece(1 - x, z, y, high), moves(0), q3r.at[0], y_peer)
    rate(NEAR)
    with scope("near"):
        take_recv(some(2 * area(parts)), nzr.at[0])
    update(NEAR, x, origin[1], y, parts)
    on_inner(lambda: pass_far(1, 3, middle))
    send_own(1)

    @on_inner
    def _():
        rate(MIDDLE)
        with scope("middle"):
            take_recv(some(2 * area(parts)), nzr.at[1])
        update(MIDDLE, x, origin[2], y, parts)
        pass_far(2, 2, near)

    rate(0)
    update(0, x, z, y, [whole])
    pass_core(0, x, y)
    new_ref[...] = full[x, c, z, y]
    col_ref[...] = column_next
    row_ref[...] = next_of(info[0, 0:1, :], info[0, 1:2, :])
    with scope("plane2"):
        take_recv(some(4 * area(halves[:1])), nr.at[1])
    update(X, 1 - x, z, y, [low])
    update(Y, x, z, 1 - y, [high])
    pass_core(0, 1 - x, y)
    pass_core(0, x, 1 - y)
    gather_far(0)

    @on_inner
    def _():
        pass_strip(0, 2, middle)
        take_z(3)
        pass_far(3, 3, near)

    pass_strip(0, 1, near)
    gather_cross(1)
    on_end(lambda: take_z(2))
    send_own(2)
    gather_side(1)
    gather_far(1)

    @on_inner
    def _():
        take_strip(1)
        pass_strip(1, 3, middle)

    gather_cross(2)
    on_end(lambda: take_z(3))
    send_own(3)

    @on_inner
    def _():
        take_strip(2)
        pass_strip(2, 2, near)

    gather_side(2)
    gather_far(2)

    @on_inner
    def _():
        take_strip(3)
        pass_strip(3, 3, near)

    on_end(lambda: take_strip(1))
    gather_cross(3)
    on_end(lambda: take_strip(2))
    gather_side(3)
    on_end(lambda: take_strip(3))
    gather_far(3)

    with scope("finish"):
        take_send(st1.at[0:nx * 2 - 1], s1s)
        take_send(st2.at[0:nz - 1], s2s)
        take_send(some(area(halves)), qs.at[0])
        take_send(some(9 * area(parts)), qs.at[1])
        take_send(some(4 * area(halves)), ns)

        @on_end
        def _():
            take_send(some(2 * area(parts)), nzs)
            take_send(info.at[0:3], ins)
            take_send(some(4 * area(strips)), gks)

        @on_inner
        def _():
            take_send(some(4 * area(parts)), nzs)
            take_send(info.at[0:4], ins)
            take_send(some(3 * area(parts)), gzs)
            take_send(some(20 * area(strips)), gks)

        take_send(full.at[:, c], gcs)
        take_recv(full.at[:, c], gcr)


def write_out(nz, new, row, col, full, new_out, row_out, col_out, full_out, sem):
    pieces = [(full.at[a, b, u], full_out.at[a, b, u]) for a in range(2) for b in range(2) for u in range(nz)]
    copies = [pltpu.make_async_copy(src, dst, sem.at[0]) for src, dst in pieces]
    small = [pltpu.make_async_copy(src, dst, sem.at[k + 1])
             for k, (src, dst) in enumerate([(new, new_out), (row, row_out), (col, col_out)])]
    for copy in copies + small:
        copy.start()
    for copy in small:
        copy.wait()
    pltpu.make_async_copy(full, full_out, sem.at[0]).wait()


def fused(nx, nz, grad_bucket, parameters, row_state, column_state):
    _, _, full_width, columns = grad_bucket.shape
    rows = parameters.shape[1]
    lane = columns // 8
    bf16, f32 = jnp.bfloat16, jnp.float32
    vmem = pl.BlockSpec(memory_space=pltpu.VMEM)
    hbm = pl.BlockSpec(memory_space=pltpu.HBM)
    dma = pltpu.SemaphoreType.DMA
    one = dma(())
    shapes = [((rows, columns), bf16), ((1, rows), f32), ((1, columns), f32), ((2, 2, nz, 2, rows, columns), bf16)]
    held = 2 * columns * (rows + full_width) + 4 * (columns + -(-rows // 128) * 128)
    stat = columns + 128
    results = pl.pallas_call(
        functools.partial(kernel, nx, nz),
        out_shape=tuple(pltpu.VMEM(*shape) for shape in shapes),
        in_specs=[hbm] * 4,
        out_specs=(vmem,) * 4,
        scratch_shapes=[
            pltpu.VMEM((nz, 2, 2, rows, columns), bf16),
            pltpu.VMEM((nz, 2, 2, rows, columns), bf16),
            pltpu.VMEM((nz, 3, rows, columns), bf16),
            pltpu.VMEM((6, rows, columns), bf16),
            pltpu.VMEM((6, 2, 2, rows, 2 * lane), bf16),
            pltpu.VMEM((9 * 8 * (rows // TILE), TILE, lane), bf16),
            pltpu.VMEM((5, rows, columns), bf16),
            pltpu.VMEM((5, rows, columns), bf16),
            pltpu.VMEM((5, 2, rows), f32),
            pltpu.VMEM((5, rows, 1), f32),
            pltpu.VMEM((5, rows, 1), f32),
            pltpu.VMEM((5, rows, 1), f32),
            pltpu.VMEM((1, stat), f32),
            pltpu.VMEM((nx * 2, 1, stat), f32),
            pltpu.VMEM((1, stat), f32),
            pltpu.VMEM((nz, 1, stat), f32),
            pltpu.VMEM((1, rows), f32),
            pltpu.VMEM((1, columns), f32),
            dma((nz,)), dma((3,)), one, dma((4,)), dma((nz,)), dma((2,)), dma((nz,)), dma((nz,)),
            one, dma((6, 2)), one, dma((6, 2)), one, one, one, one,
            one, dma((2,)), one, dma((2,)), one, dma((5,)),
        ],
        compiler_params=pltpu.CompilerParams(
            collective_id=0, has_side_effects=True, vmem_limit_bytes=VMEM_BYTES - held),
    )(grad_bucket.reshape(2, 2, nz, 2, rows, columns), parameters[0], row_state, column_state)
    new, row, col, full = pl.pallas_call(
        functools.partial(write_out, nz),
        out_shape=tuple(jax.ShapeDtypeStruct(*shape) for shape in shapes),
        in_specs=[vmem] * 4,
        out_specs=(hbm,) * 4,
        scratch_shapes=[dma((4,))],
        compiler_params=pltpu.CompilerParams(vmem_limit_bytes=4 * 1024 * 1024),
    )(*[pltpu.with_memory_space_constraint(result, pltpu.VMEM) for result in results])
    return (new[None], row, col, full.reshape(full_width, columns))


def solution(mesh):
    nx, nz, ny = (mesh.shape[a] for a in AXES)
    in_specs = (
        P(AXES, None, None, None),
        P(None, AXES, None),
        P(None, AXES),
        P(),
    )
    out_specs = (P(None, AXES, None), P(None, AXES), P(), P())
    fits = nx == 4 and ny == 2 and nz == 4

    def body(grad_bucket, parameters, row_state, column_state):
        if fits and grad_bucket.shape[1] == 1 and parameters.shape[1] % TILE == 0 and parameters.shape[1] >= 2 * TILE and grad_bucket.shape[3] % 1024 == 0:
            return fused(nx, nz, grad_bucket, parameters, row_state, column_state)
        return shards(grad_bucket, parameters, row_state, column_state)

    return jax.shard_map(body, mesh=mesh, in_specs=in_specs, out_specs=out_specs, check_vma=False)
```

```python
import functools
import math

import jax
import jax.numpy as jnp
from jax import lax
from jax.experimental import pallas as pl
from jax.experimental.pallas import tpu as pltpu
from jax.sharding import PartitionSpec as P

beta_two = 0.8
step_size = 0.5
AXES = ("gx", "gy", "gz")
TILE = 16
VMEM_BYTES = 67043328 - 131072


def shards(grad_bucket, parameters, row_state, column_state):
    local_grad = grad_bucket[0].astype(jnp.float32)
    layer_count, full_width, columns = local_grad.shape
    summed = lax.psum_scatter(local_grad, AXES, scatter_dimension=1, tiled=True)
    clip_level = 0.5 * math.sqrt(layer_count * full_width * columns)
    squares = summed * summed
    norm_square = lax.psum(jnp.sum(squares), AXES)
    factor = jnp.minimum(jnp.float32(1.0), clip_level / jnp.sqrt(norm_square + 1e-06))
    clipped = factor * summed
    clipped_square = clipped * clipped
    row_next = beta_two * row_state + (1.0 - beta_two) * jnp.mean(clipped_square, axis=2)
    column_part, row_total = lax.psum((jnp.sum(clipped_square, axis=1), jnp.sum(row_next, axis=1)), AXES)
    column_next = beta_two * column_state + (1.0 - beta_two) * column_part / full_width
    row_average = row_total / full_width
    second = row_next[:, :, None] * column_next[:, None, :] / row_average[:, None, None]
    update = clipped / jnp.sqrt(second)
    new_parameters = (parameters.astype(jnp.float32) - step_size * update).astype(jnp.bfloat16)
    first_layer = lax.all_gather(new_parameters[0], AXES, axis=0, tiled=True)
    return (new_parameters, row_next, column_next, first_layer)


def flip(index, mask, size):
    out, bit = 0, 1
    while bit < size:
        out = out + bit * (((index // bit) % 2 + (mask // bit) % 2) % 2)
        bit *= 2
    return out


def kernel(nx, nz, grad, params_in, row_in, col_in, new_ref, row_ref, col_ref, full,
           lg, cr, rx, rz, rc, unit, sums_of, params_of, info, scale, state_down, sum_down, st, st1, tot, st2, row_state, col_state,
           lsem, isem, cs, cfr, cvr, fs, fr, hr, zs, zr, ks, kr, s1s, s1r, s2s, s2r,
           ns, nr, nzs, nzr, ins, inr):
    gx, z, y = lax.axis_index("gx"), lax.axis_index("gy"), lax.axis_index("gz")
    x, c = gx // 2, gx % 2
    rows, columns = new_ref.shape
    params, sums = params_of.at[0], sums_of.at[0]
    lane = columns // 8
    stat_width = st.shape[1]
    full_width = rows * 4 * nz * 2
    core_peer = (x * 2 + 1 - c, z, y)
    x_peer = ((1 - x) * 2 + c, z, y)
    y_peer = (gx, z, 1 - y)
    tiles = rows // TILE
    f32, bf16 = jnp.float32, jnp.bfloat16
    scope = jax.named_scope
    blocks = [(1 - x, 1 - y), (1 - x, y), (x, 1 - y), (x, y)]

    def regions(cut, middle_lane):
        return ([(0, cut, 0, 6), (cut, tiles, 0, 7)], [(0, cut, 6, 8), (cut, tiles, 7, 8)],
                [(0, tiles, 0, middle_lane), (0, tiles, middle_lane, 8)])

    cut_row = (tiles * 4 + 3) // 7
    parts, strips, halves = regions(cut_row, 4)
    out_parts, out_strips, out_halves = [(0, tiles, 0, 3), (0, tiles, 3, 6)], [(0, tiles, 6, 8)], halves
    out_flat = [(0, tiles, 0, 6)]

    def area(regions):
        return sum((b - a) * (e - d) for a, b, d, e in regions)

    def at(region, shift=0):
        a, b, d, e = region
        return pl.ds(a * TILE, (b - a) * TILE), pl.ds((d - shift) * lane, (e - d) * lane)

    def spans(t):
        return halves if t == 0 else parts[::-1] if t % 2 else parts

    def zof(t):
        return flip(z, t, nz)

    inside = (z + z // 2) % 2
    near, middle, far = (gx, zof(1), y), (gx, zof(3), y), (gx, zof(2), y)
    origin = [z, zof(1), flip(z, 2 + inside, nz), flip(z, 3 - inside, nz)]

    def on_end(step):
        pl.when(inside == 0)(step)

    def on_inner(step):
        pl.when(inside == 1)(step)

    def rdma(src, dst, ssem, rsem, peer):
        return pltpu.make_async_remote_copy(
            src_ref=src, dst_ref=dst, send_sem=ssem, recv_sem=rsem,
            device_id=peer, device_id_type=pl.DeviceIdType.MESH)

    def take_recv(view, sem):
        rdma(view, view, sem, sem, core_peer).wait_recv()

    def take_send(view, sem):
        rdma(view, view, sem, sem, core_peer).wait_send()

    def some(count):
        return unit.at[pl.ds(0, count)]

    first = 3
    loads = {t: pltpu.make_async_copy(grad.at[:, c, zof(t)], lg.at[t], lsem.at[t]) for t in (3, 2, 1, 0)}
    for t in loads:
        loads[t].start()
    small = [pltpu.make_async_copy(src, dst, isem.at[k]) for k, (src, dst) in enumerate(
        [(params_in, params), (row_in, row_state), (col_in, col_state)])]
    for copy in small:
        copy.start()

    barrier = pltpu.get_barrier_semaphore()
    plane = [((gx + a) % nx, z, (y + b) % 2) for a in range(nx) for b in range(2) if (a, b) != (0, 0)]
    line = [(gx, zof(t), y) for t in range(1, nz)]
    for peer in line + plane:
        pl.semaphore_signal(barrier, inc=1, device_id=peer, device_id_type=pl.DeviceIdType.MESH)
    with scope("barrier"):
        pl.semaphore_wait(barrier, len(plane) + len(line))

    for k, (bx, by) in enumerate(blocks):
        rdma(grad.at[bx, 1 - c, zof(first), by], cr.at[first, bx, by], cs, cfr.at[k], core_peer).start()
    for t in (2, 1, 0):
        rdma(grad.at[:, 1 - c, zof(t)], cr.at[t], cs, cvr.at[t], core_peer).start()

    X, Y, NEAR, MIDDLE = 1, 2, 3, 4

    def send_plane(src, dst, swap, a=0, b=tiles):
        for region, (slot, peer) in zip(out_halves, [(X, x_peer), (Y, y_peer)] if swap else [(Y, y_peer), (X, x_peer)]):
            r, l = at((a, b) + region[2:])
            rdma(src.at[r, l], dst.at[slot, r, l], ns, nr.at[1 if swap else 0], peer).start()

    def send_near(src, dst, slot, peer, regions):
        for region in regions:
            r, l = at(region)
            rdma(src.at[r, l], dst.at[slot, r, l], nzs, nzr.at[slot - NEAR], peer).start()

    early = (tiles * 4 + 3) // 7
    if early:
        send_plane(params_in, params_of, True, 0, early)

    @on_inner
    def _():
        send_near(params_in, params_of, NEAR, near, out_flat)
        send_near(params_in, params_of, MIDDLE, middle, out_flat)

    on_end(lambda: send_near(params_in, params_of, NEAR, near, out_parts[1:]))

    def add(*terms):
        total = terms[0].astype(f32)
        for term in terms[1:]:
            total = total + term.astype(f32)
        return total

    def over(region, step, shift=0):
        a, b, d, e = region

        @pl.loop(a, b, unroll=True)
        def _(i):
            step(pl.ds(pl.multiple_of(i * TILE, TILE), TILE), pl.ds(d * lane, (e - d) * lane),
                 pl.ds((d - shift) * lane, (e - d) * lane))

    whole = (0, tiles, 0, 8)

    def pair_sum(t, bx, by):
        def step(r, l, _):
            lg[t, bx, by, r, l] = add(lg[t, bx, by, r, l], cr[t, bx, by, r, l]).astype(bf16)
        over(whole, step)

    def cross(t):
        return fs.at[1 if t else 0]

    def send(t, bx, by, slot, region, sem, peer):
        r, l = at(region)
        rdma(lg.at[t, bx, by, r, l], rx.at[t, slot, r, l], cross(t), sem.at[t], peer).start()

    def send_f(t):
        a, b = spans(t)
        send(t, 1 - x, 1 - y, 0, a, fr, x_peer)
        send(t, 1 - x, 1 - y, 0, b, fr, y_peer)

    def send_ga(t):
        send(t, 1 - x, y, 1, spans(t)[0], hr, x_peer)

    def send_gb(t):
        send(t, x, 1 - y, 1, spans(t)[1], hr, y_peer)

    def send_g(t):
        send_ga(t)
        send_gb(t)

    side = [1 - x, x]

    def send_strip(t, slot, peer, h):
        for region in strips:
            r, l = at(region)
            _, m = at(region, 6)
            rdma(lg.at[t, side[h], :, r, l], rc.at[slot, h, :, r, m], ks, kr.at[slot, h], peer).start()

    def send_strips(t, slot, peer):
        for h in range(2):
            send_strip(t, slot, peer, h)

    def take_strips(h, *slots):
        for slot in slots:
            with scope(f"line{slot}_{h}"):
                take_recv(some(2 * area(strips)), kr.at[slot, h])

    def strip_add(t, h, *slots):
        for by in range(2):
            def step(r, l, m):
                lg[t, side[h], by, r, l] = add(
                    lg[t, side[h], by, r, l], *[rc[slot, h, by, r, m] for slot in slots]).astype(bf16)
            for region in strips:
                over(region, step, 6)

    def relay(came, t, slot, peer):
        for h in range(2):
            take_strips(h, came)
            strip_add(t, h, came)
            send_strip(t, slot, peer, h)

    def stage_pair(t):
        with scope(f"pair{t}"):
            take_recv(cr.at[t], cvr.at[t])
            loads[t].wait()
            for bx, by in blocks:
                pair_sum(t, bx, by)

    def stage_first(t):
        a, b = spans(t)
        with scope(f"f{t}"):
            take_recv(some(area(spans(t))), fr.at[t])

        def step_a(r, l, _):
            lg[t, x, 1 - y, r, l] = add(lg[t, x, 1 - y, r, l], rx[t, 0, r, l]).astype(bf16)

        def step_b(r, l, _):
            lg[t, 1 - x, y, r, l] = add(lg[t, 1 - x, y, r, l], rx[t, 0, r, l]).astype(bf16)
        over(a, step_a)
        send(t, x, 1 - y, 2, a, hr, y_peer)
        over(b, step_b)
        send(t, 1 - x, y, 2, b, hr, x_peer)

    def stage_second(t):
        with scope(f"h{t}"):
            take_recv(some(2 * area(spans(t))), hr.at[t])

    def send_far(t, slot, peer, p):
        r, l = at(parts[p])
        rdma(lg.at[t, x, y, r, l], rz.at[slot, r, l], zs, zr.at[slot, p], peer).start()

    def take_far(slot, p):
        with scope(f"far{slot}_{p}"):
            take_recv(some(area(parts[p:p + 1])), zr.at[slot, p])

    def second_add(t, p, *slots):
        def step(r, l, _):
            lg[t, x, y, r, l] = add(lg[t, x, y, r, l], rx[t, 1, r, l], rx[t, 2, r, l],
                                    *[rz[slot, r, l] for slot in slots]).astype(bf16)
        over(parts[p], step)

    loads[first].wait()
    for k, (bx, by) in enumerate(blocks):
        with scope(f"core{k}"):
            take_recv(cr.at[first, bx, by], cfr.at[k])
        pair_sum(first, bx, by)
        if k == 0:
            send_f(first)
        elif k == 1:
            send_ga(first)
            on_end(lambda: send_strip(3, 3, near, 0))
        elif k == 2:
            send_gb(first)
        else:
            on_end(lambda: send_strip(3, 3, near, 1))
    stage_pair(2)
    on_end(lambda: send_strips(2, 2, near))
    send_f(2)
    stage_first(3)
    send_g(2)
    stage_pair(1)
    on_end(lambda: send_strips(1, 1, near))
    send_f(1)
    on_inner(lambda: relay(3, 2, 4, middle))
    stage_pair(0)

    @on_end
    def _():
        rz[5] = jnp.zeros((rows, columns), bf16)

    stage_first(2)
    send_g(1)
    on_inner(lambda: relay(2, 3, 5, middle))
    stage_second(3)
    for p in range(2):
        second_add(3, p)
        on_end(lambda: send_far(3, 3, near, p))
    on_inner(lambda: relay(4, 1, 0, near))
    stage_first(1)

    @on_end
    def _():
        stage_second(2)
        for p in range(2):
            second_add(2, p)
            send_far(2, 2, near, p)
        for h in range(2):
            take_strips(h, 0)
            strip_add(0, h, 0)

    @on_inner
    def _():
        for h in range(2):
            take_strips(h, 1, 5)
            strip_add(0, h, 1, 5)

    send_f(0)
    send_g(0)

    @on_inner
    def _():
        stage_second(2)
        for p in range(2):
            take_far(3, p)
            second_add(2, p, 3)
            send_far(2, 4, middle, p)

    def pass_far_sum(p):
        take_far(2, p)

        def step(r, l, _):
            lg[3, x, y, r, l] = add(lg[3, x, y, r, l], rz[2, r, l]).astype(bf16)
        over(parts[p], step)
        send_far(3, 5, middle, p)

    stage_second(1)

    @on_end
    def _():
        for p in range(2):
            second_add(1, p)
            send_far(1, 1, near, p)

    def pass_near_sum(p):
        take_far(4, p)
        second_add(1, p, 4)
        send_far(1, 1, near, p)

    @on_inner
    def _():
        pass_far_sum(0)
        pass_near_sum(0)

    stage_first(0)
    for copy in small:
        copy.wait()
    send_plane(params, params_of, False)

    @on_inner
    def _():
        pass_far_sum(1)
        pass_near_sum(1)
        send_near(params, params_of, MIDDLE, far, out_flat)

    on_end(lambda: send_near(params, params_of, NEAR, near, out_parts[:1]))
    info[0, 0:1, :] = row_state[...]
    st[:, columns:] = jnp.broadcast_to(jnp.sum(row_state[...], axis=1, keepdims=True), (1, stat_width - columns))
    stage_second(0)
    for p in range(2):
        take_far(1, p)

    @on_inner
    def _():
        for p in range(2):
            take_far(5, p)

    with scope("final"):
        cuts = [(0, 6), (6, 7), (7, 8)]
        squares = [None] * len(cuts)
        row_sums = []
        for i in range(tiles):
            r = pl.ds(i * TILE, TILE)
            row_sum = 0.0
            for k, (d, e) in enumerate(cuts):
                l = pl.ds(d * lane, (e - d) * lane)
                terms = [lg[0, x, y, r, l], rx[0, 1, r, l], rx[0, 2, r, l]]
                if e <= parts[0 if i < cut_row else 1][3]:
                    terms += [rz[1, r, l], rz[5, r, l]]
                value = add(*terms)
                sums[r, l] = value.astype(bf16)
                value = value * value
                row_sum = row_sum + jnp.sum(value, axis=1, keepdims=True)
                squares[k] = value if squares[k] is None else squares[k] + value
            sum_down[0, r, :] = row_sum
        for (d, e), value in zip(cuts, squares):
            st[:, pl.ds(d * lane, (e - d) * lane)] = jnp.sum(value, axis=0, keepdims=True)

    me = gx * 2 + y
    for peer in plane:
        rdma(st, st1.at[me], s1s, s1r, peer).start()
    st1[me] = st[...]
    diagonal = lax.broadcasted_iota(jnp.int32, (rows, rows), 0) == lax.broadcasted_iota(jnp.int32, (rows, rows), 1)

    def turned(vector, axis):
        return jnp.sum(jnp.where(diagonal, jnp.broadcast_to(vector, (rows, rows)), 0.0), axis=axis, keepdims=True)

    info[0, 1:2, :] = turned(sum_down[0], 0)

    def send_info(slot, peer):
        rdma(info.at[0], info.at[slot], ins, inr.at[slot], peer).start()

    send_info(X, x_peer)
    send_info(Y, y_peer)
    send_info(NEAR, near)

    @on_inner
    def _():
        send_info(MIDDLE, middle)
        send_info(MIDDLE, far)

    send_plane(sums, sums_of, False)
    if early < tiles:
        send_plane(params, params_of, True, early, tiles)
    send_plane(sums, sums_of, True)

    def send_sums(pieces):
        send_near(sums, sums_of, NEAR, near, pieces)
        on_inner(lambda: send_near(sums, sums_of, MIDDLE, middle, pieces))

    late = (tiles * 3) // 7
    send_sums([out_parts[0], (0, tiles - late, 3, 6)])
    take_send(cr, cs)
    take_send(some(3 * area(halves)), fs.at[0])
    take_send(some(9 * area(parts)), fs.at[1])
    take_send(some(3 * area(parts)), zs)
    take_send(some(12 * area(strips)), ks)
    with scope("stat1"):
        take_recv(st1.at[0:nx * 2 - 1], s1r)
    total = st1[0]
    for k in range(1, nx * 2):
        total = total + st1[k]
    tot[...] = total
    for t in range(1, nz):
        rdma(tot, st2.at[z], s2s, s2r, (gx, zof(t), y)).start()
    if late:
        send_sums([(tiles - late, tiles, 3, 6)])
    on_inner(lambda: send_near(sums, sums_of, MIDDLE, far, out_flat))
    st2[z] = total
    state_down[0] = turned(row_state[...], 1)

    def turn_info(slot):
        with scope(f"info{slot}"):
            take_recv(info.at[slot], inr.at[slot])
        state_down[slot] = turned(info[slot, 0:1, :], 1)
        sum_down[slot] = turned(info[slot, 1:2, :], 1)

    for slot in (X, Y, NEAR, MIDDLE):
        turn_info(slot)
    with scope("stat2"):
        take_recv(st2.at[0:nz - 1], s2r)
    total = st2[0]
    for k in range(1, nz):
        total = total + st2[k]
    column_sum = total[:, 0:columns]
    norm_square = jnp.sum(column_sum, axis=1, keepdims=True)
    state_sum = total[:, columns:columns + 1]
    clip_level = 0.5 * math.sqrt(full_width * columns)
    factor = jnp.minimum(jnp.float32(1.0), clip_level / jnp.sqrt(norm_square + 1e-06))
    square_factor = factor * factor
    column_next = beta_two * col_state[...] + (1.0 - beta_two) * (square_factor * column_sum / full_width)
    row_average = (beta_two * state_sum + (1.0 - beta_two) * (square_factor * norm_square / columns)) / full_width
    col_scale = 1.0 / jnp.sqrt(column_next)

    def next_of(state, total):
        return beta_two * state + (1.0 - beta_two) * (square_factor * total / columns)

    def rate(slot):
        scale[slot] = (step_size * factor) / jnp.sqrt(next_of(state_down[slot], sum_down[slot]) / row_average)

    def update(slot, bx, u, by, regions):
        def step(r, l, _):
            new = params_of[slot, r, l].astype(f32) - (sums_of[slot, r, l].astype(f32) * scale[slot, r, :]) * col_scale_of(l)
            full[bx, c, u, by, r, l] = new.astype(bf16)
        for region in regions:
            over(region, step)

    def col_scale_of(l):
        return col_scale[:, l.start:l.start + l.size]

    gzs, gzr, qs, q1r, q2r, q3r, gks, gcs = zs, cfr, fs, fr, hr, cvr, ks, cs
    gcr = zr.at[0, 0]
    parts, strips, halves = out_parts, out_strips, out_halves

    def same(view, ssem, rsem, peer):
        rdma(view, view, ssem, rsem, peer).start()

    def moves(t):
        return qs.at[1 if t else 0]

    def piece(bx, u, by, region):
        r, l = at(region)
        return full.at[bx, c, u, by, r, l]

    def pass_core(t, bx, by):
        for region in out_flat if t else [whole]:
            same(piece(bx, origin[t], by, region), gcs, gcr, core_peer)

    def send_q1(t):
        u, (a, b) = origin[t], spans(t)
        same(piece(x, u, y, a), moves(t), q1r.at[t], y_peer)
        same(piece(x, u, y, b), moves(t), q1r.at[t], x_peer)

    def send_q2(t):
        u, (a, b) = origin[t], spans(t)
        same(piece(x, u, y, a), moves(t), q2r.at[t], x_peer)
        same(piece(x, u, y, b), moves(t), q2r.at[t], y_peer)
        pass_core(t, x, y)

    def send_own(t):
        send_q1(t)
        send_q2(t)

    def pass_far(t, slot, peer):
        for region in out_flat:
            same(piece(x, origin[t], y, region), gzs, gzr.at[slot], peer)

    def take_z(t):
        with scope(f"gz{t}"):
            take_recv(some(area(parts)), gzr.at[t])

    def gather_cross(t):
        u, (a, b) = origin[t], spans(t)
        with scope(f"q1_{t}"):
            take_recv(some(area(spans(t))), q1r.at[t])
        same(piece(x, u, 1 - y, a), moves(t), q3r.at[t], x_peer)
        same(piece(1 - x, u, y, b), moves(t), q3r.at[t], y_peer)

    def gather_side(t):
        with scope(f"q2_{t}"):
            take_recv(some(area(spans(t))), q2r.at[t])
        pass_core(t, 1 - x, y)
        pass_core(t, x, 1 - y)

    def gather_far(t):
        with scope(f"q3_{t}"):
            take_recv(some(area(spans(t))), q3r.at[t])
        pass_core(t, 1 - x, 1 - y)

    def each_strip(t, p, ssem, rsem, peer):
        r, l = at(strips[0])
        for bx, by in [(1 - x, 1 - y)] if p else [(x, y), (1 - x, y), (x, 1 - y)]:
            same(full.at[bx, c, origin[t], by, r, l], ssem, rsem, peer)

    def pass_strip(t, p, slot, peer):
        each_strip(t, p, gks, kr.at[slot, p], peer)

    def take_strip(t, p):
        with scope(f"strip{t}_{p}"):
            take_recv(some((1 if p else 3) * area(strips)), kr.at[t, p])
        each_strip(t, p, gcs, gcr, core_peer)

    def own_strip(p):
        pass_strip(0, p, 1, near)
        on_inner(lambda: pass_strip(0, p, 2, middle))

    low, high = halves
    rate(X)
    rate(Y)
    with scope("plane1"):
        take_recv(some(4 * area(halves[:1])), nr.at[0])
    update(Y, x, z, 1 - y, [low])
    update(X, 1 - x, z, y, [high])
    same(piece(x, z, 1 - y, low), moves(0), q3r.at[0], x_peer)
    same(piece(1 - x, z, y, high), moves(0), q3r.at[0], y_peer)
    rate(NEAR)
    with scope("near"):
        take_recv(some(2 * area(parts)), nzr.at[0])
    update(NEAR, x, origin[1], y, parts)
    on_inner(lambda: pass_far(1, 3, middle))
    send_own(1)

    rate(0)
    update(0, x, z, y, [whole])
    pass_core(0, x, y)
    new_ref[...] = full[x, c, z, y]
    col_ref[...] = column_next
    row_ref[...] = next_of(info[0, 0:1, :], info[0, 1:2, :])
    with scope("plane2"):
        take_recv(some(4 * area(halves[:1])), nr.at[1])
    update(X, 1 - x, z, y, [low])
    update(Y, x, z, 1 - y, [high])
    own_strip(0)
    pass_core(0, 1 - x, y)
    pass_core(0, x, 1 - y)
    rate(MIDDLE)
    with scope("middle"):
        take_recv(some(2 * area(parts)), nzr.at[1])
    update(MIDDLE, x, origin[2], y, parts)
    gather_far(0)
    own_strip(1)
    gather_cross(1)
    send_own(2)

    @on_inner
    def _():
        take_z(3)
        pass_far(3, 3, near)

    def relay_strip(t, p, slot, peer):
        take_strip(t, p)
        pass_strip(t, p, slot, peer)

    on_inner(lambda: relay_strip(1, 0, 3, middle))
    gather_side(1)
    gather_far(1)
    on_inner(lambda: relay_strip(1, 1, 3, middle))

    def pass_second():
        relay_strip(2, 0, 2, near)
        relay_strip(2, 1, 2, near)

    pl.when((inside == 1) & (c == 0))(pass_second)
    gather_cross(2)
    on_end(lambda: take_z(3))
    send_own(3)
    pl.when((inside == 1) & (c == 1))(pass_second)

    @on_inner
    def _():
        relay_strip(3, 0, 3, near)
        relay_strip(3, 1, 3, near)

    gather_side(2)
    gather_far(2)

    def end_strip(t):
        take_strip(t, 0)
        take_strip(t, 1)

    on_end(lambda: end_strip(1))
    gather_cross(3)
    on_end(lambda: end_strip(2))
    gather_side(3)
    on_end(lambda: end_strip(3))
    gather_far(3)

    with scope("finish"):
        take_send(st1.at[0:nx * 2 - 1], s1s)
        take_send(st2.at[0:nz - 1], s2s)
        take_send(some(area(halves)), qs.at[0])
        take_send(some(9 * area(parts)), qs.at[1])
        take_send(some(4 * area(halves)), ns)

        @on_end
        def _():
            take_send(some(2 * area(parts)), nzs)
            take_send(info.at[0:3], ins)
            take_send(some(4 * area(strips)), gks)

        @on_inner
        def _():
            take_send(some(6 * area(parts)), nzs)
            take_send(info, ins)
            take_send(some(2 * area(parts)), gzs)
            take_send(some(20 * area(strips)), gks)

        take_send(full.at[:, c], gcs)
        take_recv(full.at[:, c], gcr)


def write_out(nz, new, row, col, full, new_out, row_out, col_out, full_out, sem):
    pieces = [(full.at[a, b, u], full_out.at[a, b, u]) for a in range(2) for b in range(2) for u in range(nz)]
    copies = [pltpu.make_async_copy(src, dst, sem.at[0]) for src, dst in pieces]
    small = [pltpu.make_async_copy(src, dst, sem.at[k + 1])
             for k, (src, dst) in enumerate([(new, new_out), (row, row_out), (col, col_out)])]
    for copy in copies + small:
        copy.start()
    for copy in small:
        copy.wait()
    pltpu.make_async_copy(full, full_out, sem.at[0]).wait()


def fused(nx, nz, grad_bucket, parameters, row_state, column_state):
    _, _, full_width, columns = grad_bucket.shape
    rows = parameters.shape[1]
    lane = columns // 8
    bf16, f32 = jnp.bfloat16, jnp.float32
    vmem = pl.BlockSpec(memory_space=pltpu.VMEM)
    hbm = pl.BlockSpec(memory_space=pltpu.HBM)
    dma = pltpu.SemaphoreType.DMA
    one = dma(())
    shapes = [((rows, columns), bf16), ((1, rows), f32), ((1, columns), f32), ((2, 2, nz, 2, rows, columns), bf16)]
    held = 2 * columns * (rows + full_width) + 4 * (columns + -(-rows // 128) * 128)
    stat = columns + 128
    results = pl.pallas_call(
        functools.partial(kernel, nx, nz),
        out_shape=tuple(pltpu.VMEM(*shape) for shape in shapes),
        in_specs=[hbm] * 4,
        out_specs=(vmem,) * 4,
        scratch_shapes=[
            pltpu.VMEM((nz, 2, 2, rows, columns), bf16),
            pltpu.VMEM((nz, 2, 2, rows, columns), bf16),
            pltpu.VMEM((nz, 3, rows, columns), bf16),
            pltpu.VMEM((6, rows, columns), bf16),
            pltpu.VMEM((6, 2, 2, rows, 2 * lane), bf16),
            pltpu.VMEM((9 * 8 * (rows // TILE), TILE, lane), bf16),
            pltpu.VMEM((5, rows, columns), bf16),
            pltpu.VMEM((5, rows, columns), bf16),
            pltpu.VMEM((5, 2, rows), f32),
            pltpu.VMEM((5, rows, 1), f32),
            pltpu.VMEM((5, rows, 1), f32),
            pltpu.VMEM((5, rows, 1), f32),
            pltpu.VMEM((1, stat), f32),
            pltpu.VMEM((nx * 2, 1, stat), f32),
            pltpu.VMEM((1, stat), f32),
            pltpu.VMEM((nz, 1, stat), f32),
            pltpu.VMEM((1, rows), f32),
            pltpu.VMEM((1, columns), f32),
            dma((nz,)), dma((3,)), one, dma((4,)), dma((nz,)), dma((2,)), dma((nz,)), dma((nz,)),
            one, dma((6, 2)), one, dma((6, 2)), one, one, one, one,
            one, dma((2,)), one, dma((2,)), one, dma((5,)),
        ],
        compiler_params=pltpu.CompilerParams(
            collective_id=0, has_side_effects=True, vmem_limit_bytes=VMEM_BYTES - held),
    )(grad_bucket.reshape(2, 2, nz, 2, rows, columns), parameters[0], row_state, column_state)
    new, row, col, full = pl.pallas_call(
        functools.partial(write_out, nz),
        out_shape=tuple(jax.ShapeDtypeStruct(*shape) for shape in shapes),
        in_specs=[vmem] * 4,
        out_specs=(hbm,) * 4,
        scratch_shapes=[dma((4,))],
        compiler_params=pltpu.CompilerParams(vmem_limit_bytes=4 * 1024 * 1024),
    )(*[pltpu.with_memory_space_constraint(result, pltpu.VMEM) for result in results])
    return (new[None], row, col, full.reshape(full_width, columns))


def solution(mesh):
    nx, nz, ny = (mesh.shape[a] for a in AXES)
    in_specs = (
        P(AXES, None, None, None),
        P(None, AXES, None),
        P(None, AXES),
        P(),
    )
    out_specs = (P(None, AXES, None), P(None, AXES), P(), P())
    fits = nx == 4 and ny == 2 and nz == 4

    def body(grad_bucket, parameters, row_state, column_state):
        if fits and grad_bucket.shape[1] == 1 and parameters.shape[1] % TILE == 0 and parameters.shape[1] >= 2 * TILE and grad_bucket.shape[3] % 1024 == 0:
            return fused(nx, nz, grad_bucket, parameters, row_state, column_state)
        return shards(grad_bucket, parameters, row_state, column_state)

    return jax.shard_map(body, mesh=mesh, in_specs=in_specs, out_specs=out_specs, check_vma=False)
```

```python
import functools
import math

import jax
import jax.numpy as jnp
from jax import lax
from jax.experimental import pallas as pl
from jax.experimental.pallas import tpu as pltpu
from jax.sharding import PartitionSpec as P

beta_two = 0.8
step_size = 0.5
AXES = ("gx", "gy", "gz")
TILE = 16
VMEM_BYTES = 67043328 - 131072


def shards(grad_bucket, parameters, row_state, column_state):
    local_grad = grad_bucket[0].astype(jnp.float32)
    layer_count, full_width, columns = local_grad.shape
    summed = lax.psum_scatter(local_grad, AXES, scatter_dimension=1, tiled=True)
    clip_level = 0.5 * math.sqrt(layer_count * full_width * columns)
    squares = summed * summed
    norm_square = lax.psum(jnp.sum(squares), AXES)
    factor = jnp.minimum(jnp.float32(1.0), clip_level / jnp.sqrt(norm_square + 1e-06))
    clipped = factor * summed
    clipped_square = clipped * clipped
    row_next = beta_two * row_state + (1.0 - beta_two) * jnp.mean(clipped_square, axis=2)
    column_part, row_total = lax.psum((jnp.sum(clipped_square, axis=1), jnp.sum(row_next, axis=1)), AXES)
    column_next = beta_two * column_state + (1.0 - beta_two) * column_part / full_width
    row_average = row_total / full_width
    second = row_next[:, :, None] * column_next[:, None, :] / row_average[:, None, None]
    update = clipped / jnp.sqrt(second)
    new_parameters = (parameters.astype(jnp.float32) - step_size * update).astype(jnp.bfloat16)
    first_layer = lax.all_gather(new_parameters[0], AXES, axis=0, tiled=True)
    return (new_parameters, row_next, column_next, first_layer)


def flip(index, mask, size):
    out, bit = 0, 1
    while bit < size:
        out = out + bit * (((index // bit) % 2 + (mask // bit) % 2) % 2)
        bit *= 2
    return out


def kernel(nx, nz, grad, params_in, row_in, col_in, new_ref, row_ref, col_ref, full,
           lg, cr, rx, rz, rc, unit, sums_of, params_of, info, scale, state_down, sum_down, st, st1, tot, st2, row_state, col_state,
           lsem, isem, cs, cfr, cvr, fs, fr, hr, zs, zr, ks, kr, s1s, s1r, s2s, s2r,
           ns, nr, nzs, nzr, ins, inr):
    gx, z, y = lax.axis_index("gx"), lax.axis_index("gy"), lax.axis_index("gz")
    x, c = gx // 2, gx % 2
    rows, columns = new_ref.shape
    params, sums = params_of.at[0], sums_of.at[0]
    lane = columns // 8
    stat_width = st.shape[1]
    full_width = rows * 4 * nz * 2
    core_peer = (x * 2 + 1 - c, z, y)
    x_peer = ((1 - x) * 2 + c, z, y)
    y_peer = (gx, z, 1 - y)
    tiles = rows // TILE
    f32, bf16 = jnp.float32, jnp.bfloat16
    scope = jax.named_scope
    blocks = [(1 - x, 1 - y), (1 - x, y), (x, 1 - y), (x, y)]

    def regions(cut, middle_lane):
        return ([(0, cut, 0, 6), (cut, tiles, 0, 7)], [(0, cut, 6, 8), (cut, tiles, 7, 8)],
                [(0, tiles, 0, middle_lane), (0, tiles, middle_lane, 8)])

    cut_row = (tiles * 4 + 3) // 7
    parts, strips, halves = regions(cut_row, 4)
    out_parts, out_strips, out_halves = [(0, tiles, 0, 3), (0, tiles, 3, 6)], [(0, tiles, 6, 8)], halves
    out_flat = [(0, tiles, 0, 6)]

    def area(regions):
        return sum((b - a) * (e - d) for a, b, d, e in regions)

    def at(region, shift=0):
        a, b, d, e = region
        return pl.ds(a * TILE, (b - a) * TILE), pl.ds((d - shift) * lane, (e - d) * lane)

    def spans(t):
        return halves if t == 0 else parts[::-1] if t % 2 else parts

    def zof(t):
        return flip(z, t, nz)

    inside = (z + z // 2) % 2
    near, middle, far = (gx, zof(1), y), (gx, zof(3), y), (gx, zof(2), y)
    origin = [z, zof(1), flip(z, 2 + inside, nz), flip(z, 3 - inside, nz)]

    def on_end(step):
        pl.when(inside == 0)(step)

    def on_inner(step):
        pl.when(inside == 1)(step)

    def rdma(src, dst, ssem, rsem, peer):
        return pltpu.make_async_remote_copy(
            src_ref=src, dst_ref=dst, send_sem=ssem, recv_sem=rsem,
            device_id=peer, device_id_type=pl.DeviceIdType.MESH)

    def take_recv(view, sem):
        rdma(view, view, sem, sem, core_peer).wait_recv()

    def take_send(view, sem):
        rdma(view, view, sem, sem, core_peer).wait_send()

    def some(count):
        return unit.at[pl.ds(0, count)]

    first = 3
    loads = {t: pltpu.make_async_copy(grad.at[:, c, zof(t)], lg.at[t], lsem.at[t]) for t in (3, 2, 1, 0)}
    for t in loads:
        loads[t].start()
    small = [pltpu.make_async_copy(src, dst, isem.at[k]) for k, (src, dst) in enumerate(
        [(params_in, params), (row_in, row_state), (col_in, col_state)])]
    for copy in small:
        copy.start()

    barrier = pltpu.get_barrier_semaphore()
    plane = [((gx + a) % nx, z, (y + b) % 2) for a in range(nx) for b in range(2) if (a, b) != (0, 0)]
    line = [(gx, zof(t), y) for t in range(1, nz)]
    for peer in line + plane:
        pl.semaphore_signal(barrier, inc=1, device_id=peer, device_id_type=pl.DeviceIdType.MESH)
    with scope("barrier"):
        pl.semaphore_wait(barrier, len(plane) + len(line))

    for k, (bx, by) in enumerate(blocks):
        rdma(grad.at[bx, 1 - c, zof(first), by], cr.at[first, bx, by], cs, cfr.at[k], core_peer).start()
    for t in (2, 1, 0):
        rdma(grad.at[:, 1 - c, zof(t)], cr.at[t], cs, cvr.at[t], core_peer).start()

    X, Y, NEAR, MIDDLE = 1, 2, 3, 4

    def send_plane(src, dst, swap, a=0, b=tiles):
        for region, (slot, peer) in zip(out_halves, [(X, x_peer), (Y, y_peer)] if swap else [(Y, y_peer), (X, x_peer)]):
            r, l = at((a, b) + region[2:])
            rdma(src.at[r, l], dst.at[slot, r, l], ns, nr.at[1 if swap else 0], peer).start()

    def send_near(src, dst, slot, peer, regions):
        for region in regions:
            r, l = at(region)
            rdma(src.at[r, l], dst.at[slot, r, l], nzs, nzr.at[slot - NEAR], peer).start()

    early = (tiles * 4 + 3) // 7
    if early:
        send_plane(params_in, params_of, True, 0, early)

    @on_inner
    def _():
        send_near(params_in, params_of, NEAR, near, out_flat)
        send_near(params_in, params_of, MIDDLE, middle, out_flat)

    on_end(lambda: send_near(params_in, params_of, NEAR, near, out_parts[1:]))

    def add(*terms):
        total = terms[0].astype(f32)
        for term in terms[1:]:
            total = total + term.astype(f32)
        return total

    def over(region, step, shift=0):
        a, b, d, e = region

        @pl.loop(a, b, unroll=True)
        def _(i):
            step(pl.ds(pl.multiple_of(i * TILE, TILE), TILE), pl.ds(d * lane, (e - d) * lane),
                 pl.ds((d - shift) * lane, (e - d) * lane))

    whole = (0, tiles, 0, 8)

    def pair_sum(t, bx, by):
        def step(r, l, _):
            lg[t, bx, by, r, l] = add(lg[t, bx, by, r, l], cr[t, bx, by, r, l]).astype(bf16)
        over(whole, step)

    def cross(t):
        return fs.at[1 if t else 0]

    def send(t, bx, by, slot, region, sem, peer):
        r, l = at(region)
        rdma(lg.at[t, bx, by, r, l], rx.at[t, slot, r, l], cross(t), sem.at[t], peer).start()

    def send_f(t):
        a, b = spans(t)
        send(t, 1 - x, 1 - y, 0, a, fr, x_peer)
        send(t, 1 - x, 1 - y, 0, b, fr, y_peer)

    def send_ga(t):
        send(t, 1 - x, y, 1, spans(t)[0], hr, x_peer)

    def send_gb(t):
        send(t, x, 1 - y, 1, spans(t)[1], hr, y_peer)

    def send_g(t):
        send_ga(t)
        send_gb(t)

    side = [1 - x, x]

    def send_strip(t, slot, peer, h):
        for region in strips:
            r, l = at(region)
            _, m = at(region, 6)
            rdma(lg.at[t, side[h], :, r, l], rc.at[slot, h, :, r, m], ks, kr.at[slot, h], peer).start()

    def send_strips(t, slot, peer):
        for h in range(2):
            send_strip(t, slot, peer, h)

    def take_strips(h, *slots):
        for slot in slots:
            with scope(f"line{slot}_{h}"):
                take_recv(some(2 * area(strips)), kr.at[slot, h])

    def strip_add(t, h, *slots):
        for by in range(2):
            def step(r, l, m):
                lg[t, side[h], by, r, l] = add(
                    lg[t, side[h], by, r, l], *[rc[slot, h, by, r, m] for slot in slots]).astype(bf16)
            for region in strips:
                over(region, step, 6)

    def relay(came, t, slot, peer):
        for h in range(2):
            take_strips(h, came)
            strip_add(t, h, came)
            send_strip(t, slot, peer, h)

    def stage_pair(t):
        with scope(f"pair{t}"):
            take_recv(cr.at[t], cvr.at[t])
            loads[t].wait()
            for bx, by in blocks:
                pair_sum(t, bx, by)

    def stage_first(t):
        a, b = spans(t)
        with scope(f"f{t}"):
            take_recv(some(area(spans(t))), fr.at[t])

        def step_a(r, l, _):
            lg[t, x, 1 - y, r, l] = add(lg[t, x, 1 - y, r, l], rx[t, 0, r, l]).astype(bf16)

        def step_b(r, l, _):
            lg[t, 1 - x, y, r, l] = add(lg[t, 1 - x, y, r, l], rx[t, 0, r, l]).astype(bf16)
        over(a, step_a)
        send(t, x, 1 - y, 2, a, hr, y_peer)
        over(b, step_b)
        send(t, 1 - x, y, 2, b, hr, x_peer)

    def stage_second(t):
        with scope(f"h{t}"):
            take_recv(some(2 * area(spans(t))), hr.at[t])

    def send_far(t, slot, peer, p):
        r, l = at(parts[p])
        rdma(lg.at[t, x, y, r, l], rz.at[slot, r, l], zs, zr.at[slot, p], peer).start()

    def take_far(slot, p):
        with scope(f"far{slot}_{p}"):
            take_recv(some(area(parts[p:p + 1])), zr.at[slot, p])

    def second_add(t, p, *slots):
        def step(r, l, _):
            lg[t, x, y, r, l] = add(lg[t, x, y, r, l], rx[t, 1, r, l], rx[t, 2, r, l],
                                    *[rz[slot, r, l] for slot in slots]).astype(bf16)
        over(parts[p], step)

    loads[first].wait()
    for k, (bx, by) in enumerate(blocks):
        with scope(f"core{k}"):
            take_recv(cr.at[first, bx, by], cfr.at[k])
        pair_sum(first, bx, by)
        if k == 0:
            send_f(first)
        elif k == 1:
            send_ga(first)
            on_end(lambda: send_strip(3, 3, near, 0))
        elif k == 2:
            send_gb(first)
        else:
            on_end(lambda: send_strip(3, 3, near, 1))
    stage_pair(2)
    on_end(lambda: send_strips(2, 2, near))
    send_f(2)
    stage_first(3)
    send_g(2)
    stage_pair(1)
    on_end(lambda: send_strips(1, 1, near))
    send_f(1)
    on_inner(lambda: relay(3, 2, 4, middle))
    stage_pair(0)

    @on_end
    def _():
        rz[5] = jnp.zeros((rows, columns), bf16)

    stage_first(2)
    send_g(1)
    on_inner(lambda: relay(2, 3, 5, middle))
    stage_second(3)
    for p in range(2):
        second_add(3, p)
        on_end(lambda: send_far(3, 3, near, p))
    on_inner(lambda: relay(4, 1, 0, near))
    stage_first(1)

    @on_end
    def _():
        stage_second(2)
        for p in range(2):
            second_add(2, p)
            send_far(2, 2, near, p)
        for h in range(2):
            take_strips(h, 0)
            strip_add(0, h, 0)

    @on_inner
    def _():
        for h in range(2):
            take_strips(h, 1, 5)
            strip_add(0, h, 1, 5)

    send_f(0)
    send_g(0)

    @on_inner
    def _():
        stage_second(2)
        for p in range(2):
            take_far(3, p)
            second_add(2, p, 3)
            send_far(2, 4, middle, p)

    def pass_far_sum(p):
        take_far(2, p)

        def step(r, l, _):
            lg[3, x, y, r, l] = add(lg[3, x, y, r, l], rz[2, r, l]).astype(bf16)
        over(parts[p], step)
        send_far(3, 5, middle, p)

    stage_second(1)

    @on_end
    def _():
        for p in range(2):
            second_add(1, p)
            send_far(1, 1, near, p)

    def pass_near_sum(p):
        take_far(4, p)
        second_add(1, p, 4)
        send_far(1, 1, near, p)

    @on_inner
    def _():
        pass_far_sum(0)
        pass_near_sum(0)

    stage_first(0)
    for copy in small:
        copy.wait()
    send_plane(params, params_of, False)

    @on_inner
    def _():
        pass_far_sum(1)
        pass_near_sum(1)
        send_near(params, params_of, MIDDLE, far, out_flat)

    on_end(lambda: send_near(params, params_of, NEAR, near, out_parts[:1]))
    info[0, 0:1, :] = row_state[...]
    st[:, columns:] = jnp.broadcast_to(jnp.sum(row_state[...], axis=1, keepdims=True), (1, stat_width - columns))
    stage_second(0)
    for p in range(2):
        take_far(1, p)

    @on_inner
    def _():
        for p in range(2):
            take_far(5, p)

    with scope("final"):
        cuts = [(0, 6), (6, 7), (7, 8)]
        squares = [None] * len(cuts)
        row_sums = []
        for i in range(tiles):
            r = pl.ds(i * TILE, TILE)
            row_sum = 0.0
            for k, (d, e) in enumerate(cuts):
                l = pl.ds(d * lane, (e - d) * lane)
                terms = [lg[0, x, y, r, l], rx[0, 1, r, l], rx[0, 2, r, l]]
                if e <= parts[0 if i < cut_row else 1][3]:
                    terms += [rz[1, r, l], rz[5, r, l]]
                value = add(*terms)
                sums[r, l] = value.astype(bf16)
                value = value * value
                row_sum = row_sum + jnp.sum(value, axis=1, keepdims=True)
                squares[k] = value if squares[k] is None else squares[k] + value
            sum_down[0, r, :] = row_sum
        for (d, e), value in zip(cuts, squares):
            st[:, pl.ds(d * lane, (e - d) * lane)] = jnp.sum(value, axis=0, keepdims=True)

    me = gx * 2 + y
    for peer in plane:
        rdma(st, st1.at[me], s1s, s1r, peer).start()
    st1[me] = st[...]
    diagonal = lax.broadcasted_iota(jnp.int32, (rows, rows), 0) == lax.broadcasted_iota(jnp.int32, (rows, rows), 1)

    def turned(vector, axis):
        return jnp.sum(jnp.where(diagonal, jnp.broadcast_to(vector, (rows, rows)), 0.0), axis=axis, keepdims=True)

    info[0, 1:2, :] = turned(sum_down[0], 0)

    def send_info(slot, peer):
        rdma(info.at[0], info.at[slot], ins, inr.at[slot], peer).start()

    send_info(X, x_peer)
    send_info(Y, y_peer)
    send_info(NEAR, near)

    @on_inner
    def _():
        send_info(MIDDLE, middle)
        send_info(MIDDLE, far)

    send_plane(sums, sums_of, False)
    if early < tiles:
        send_plane(params, params_of, True, early, tiles)
    send_plane(sums, sums_of, True)

    def send_sums(pieces):
        send_near(sums, sums_of, NEAR, near, pieces)
        on_inner(lambda: send_near(sums, sums_of, MIDDLE, middle, pieces))

    send_sums(out_parts)
    take_send(cr, cs)
    take_send(some(3 * area(halves)), fs.at[0])
    take_send(some(9 * area(parts)), fs.at[1])
    take_send(some(3 * area(parts)), zs)
    take_send(some(12 * area(strips)), ks)
    with scope("stat1"):
        take_recv(st1.at[0:nx * 2 - 1], s1r)
    total = st1[0]
    for k in range(1, nx * 2):
        total = total + st1[k]
    tot[...] = total
    for t in range(1, nz):
        rdma(tot, st2.at[z], s2s, s2r, (gx, zof(t), y)).start()
    on_inner(lambda: send_near(sums, sums_of, MIDDLE, far, out_flat))
    st2[z] = total
    state_down[0] = turned(row_state[...], 1)

    def turn_info(slot):
        with scope(f"info{slot}"):
            take_recv(info.at[slot], inr.at[slot])
        state_down[slot] = turned(info[slot, 0:1, :], 1)
        sum_down[slot] = turned(info[slot, 1:2, :], 1)

    for slot in (X, Y, NEAR, MIDDLE):
        turn_info(slot)
    with scope("stat2"):
        take_recv(st2.at[0:nz - 1], s2r)
    total = st2[0]
    for k in range(1, nz):
        total = total + st2[k]
    column_sum = total[:, 0:columns]
    norm_square = jnp.sum(column_sum, axis=1, keepdims=True)
    state_sum = total[:, columns:columns + 1]
    clip_level = 0.5 * math.sqrt(full_width * columns)
    factor = jnp.minimum(jnp.float32(1.0), clip_level / jnp.sqrt(norm_square + 1e-06))
    square_factor = factor * factor
    column_next = beta_two * col_state[...] + (1.0 - beta_two) * (square_factor * column_sum / full_width)
    row_average = (beta_two * state_sum + (1.0 - beta_two) * (square_factor * norm_square / columns)) / full_width
    col_scale = 1.0 / jnp.sqrt(column_next)

    def next_of(state, total):
        return beta_two * state + (1.0 - beta_two) * (square_factor * total / columns)

    def rate(slot):
        scale[slot] = (step_size * factor) / jnp.sqrt(next_of(state_down[slot], sum_down[slot]) / row_average)

    def update(slot, bx, u, by, regions):
        def step(r, l, _):
            new = params_of[slot, r, l].astype(f32) - (sums_of[slot, r, l].astype(f32) * scale[slot, r, :]) * col_scale_of(l)
            full[bx, c, u, by, r, l] = new.astype(bf16)
        for region in regions:
            over(region, step)

    def col_scale_of(l):
        return col_scale[:, l.start:l.start + l.size]

    gzs, gzr, qs, q1r, q2r, q3r, gks, gcs = zs, cfr, fs, fr, hr, cvr, ks, cs
    gcr = zr.at[0, 0]
    parts, strips, halves = out_parts, out_strips, out_halves

    def same(view, ssem, rsem, peer):
        rdma(view, view, ssem, rsem, peer).start()

    def moves(t):
        return qs.at[1 if t else 0]

    def piece(bx, u, by, region):
        r, l = at(region)
        return full.at[bx, c, u, by, r, l]

    def pass_core(t, bx, by):
        for region in out_flat if t else [whole]:
            same(piece(bx, origin[t], by, region), gcs, gcr, core_peer)

    def send_q1(t):
        u, (a, b) = origin[t], spans(t)
        same(piece(x, u, y, a), moves(t), q1r.at[t], y_peer)
        same(piece(x, u, y, b), moves(t), q1r.at[t], x_peer)

    def send_q2(t):
        u, (a, b) = origin[t], spans(t)
        same(piece(x, u, y, a), moves(t), q2r.at[t], x_peer)
        same(piece(x, u, y, b), moves(t), q2r.at[t], y_peer)
        pass_core(t, x, y)

    def send_own(t):
        send_q1(t)
        send_q2(t)

    def pass_far(t, slot, peer):
        for region in out_flat:
            same(piece(x, origin[t], y, region), gzs, gzr.at[slot], peer)

    def take_z(t):
        with scope(f"gz{t}"):
            take_recv(some(area(parts)), gzr.at[t])

    def gather_cross(t):
        u, (a, b) = origin[t], spans(t)
        with scope(f"q1_{t}"):
            take_recv(some(area(spans(t))), q1r.at[t])
        same(piece(x, u, 1 - y, a), moves(t), q3r.at[t], x_peer)
        same(piece(1 - x, u, y, b), moves(t), zr.at[0, 1] if t == 3 else q3r.at[t], y_peer)

    def gather_side(t):
        with scope(f"q2_{t}"):
            take_recv(some(area(spans(t))), q2r.at[t])
        pass_core(t, 1 - x, y)
        pass_core(t, x, 1 - y)

    def gather_far(t):
        with scope(f"q3_{t}"):
            take_recv(some(area(spans(t))), q3r.at[t])
        pass_core(t, 1 - x, 1 - y)

    def each_strip(t, p, ssem, rsem, peer):
        r, l = at(strips[0])
        for bx, by in [(1 - x, 1 - y)] if p else [(x, y), (1 - x, y), (x, 1 - y)]:
            same(full.at[bx, c, origin[t], by, r, l], ssem, rsem, peer)

    def pass_strip(t, p, slot, peer):
        each_strip(t, p, gks, kr.at[slot, p], peer)

    def take_strip(t, p):
        with scope(f"strip{t}_{p}"):
            take_recv(some((1 if p else 3) * area(strips)), kr.at[t, p])
        each_strip(t, p, gcs, gcr, core_peer)

    def own_strip(p):
        pass_strip(0, p, 1, near)
        on_inner(lambda: pass_strip(0, p, 2, middle))

    low, high = halves
    rate(X)
    rate(Y)
    with scope("plane1"):
        take_recv(some(4 * area(halves[:1])), nr.at[0])
    update(Y, x, z, 1 - y, [low])
    update(X, 1 - x, z, y, [high])
    same(piece(x, z, 1 - y, low), moves(0), q3r.at[0], x_peer)
    same(piece(1 - x, z, y, high), moves(0), q3r.at[0], y_peer)
    rate(NEAR)
    with scope("near"):
        take_recv(some(2 * area(parts)), nzr.at[0])
    update(NEAR, x, origin[1], y, parts)
    on_inner(lambda: pass_far(1, 3, middle))
    send_own(1)

    rate(0)
    update(0, x, z, y, [whole])
    pass_core(0, x, y)
    new_ref[...] = full[x, c, z, y]
    col_ref[...] = column_next
    row_ref[...] = next_of(info[0, 0:1, :], info[0, 1:2, :])
    with scope("plane2"):
        take_recv(some(4 * area(halves[:1])), nr.at[1])
    update(X, 1 - x, z, y, [low])
    update(Y, x, z, 1 - y, [high])
    own_strip(0)
    pass_core(0, 1 - x, y)
    pass_core(0, x, 1 - y)

    def update_middle():
        rate(MIDDLE)
        with scope("middle"):
            take_recv(some(2 * area(parts)), nzr.at[1])
        update(MIDDLE, x, origin[2], y, parts)

    on_inner(update_middle)
    gather_far(0)
    own_strip(1)
    gather_cross(1)
    on_end(update_middle)
    send_own(2)

    @on_inner
    def _():
        take_z(3)
        pass_far(3, 3, near)

    def relay_strip(t, p, slot, peer):
        take_strip(t, p)
        pass_strip(t, p, slot, peer)

    on_inner(lambda: relay_strip(1, 0, 3, middle))
    gather_side(1)
    gather_far(1)
    on_inner(lambda: relay_strip(1, 1, 3, middle))

    def pass_second():
        relay_strip(2, 0, 2, near)
        relay_strip(2, 1, 2, near)

    pl.when((inside == 1) & (c == 0))(pass_second)
    gather_cross(2)
    on_end(lambda: take_z(3))
    send_own(3)
    pl.when((inside == 1) & (c == 1))(pass_second)

    @on_inner
    def _():
        relay_strip(3, 0, 3, near)
        relay_strip(3, 1, 3, near)

    gather_side(2)
    gather_far(2)

    def end_strip(t):
        take_strip(t, 0)
        take_strip(t, 1)

    on_end(lambda: end_strip(1))
    gather_cross(3)
    on_end(lambda: end_strip(2))
    gather_side(3)
    on_end(lambda: end_strip(3))
    for span, sem in zip(spans(3), (q3r.at[3], zr.at[0, 1])):
        with scope(f"q3_3_{span[2]}"):
            take_recv(some(area([span])), sem)
        same(piece(1 - x, origin[3], 1 - y, span), gcs, gcr, core_peer)

    with scope("finish"):
        take_send(st1.at[0:nx * 2 - 1], s1s)
        take_send(st2.at[0:nz - 1], s2s)
        take_send(some(area(halves)), qs.at[0])
        take_send(some(9 * area(parts)), qs.at[1])
        take_send(some(4 * area(halves)), ns)

        @on_end
        def _():
            take_send(some(2 * area(parts)), nzs)
            take_send(info.at[0:3], ins)
            take_send(some(4 * area(strips)), gks)

        @on_inner
        def _():
            take_send(some(6 * area(parts)), nzs)
            take_send(info, ins)
            take_send(some(2 * area(parts)), gzs)
            take_send(some(20 * area(strips)), gks)

        take_send(full.at[:, c], gcs)
        take_recv(full.at[:, c], gcr)


def write_out(nz, new, row, col, full, new_out, row_out, col_out, full_out, sem):
    pieces = [(full.at[a, b, u], full_out.at[a, b, u]) for a in range(2) for b in range(2) for u in range(nz)]
    copies = [pltpu.make_async_copy(src, dst, sem.at[0]) for src, dst in pieces]
    small = [pltpu.make_async_copy(src, dst, sem.at[k + 1])
             for k, (src, dst) in enumerate([(new, new_out), (row, row_out), (col, col_out)])]
    for copy in copies + small:
        copy.start()
    for copy in small:
        copy.wait()
    pltpu.make_async_copy(full, full_out, sem.at[0]).wait()


def fused(nx, nz, grad_bucket, parameters, row_state, column_state):
    _, _, full_width, columns = grad_bucket.shape
    rows = parameters.shape[1]
    lane = columns // 8
    bf16, f32 = jnp.bfloat16, jnp.float32
    vmem = pl.BlockSpec(memory_space=pltpu.VMEM)
    hbm = pl.BlockSpec(memory_space=pltpu.HBM)
    dma = pltpu.SemaphoreType.DMA
    one = dma(())
    shapes = [((rows, columns), bf16), ((1, rows), f32), ((1, columns), f32), ((2, 2, nz, 2, rows, columns), bf16)]
    held = 2 * columns * (rows + full_width) + 4 * (columns + -(-rows // 128) * 128)
    stat = columns + 128
    results = pl.pallas_call(
        functools.partial(kernel, nx, nz),
        out_shape=tuple(pltpu.VMEM(*shape) for shape in shapes),
        in_specs=[hbm] * 4,
        out_specs=(vmem,) * 4,
        scratch_shapes=[
            pltpu.VMEM((nz, 2, 2, rows, columns), bf16),
            pltpu.VMEM((nz, 2, 2, rows, columns), bf16),
            pltpu.VMEM((nz, 3, rows, columns), bf16),
            pltpu.VMEM((6, rows, columns), bf16),
            pltpu.VMEM((6, 2, 2, rows, 2 * lane), bf16),
            pltpu.VMEM((9 * 8 * (rows // TILE), TILE, lane), bf16),
            pltpu.VMEM((5, rows, columns), bf16),
            pltpu.VMEM((5, rows, columns), bf16),
            pltpu.VMEM((5, 2, rows), f32),
            pltpu.VMEM((5, rows, 1), f32),
            pltpu.VMEM((5, rows, 1), f32),
            pltpu.VMEM((5, rows, 1), f32),
            pltpu.VMEM((1, stat), f32),
            pltpu.VMEM((nx * 2, 1, stat), f32),
            pltpu.VMEM((1, stat), f32),
            pltpu.VMEM((nz, 1, stat), f32),
            pltpu.VMEM((1, rows), f32),
            pltpu.VMEM((1, columns), f32),
            dma((nz,)), dma((3,)), one, dma((4,)), dma((nz,)), dma((2,)), dma((nz,)), dma((nz,)),
            one, dma((6, 2)), one, dma((6, 2)), one, one, one, one,
            one, dma((2,)), one, dma((2,)), one, dma((5,)),
        ],
        compiler_params=pltpu.CompilerParams(
            collective_id=0, has_side_effects=True, vmem_limit_bytes=VMEM_BYTES - held),
    )(grad_bucket.reshape(2, 2, nz, 2, rows, columns), parameters[0], row_state, column_state)
    new, row, col, full = pl.pallas_call(
        functools.partial(write_out, nz),
        out_shape=tuple(jax.ShapeDtypeStruct(*shape) for shape in shapes),
        in_specs=[vmem] * 4,
        out_specs=(hbm,) * 4,
        scratch_shapes=[dma((4,))],
        compiler_params=pltpu.CompilerParams(vmem_limit_bytes=4 * 1024 * 1024),
    )(*[pltpu.with_memory_space_constraint(result, pltpu.VMEM) for result in results])
    return (new[None], row, col, full.reshape(full_width, columns))


def solution(mesh):
    nx, nz, ny = (mesh.shape[a] for a in AXES)
    in_specs = (
        P(AXES, None, None, None),
        P(None, AXES, None),
        P(None, AXES),
        P(),
    )
    out_specs = (P(None, AXES, None), P(None, AXES), P(), P())
    fits = nx == 4 and ny == 2 and nz == 4

    def body(grad_bucket, parameters, row_state, column_state):
        if fits and grad_bucket.shape[1] == 1 and parameters.shape[1] % TILE == 0 and parameters.shape[1] >= 2 * TILE and grad_bucket.shape[3] % 1024 == 0:
            return fused(nx, nz, grad_bucket, parameters, row_state, column_state)
        return shards(grad_bucket, parameters, row_state, column_state)

    return jax.shard_map(body, mesh=mesh, in_specs=in_specs, out_specs=out_specs, check_vma=False)
```

```python
import functools
import math

import jax
import jax.numpy as jnp
from jax import lax
from jax.experimental import pallas as pl
from jax.experimental.pallas import tpu as pltpu
from jax.sharding import PartitionSpec as P

beta_two = 0.8
step_size = 0.5
AXES = ("gx", "gy", "gz")
TILE = 16
VMEM_BYTES = 67043328 - 131072


def shards(grad_bucket, parameters, row_state, column_state):
    local_grad = grad_bucket[0].astype(jnp.float32)
    layer_count, full_width, columns = local_grad.shape
    summed = lax.psum_scatter(local_grad, AXES, scatter_dimension=1, tiled=True)
    clip_level = 0.5 * math.sqrt(layer_count * full_width * columns)
    squares = summed * summed
    norm_square = lax.psum(jnp.sum(squares), AXES)
    factor = jnp.minimum(jnp.float32(1.0), clip_level / jnp.sqrt(norm_square + 1e-06))
    clipped = factor * summed
    clipped_square = clipped * clipped
    row_next = beta_two * row_state + (1.0 - beta_two) * jnp.mean(clipped_square, axis=2)
    column_part, row_total = lax.psum((jnp.sum(clipped_square, axis=1), jnp.sum(row_next, axis=1)), AXES)
    column_next = beta_two * column_state + (1.0 - beta_two) * column_part / full_width
    row_average = row_total / full_width
    second = row_next[:, :, None] * column_next[:, None, :] / row_average[:, None, None]
    update = clipped / jnp.sqrt(second)
    new_parameters = (parameters.astype(jnp.float32) - step_size * update).astype(jnp.bfloat16)
    first_layer = lax.all_gather(new_parameters[0], AXES, axis=0, tiled=True)
    return (new_parameters, row_next, column_next, first_layer)


def flip(index, mask, size):
    out, bit = 0, 1
    while bit < size:
        out = out + bit * (((index // bit) % 2 + (mask // bit) % 2) % 2)
        bit *= 2
    return out


def kernel(nx, nz, grad, params_in, row_in, col_in, new_ref, row_ref, col_ref, full,
           lg, cr, rx, rz, rc, unit, sums_of, params_of, info, scale, state_down, sum_down, st, st1, tot, st2, row_state, col_state,
           lsem, isem, cs, cfr, cvr, fs, fr, hr, zs, zr, ks, kr, s1s, s1r, s2s, s2r,
           ns, nr, nzs, nzr, ins, inr):
    gx, z, y = lax.axis_index("gx"), lax.axis_index("gy"), lax.axis_index("gz")
    x, c = gx // 2, gx % 2
    rows, columns = new_ref.shape
    params, sums = params_of.at[0], sums_of.at[0]
    lane = columns // 8
    stat_width = st.shape[1]
    full_width = rows * 4 * nz * 2
    core_peer = (x * 2 + 1 - c, z, y)
    x_peer = ((1 - x) * 2 + c, z, y)
    y_peer = (gx, z, 1 - y)
    tiles = rows // TILE
    f32, bf16 = jnp.float32, jnp.bfloat16
    scope = jax.named_scope
    blocks = [(1 - x, 1 - y), (1 - x, y), (x, 1 - y), (x, y)]

    def regions(cut, middle_lane):
        return ([(0, cut, 0, 6), (cut, tiles, 0, 7)], [(0, cut, 6, 8), (cut, tiles, 7, 8)],
                [(0, tiles, 0, middle_lane), (0, tiles, middle_lane, 8)])

    cut_row = (tiles * 4 + 3) // 7
    parts, strips, halves = regions(cut_row, 4)
    out_parts, out_strips, out_halves = [(0, tiles, 0, 3), (0, tiles, 3, 6)], [(0, tiles, 6, 8)], halves
    out_flat = [(0, tiles, 0, 6)]

    def area(regions):
        return sum((b - a) * (e - d) for a, b, d, e in regions)

    def at(region, shift=0):
        a, b, d, e = region
        return pl.ds(a * TILE, (b - a) * TILE), pl.ds((d - shift) * lane, (e - d) * lane)

    def spans(t):
        return halves if t == 0 else parts[::-1] if t % 2 else parts

    def zof(t):
        return flip(z, t, nz)

    inside = (z + z // 2) % 2
    near, middle, far = (gx, zof(1), y), (gx, zof(3), y), (gx, zof(2), y)
    origin = [z, zof(1), flip(z, 2 + inside, nz), flip(z, 3 - inside, nz)]

    def on_end(step):
        pl.when(inside == 0)(step)

    def on_inner(step):
        pl.when(inside == 1)(step)

    def rdma(src, dst, ssem, rsem, peer):
        return pltpu.make_async_remote_copy(
            src_ref=src, dst_ref=dst, send_sem=ssem, recv_sem=rsem,
            device_id=peer, device_id_type=pl.DeviceIdType.MESH)

    def take_recv(view, sem):
        rdma(view, view, sem, sem, core_peer).wait_recv()

    def take_send(view, sem):
        rdma(view, view, sem, sem, core_peer).wait_send()

    def some(count):
        return unit.at[pl.ds(0, count)]

    first = 3
    loads = {t: pltpu.make_async_copy(grad.at[:, c, zof(t)], lg.at[t], lsem.at[0 if t == 3 else 1]) for t in (3, 2, 1, 0)}
    for t in loads:
        loads[t].start()
    small = [pltpu.make_async_copy(src, dst, isem.at[k]) for k, (src, dst) in enumerate(
        [(params_in, params), (row_in, row_state), (col_in, col_state)])]
    for copy in small:
        copy.start()

    barrier = pltpu.get_barrier_semaphore()
    plane = [((gx + a) % nx, z, (y + b) % 2) for a in range(nx) for b in range(2) if (a, b) != (0, 0)]
    line = [(gx, zof(t), y) for t in range(1, nz)]
    for peer in line + plane:
        pl.semaphore_signal(barrier, inc=1, device_id=peer, device_id_type=pl.DeviceIdType.MESH)
    with scope("barrier"):
        pl.semaphore_wait(barrier, len(plane) + len(line))

    for k, (bx, by) in enumerate(blocks):
        rdma(grad.at[bx, 1 - c, zof(first), by], cr.at[first, bx, by], cs, cfr.at[k], core_peer).start()
    for t in (2, 1, 0):
        rdma(grad.at[:, 1 - c, zof(t)], cr.at[t], cs, cvr.at[t], core_peer).start()

    X, Y, NEAR, MIDDLE = 1, 2, 3, 4

    def send_plane(src, dst, swap, a=0, b=tiles):
        for region, (slot, peer) in zip(out_halves, [(X, x_peer), (Y, y_peer)] if swap else [(Y, y_peer), (X, x_peer)]):
            r, l = at((a, b) + region[2:])
            rdma(src.at[r, l], dst.at[slot, r, l], ns, nr.at[1 if swap else 0], peer).start()

    def send_near(src, dst, slot, peer, regions):
        for region in regions:
            r, l = at(region)
            rdma(src.at[r, l], dst.at[slot, r, l], nzs, nzr.at[slot - NEAR], peer).start()

    early = (tiles * 4 + 3) // 7
    if early:
        send_plane(params_in, params_of, True, 0, early)

    @on_inner
    def _():
        send_near(params_in, params_of, NEAR, near, out_flat)
        send_near(params_in, params_of, MIDDLE, middle, out_flat)

    on_end(lambda: send_near(params_in, params_of, NEAR, near, out_parts[1:]))

    def add(*terms):
        total = terms[0].astype(f32)
        for term in terms[1:]:
            total = total + term.astype(f32)
        return total

    def over(region, step, shift=0):
        a, b, d, e = region

        @pl.loop(a, b, unroll=True)
        def _(i):
            step(pl.ds(pl.multiple_of(i * TILE, TILE), TILE), pl.ds(d * lane, (e - d) * lane),
                 pl.ds((d - shift) * lane, (e - d) * lane))

    whole = (0, tiles, 0, 8)

    def pair_sum(t, bx, by):
        def step(r, l, _):
            lg[t, bx, by, r, l] = add(lg[t, bx, by, r, l], cr[t, bx, by, r, l]).astype(bf16)
        over(whole, step)

    def cross(t):
        return fs.at[1 if t else 0]

    def send(t, bx, by, slot, region, sem, peer):
        r, l = at(region)
        rdma(lg.at[t, bx, by, r, l], rx.at[t, slot, r, l], cross(t), sem.at[t], peer).start()

    def send_f(t):
        a, b = spans(t)
        send(t, 1 - x, 1 - y, 0, a, fr, x_peer)
        send(t, 1 - x, 1 - y, 0, b, fr, y_peer)

    def send_ga(t):
        send(t, 1 - x, y, 1, spans(t)[0], hr, x_peer)

    def send_gb(t):
        send(t, x, 1 - y, 1, spans(t)[1], hr, y_peer)

    def send_g(t):
        send_ga(t)
        send_gb(t)

    side = [1 - x, x]

    def send_strip(t, slot, peer, h):
        for region in strips:
            r, l = at(region)
            _, m = at(region, 6)
            rdma(lg.at[t, side[h], :, r, l], rc.at[slot, h, :, r, m], ks, kr.at[max(slot, 1) - 1, h], peer).start()

    def send_strips(t, slot, peer):
        for h in range(2):
            send_strip(t, slot, peer, h)

    def take_strips(h, *slots):
        for slot in slots:
            with scope(f"line{slot}_{h}"):
                take_recv(some(2 * area(strips)), kr.at[max(slot, 1) - 1, h])

    def strip_add(t, h, *slots):
        for by in range(2):
            def step(r, l, m):
                lg[t, side[h], by, r, l] = add(
                    lg[t, side[h], by, r, l], *[rc[slot, h, by, r, m] for slot in slots]).astype(bf16)
            for region in strips:
                over(region, step, 6)

    def relay(came, t, slot, peer):
        for h in range(2):
            take_strips(h, came)
            strip_add(t, h, came)
            send_strip(t, slot, peer, h)

    def stage_pair(t):
        with scope(f"pair{t}"):
            take_recv(cr.at[t], cvr.at[t])
            if t == 2:
                take_recv(lg.at[0:3], lsem.at[1])
            for bx, by in blocks:
                pair_sum(t, bx, by)

    def stage_first(t):
        a, b = spans(t)
        with scope(f"f{t}"):
            take_recv(some(area(spans(t))), fr.at[t])

        def step_a(r, l, _):
            lg[t, x, 1 - y, r, l] = add(lg[t, x, 1 - y, r, l], rx[t, 0, r, l]).astype(bf16)

        def step_b(r, l, _):
            lg[t, 1 - x, y, r, l] = add(lg[t, 1 - x, y, r, l], rx[t, 0, r, l]).astype(bf16)
        over(a, step_a)
        send(t, x, 1 - y, 2, a, hr, y_peer)
        over(b, step_b)
        send(t, 1 - x, y, 2, b, hr, x_peer)

    def stage_second(t):
        with scope(f"h{t}"):
            take_recv(some(2 * area(spans(t))), hr.at[t])

    def send_far(t, slot, peer, p):
        r, l = at(parts[p])
        rdma(lg.at[t, x, y, r, l], rz.at[slot, r, l], zs, zr.at[slot, p], peer).start()

    def take_far(slot, p):
        with scope(f"far{slot}_{p}"):
            take_recv(some(area(parts[p:p + 1])), zr.at[slot, p])

    def second_add(t, p, *slots):
        def step(r, l, _):
            lg[t, x, y, r, l] = add(lg[t, x, y, r, l], rx[t, 1, r, l], rx[t, 2, r, l],
                                    *[rz[slot, r, l] for slot in slots]).astype(bf16)
        over(parts[p], step)

    loads[first].wait()
    for k, (bx, by) in enumerate(blocks):
        with scope(f"core{k}"):
            take_recv(cr.at[first, bx, by], cfr.at[k])
        pair_sum(first, bx, by)
        if k == 0:
            send_f(first)
        elif k == 1:
            send_ga(first)
            on_end(lambda: send_strip(3, 3, near, 0))
        elif k == 2:
            send_gb(first)
        else:
            on_end(lambda: send_strip(3, 3, near, 1))
    stage_pair(2)
    on_end(lambda: send_strips(2, 2, near))
    send_f(2)
    stage_first(3)
    send_g(2)
    stage_pair(1)
    on_end(lambda: send_strips(1, 1, near))
    send_f(1)
    on_inner(lambda: relay(3, 2, 4, middle))
    stage_pair(0)

    @on_end
    def _():
        rz[5] = jnp.zeros((rows, columns), bf16)

    stage_first(2)
    send_g(1)
    on_inner(lambda: relay(2, 3, 5, middle))
    stage_second(3)
    for p in range(2):
        second_add(3, p)
        on_end(lambda: send_far(3, 3, near, p))
    on_inner(lambda: relay(4, 1, 0, near))
    stage_first(1)

    @on_end
    def _():
        stage_second(2)
        for p in range(2):
            second_add(2, p)
            send_far(2, 2, near, p)
        for h in range(2):
            take_strips(h, 0)
            strip_add(0, h, 0)

    @on_inner
    def _():
        for h in range(2):
            take_strips(h, 1, 5)
            strip_add(0, h, 1, 5)

    send_f(0)
    send_g(0)

    @on_inner
    def _():
        stage_second(2)
        for p in range(2):
            take_far(3, p)
            second_add(2, p, 3)
            send_far(2, 4, middle, p)

    def pass_far_sum(p):
        take_far(2, p)

        def step(r, l, _):
            lg[3, x, y, r, l] = add(lg[3, x, y, r, l], rz[2, r, l]).astype(bf16)
        over(parts[p], step)
        send_far(3, 5, middle, p)

    stage_second(1)

    @on_end
    def _():
        for p in range(2):
            second_add(1, p)
            send_far(1, 1, near, p)

    def pass_near_sum(p):
        take_far(4, p)
        second_add(1, p, 4)
        send_far(1, 1, near, p)

    @on_inner
    def _():
        pass_far_sum(0)
        pass_near_sum(0)

    stage_first(0)
    for copy in small:
        copy.wait()
    send_plane(params, params_of, False)

    @on_inner
    def _():
        pass_far_sum(1)
        pass_near_sum(1)
        send_near(params, params_of, MIDDLE, far, out_flat)

    on_end(lambda: send_near(params, params_of, NEAR, near, out_parts[:1]))
    info[0, 0:1, :] = row_state[...]
    st[:, columns:] = jnp.broadcast_to(jnp.sum(row_state[...], axis=1, keepdims=True), (1, stat_width - columns))
    stage_second(0)
    for p in range(2):
        take_far(1, p)

    @on_inner
    def _():
        for p in range(2):
            take_far(5, p)

    with scope("final"):
        cuts = [(0, 6), (6, 7), (7, 8)]
        squares = [None] * len(cuts)
        row_sums = []
        for i in range(tiles):
            r = pl.ds(i * TILE, TILE)
            row_sum = 0.0
            for k, (d, e) in enumerate(cuts):
                l = pl.ds(d * lane, (e - d) * lane)
                terms = [lg[0, x, y, r, l], rx[0, 1, r, l], rx[0, 2, r, l]]
                if e <= parts[0 if i < cut_row else 1][3]:
                    terms += [rz[1, r, l], rz[5, r, l]]
                value = add(*terms)
                sums[r, l] = value.astype(bf16)
                value = value * value
                row_sum = row_sum + jnp.sum(value, axis=1, keepdims=True)
                squares[k] = value if squares[k] is None else squares[k] + value
            sum_down[0, r, :] = row_sum
        for (d, e), value in zip(cuts, squares):
            st[:, pl.ds(d * lane, (e - d) * lane)] = jnp.sum(value, axis=0, keepdims=True)

    me = gx * 2 + y
    for peer in plane:
        rdma(st, st1.at[me], s1s, s1r, peer).start()
    st1[me] = st[...]
    diagonal = lax.broadcasted_iota(jnp.int32, (rows, rows), 0) == lax.broadcasted_iota(jnp.int32, (rows, rows), 1)

    def turned(vector, axis):
        return jnp.sum(jnp.where(diagonal, jnp.broadcast_to(vector, (rows, rows)), 0.0), axis=axis, keepdims=True)

    info[0, 1:2, :] = turned(sum_down[0], 0)

    def send_info(slot, peer):
        rdma(info.at[0], info.at[slot], ins, inr.at[max(slot - Y, 0)], peer).start()

    send_info(X, x_peer)
    send_info(Y, y_peer)
    send_info(NEAR, near)

    @on_inner
    def _():
        send_info(MIDDLE, middle)
        send_info(MIDDLE, far)

    send_plane(sums, sums_of, False)
    if early < tiles:
        send_plane(params, params_of, True, early, tiles)
    send_plane(sums, sums_of, True)

    def send_sums(pieces):
        send_near(sums, sums_of, NEAR, near, pieces)
        on_inner(lambda: send_near(sums, sums_of, MIDDLE, middle, pieces))

    send_sums(out_parts)
    take_send(cr, cs)
    take_send(some(3 * area(halves)), fs.at[0])
    take_send(some(9 * area(parts)), fs.at[1])
    take_send(some(3 * area(parts)), zs)
    take_send(some(12 * area(strips)), ks)
    with scope("stat1"):
        take_recv(st1.at[0:nx * 2 - 1], s1r)
    total = st1[0]
    for k in range(1, nx * 2):
        total = total + st1[k]
    tot[...] = total
    for t in range(1, nz):
        rdma(tot, st2.at[z], s2s, s2r, (gx, zof(t), y)).start()
    on_inner(lambda: send_near(sums, sums_of, MIDDLE, far, out_flat))
    st2[z] = total
    state_down[0] = turned(row_state[...], 1)

    def turn_info(slot):
        with scope(f"info{slot}"):
            if slot == X:
                take_recv(info.at[X:NEAR], inr.at[0])
            elif slot > Y:
                take_recv(info.at[slot], inr.at[slot - Y])
        state_down[slot] = turned(info[slot, 0:1, :], 1)
        sum_down[slot] = turned(info[slot, 1:2, :], 1)

    for slot in (X, Y, NEAR, MIDDLE):
        turn_info(slot)
    with scope("stat2"):
        take_recv(st2.at[0:nz - 1], s2r)
    total = st2[0]
    for k in range(1, nz):
        total = total + st2[k]
    column_sum = total[:, 0:columns]
    norm_square = jnp.sum(column_sum, axis=1, keepdims=True)
    state_sum = total[:, columns:columns + 1]
    clip_level = 0.5 * math.sqrt(full_width * columns)
    factor = jnp.minimum(jnp.float32(1.0), clip_level / jnp.sqrt(norm_square + 1e-06))
    square_factor = factor * factor
    column_next = beta_two * col_state[...] + (1.0 - beta_two) * (square_factor * column_sum / full_width)
    row_average = (beta_two * state_sum + (1.0 - beta_two) * (square_factor * norm_square / columns)) / full_width
    col_scale = 1.0 / jnp.sqrt(column_next)

    def next_of(state, total):
        return beta_two * state + (1.0 - beta_two) * (square_factor * total / columns)

    def rate(slot):
        scale[slot] = (step_size * factor) / jnp.sqrt(next_of(state_down[slot], sum_down[slot]) / row_average)

    def update(slot, bx, u, by, regions):
        def step(r, l, _):
            new = params_of[slot, r, l].astype(f32) - (sums_of[slot, r, l].astype(f32) * scale[slot, r, :]) * col_scale_of(l)
            full[bx, c, u, by, r, l] = new.astype(bf16)
        for region in regions:
            over(region, step)

    def col_scale_of(l):
        return col_scale[:, l.start:l.start + l.size]

    gzs, gzr, qs, q1r, q2r, q3r, gks, gcs = zs, cfr, fs, fr, hr, cvr, ks, cs
    gcr = zr.at[0, 0]
    parts, strips, halves = out_parts, out_strips, out_halves

    def same(view, ssem, rsem, peer):
        rdma(view, view, ssem, rsem, peer).start()

    def moves(t):
        return qs.at[1 if t else 0]

    def piece(bx, u, by, region):
        r, l = at(region)
        return full.at[bx, c, u, by, r, l]

    def pass_core(t, bx, by):
        for region in out_flat if t else [whole]:
            same(piece(bx, origin[t], by, region), gcs, gcr, core_peer)

    def send_q1(t):
        u, (a, b) = origin[t], spans(t)
        same(piece(x, u, y, a), moves(t), q1r.at[t], y_peer)
        same(piece(x, u, y, b), moves(t), q1r.at[t], x_peer)

    def send_q2(t):
        u, (a, b) = origin[t], spans(t)
        same(piece(x, u, y, a), moves(t), q2r.at[t], x_peer)
        same(piece(x, u, y, b), moves(t), q2r.at[t], y_peer)
        pass_core(t, x, y)

    def send_own(t):
        send_q1(t)
        send_q2(t)

    def pass_far(t, slot, peer):
        for region in out_flat:
            same(piece(x, origin[t], y, region), gzs, gzr.at[slot], peer)

    def take_z(t):
        with scope(f"gz{t}"):
            take_recv(some(area(parts)), gzr.at[t])

    def gather_cross(t):
        u, (a, b) = origin[t], spans(t)
        with scope(f"q1_{t}"):
            take_recv(some(area(spans(t))), q1r.at[t])
        same(piece(x, u, 1 - y, a), moves(t), q3r.at[t], x_peer)
        same(piece(1 - x, u, y, b), moves(t), zr.at[0, 1] if t == 3 else q3r.at[t], y_peer)

    def gather_side(t):
        with scope(f"q2_{t}"):
            take_recv(some(area(spans(t))), q2r.at[t])
        pass_core(t, 1 - x, y)
        pass_core(t, x, 1 - y)

    def gather_far(t):
        with scope(f"q3_{t}"):
            take_recv(some(area(spans(t))), q3r.at[t])
        pass_core(t, 1 - x, 1 - y)

    def each_strip(t, p, ssem, rsem, peer):
        r, l = at(strips[0])
        for bx, by in [(1 - x, 1 - y)] if p else [(x, y), (1 - x, y), (x, 1 - y)]:
            same(full.at[bx, c, origin[t], by, r, l], ssem, rsem, peer)

    def pass_strip(t, p, slot, peer):
        each_strip(t, p, gks, kr.at[slot - 1, p], peer)

    def take_strip(t, p):
        with scope(f"strip{t}_{p}"):
            take_recv(some((1 if p else 3) * area(strips)), kr.at[t - 1, p])
        each_strip(t, p, gcs, gcr, core_peer)

    def own_strip(p):
        pass_strip(0, p, 1, near)
        on_inner(lambda: pass_strip(0, p, 2, middle))

    low, high = halves
    rate(X)
    rate(Y)
    with scope("plane1"):
        take_recv(some(4 * area(halves[:1])), nr.at[0])
    update(Y, x, z, 1 - y, [low])
    update(X, 1 - x, z, y, [high])
    same(piece(x, z, 1 - y, low), moves(0), q3r.at[0], x_peer)
    same(piece(1 - x, z, y, high), moves(0), q3r.at[0], y_peer)
    rate(NEAR)
    with scope("near"):
        take_recv(some(2 * area(parts)), nzr.at[0])
    update(NEAR, x, origin[1], y, parts)
    on_inner(lambda: pass_far(1, 3, middle))
    send_own(1)

    rate(0)
    update(0, x, z, y, [whole])
    pass_core(0, x, y)
    new_ref[...] = full[x, c, z, y]
    col_ref[...] = column_next
    row_ref[...] = next_of(info[0, 0:1, :], info[0, 1:2, :])
    with scope("plane2"):
        take_recv(some(4 * area(halves[:1])), nr.at[1])
    update(X, 1 - x, z, y, [low])
    update(Y, x, z, 1 - y, [high])
    own_strip(0)
    pass_core(0, 1 - x, y)
    pass_core(0, x, 1 - y)

    def update_middle():
        rate(MIDDLE)
        with scope("middle"):
            take_recv(some(2 * area(parts)), nzr.at[1])
        update(MIDDLE, x, origin[2], y, parts)

    on_inner(update_middle)
    gather_far(0)
    own_strip(1)
    gather_cross(1)
    on_end(update_middle)
    send_own(2)

    @on_inner
    def _():
        take_z(3)
        pass_far(3, 3, near)

    def relay_strip(t, p, slot, peer):
        take_strip(t, p)
        pass_strip(t, p, slot, peer)

    on_inner(lambda: relay_strip(1, 0, 3, middle))
    gather_side(1)
    gather_far(1)
    on_inner(lambda: relay_strip(1, 1, 3, middle))

    def pass_second():
        relay_strip(2, 0, 2, near)
        relay_strip(2, 1, 2, near)

    pl.when((inside == 1) & (c == 0))(pass_second)
    gather_cross(2)
    on_end(lambda: take_z(3))
    send_own(3)
    pl.when((inside == 1) & (c == 1))(pass_second)

    @on_inner
    def _():
        relay_strip(3, 0, 3, near)
        relay_strip(3, 1, 3, near)

    gather_side(2)
    gather_far(2)

    def end_strip(t):
        take_strip(t, 0)
        take_strip(t, 1)

    on_end(lambda: end_strip(1))
    gather_cross(3)
    on_end(lambda: end_strip(2))
    gather_side(3)
    on_end(lambda: end_strip(3))
    for span, sem in zip(spans(3), (q3r.at[3], zr.at[0, 1])):
        with scope(f"q3_3_{span[2]}"):
            take_recv(some(area([span])), sem)
        same(piece(1 - x, origin[3], 1 - y, span), gcs, gcr, core_peer)

    with scope("finish"):
        take_send(st1.at[0:nx * 2 - 1], s1s)
        take_send(st2.at[0:nz - 1], s2s)
        take_send(some(area(halves)), qs.at[0])
        take_send(some(9 * area(parts)), qs.at[1])
        take_send(some(4 * area(halves)), ns)

        @on_end
        def _():
            take_send(some(2 * area(parts)), nzs)
            take_send(info.at[0:3], ins)
            take_send(some(4 * area(strips)), gks)

        @on_inner
        def _():
            take_send(some(6 * area(parts)), nzs)
            take_send(info, ins)
            take_send(some(2 * area(parts)), gzs)
            take_send(some(20 * area(strips)), gks)

        take_send(full.at[:, c], gcs)
        take_recv(full.at[:, c], gcr)


def write_out(nz, new, row, col, full, new_out, row_out, col_out, full_out, sem):
    pieces = [(full.at[a, b, u], full_out.at[a, b, u]) for a in range(2) for b in range(2) for u in range(nz)]
    copies = [pltpu.make_async_copy(src, dst, sem.at[0]) for src, dst in pieces]
    small = [pltpu.make_async_copy(src, dst, sem.at[k + 1])
             for k, (src, dst) in enumerate([(new, new_out), (row, row_out), (col, col_out)])]
    for copy in copies + small:
        copy.start()
    for copy in small:
        copy.wait()
    pltpu.make_async_copy(full, full_out, sem.at[0]).wait()


def fused(nx, nz, grad_bucket, parameters, row_state, column_state):
    _, _, full_width, columns = grad_bucket.shape
    rows = parameters.shape[1]
    lane = columns // 8
    bf16, f32 = jnp.bfloat16, jnp.float32
    vmem = pl.BlockSpec(memory_space=pltpu.VMEM)
    hbm = pl.BlockSpec(memory_space=pltpu.HBM)
    dma = pltpu.SemaphoreType.DMA
    one = dma(())
    shapes = [((rows, columns), bf16), ((1, rows), f32), ((1, columns), f32), ((2, 2, nz, 2, rows, columns), bf16)]
    held = 2 * columns * (rows + full_width) + 4 * (columns + -(-rows // 128) * 128)
    stat = columns + 128
    results = pl.pallas_call(
        functools.partial(kernel, nx, nz),
        out_shape=tuple(pltpu.VMEM(*shape) for shape in shapes),
        in_specs=[hbm] * 4,
        out_specs=(vmem,) * 4,
        scratch_shapes=[
            pltpu.VMEM((nz, 2, 2, rows, columns), bf16),
            pltpu.VMEM((nz, 2, 2, rows, columns), bf16),
            pltpu.VMEM((nz, 3, rows, columns), bf16),
            pltpu.VMEM((6, rows, columns), bf16),
            pltpu.VMEM((6, 2, 2, rows, 2 * lane), bf16),
            pltpu.VMEM((9 * 8 * (rows // TILE), TILE, lane), bf16),
            pltpu.VMEM((5, rows, columns), bf16),
            pltpu.VMEM((5, rows, columns), bf16),
            pltpu.VMEM((5, 2, rows), f32),
            pltpu.VMEM((5, rows, 1), f32),
            pltpu.VMEM((5, rows, 1), f32),
            pltpu.VMEM((5, rows, 1), f32),
            pltpu.VMEM((1, stat), f32),
            pltpu.VMEM((nx * 2, 1, stat), f32),
            pltpu.VMEM((1, stat), f32),
            pltpu.VMEM((nz, 1, stat), f32),
            pltpu.VMEM((1, rows), f32),
            pltpu.VMEM((1, columns), f32),
            dma((2,)), dma((3,)), one, dma((4,)), dma((nz,)), dma((2,)), dma((nz,)), dma((nz,)),
            one, dma((6, 2)), one, dma((5, 2)), one, one, one, one,
            one, dma((2,)), one, dma((2,)), one, dma((3,)),
        ],
        compiler_params=pltpu.CompilerParams(
            collective_id=0, has_side_effects=True, vmem_limit_bytes=VMEM_BYTES - held),
    )(grad_bucket.reshape(2, 2, nz, 2, rows, columns), parameters[0], row_state, column_state)
    new, row, col, full = pl.pallas_call(
        functools.partial(write_out, nz),
        out_shape=tuple(jax.ShapeDtypeStruct(*shape) for shape in shapes),
        in_specs=[vmem] * 4,
        out_specs=(hbm,) * 4,
        scratch_shapes=[dma((4,))],
        compiler_params=pltpu.CompilerParams(vmem_limit_bytes=4 * 1024 * 1024),
    )(*[pltpu.with_memory_space_constraint(result, pltpu.VMEM) for result in results])
    return (new[None], row, col, full.reshape(full_width, columns))


def solution(mesh):
    nx, nz, ny = (mesh.shape[a] for a in AXES)
    in_specs = (
        P(AXES, None, None, None),
        P(None, AXES, None),
        P(None, AXES),
        P(),
    )
    out_specs = (P(None, AXES, None), P(None, AXES), P(), P())
    fits = nx == 4 and ny == 2 and nz == 4

    def body(grad_bucket, parameters, row_state, column_state):
        if fits and grad_bucket.shape[1] == 1 and parameters.shape[1] % TILE == 0 and parameters.shape[1] >= 2 * TILE and grad_bucket.shape[3] % 1024 == 0:
            return fused(nx, nz, grad_bucket, parameters, row_state, column_state)
        return shards(grad_bucket, parameters, row_state, column_state)

    return jax.shard_map(body, mesh=mesh, in_specs=in_specs, out_specs=out_specs, check_vma=False)
```
